8 devices in a mesh: data: 8 (over z, y, x, core).
Axes of the slice: x: 2, y: 2, z: 1, core: 2. Of those that a mesh axis runs over, the one named last changes fastest.
Arguments:
- feat_a: bfloat16 [2048, 512], P('data')
- feat_b: bfloat16 [2048, 512], P('data')
- w_one: bfloat16 [512, 2048], replicated
- w_two: bfloat16 [2048, 2048], replicated
- w_three: bfloat16 [2048, 2048], replicated
- g_one: float32 [2048], replicated
- b_one: float32 [2048], replicated
- g_two: float32 [2048], replicated
- b_two: float32 [2048], replicated
- lam_off: float32 [], replicated
Outputs:
- output 1: float32 [], replicated
- output 2: float32 [512, 2048], replicated
- output 3: float32 [2048, 2048], replicated
- output 4: float32 [2048, 2048], replicated
- output 5: float32 [2048], replicated
- output 6: float32 [2048], replicated
- output 7: float32 [2048], replicated
- output 8: float32 [2048], replicated
All inputs are finite; a program needn't handle non-finite values.
Results may differ from the reference program's by a relative error of at most 0.00599.
Values are sent between devices in bfloat16 or wider.
A program may use at most 1 GiB of HBM per device.

```python
import jax
import jax.numpy as jnp
from jax import lax

F = 512
D = 2048
ROWS_DEV = 256
DATA_DEVS = 8
ROWS_ALL = ROWS_DEV * DATA_DEVS
NORM_EPS = 1e-5


def setup_inputs(seed: int = 0) -> dict:
    key_list = jax.random.split(jax.random.key(seed), 13)
    common = jax.random.normal(key_list[0], (ROWS_ALL, F), jnp.float32)
    offset = 0.8 * jax.random.normal(key_list[3], (DATA_DEVS, 1, F), jnp.float32)
    spread = jax.random.uniform(key_list[4], (DATA_DEVS, 1, F), jnp.float32, 0.5, 1.5)

    def shard_shift(values):
        return (values.reshape(DATA_DEVS, ROWS_DEV, F) * spread + offset).reshape(ROWS_ALL, F)

    noise_a = jax.random.normal(key_list[1], (ROWS_ALL, F), jnp.float32)
    noise_b = jax.random.normal(key_list[2], (ROWS_ALL, F), jnp.float32)
    feat_a = shard_shift(common + 0.65 * noise_a)
    feat_b = shard_shift(common + 0.65 * noise_b)
    w_one = jax.random.normal(key_list[5], (F, D), jnp.float32) * F ** -0.5
    w_two = jax.random.normal(key_list[6], (D, D), jnp.float32) * D ** -0.5
    w_three = jax.random.normal(key_list[7], (D, D), jnp.float32) * D ** -0.5
    g_one = jax.random.uniform(key_list[8], (D,), jnp.float32, 0.5, 1.5)
    b_one = 0.5 * jax.random.normal(key_list[9], (D,), jnp.float32)
    g_two = jax.random.uniform(key_list[10], (D,), jnp.float32, 0.5, 1.5)
    b_two = 0.5 * jax.random.normal(key_list[11], (D,), jnp.float32)
    lam_off = jax.random.uniform(key_list[12], (), jnp.float32, 0.15, 0.45) * ROWS_ALL / D
    return {'feat_a': feat_a.astype(jnp.bfloat16), 'feat_b': feat_b.astype(jnp.bfloat16), 'w_one': w_one.astype(jnp.bfloat16), 'w_two': w_two.astype(jnp.bfloat16), 'w_three': w_three.astype(jnp.bfloat16), 'g_one': g_one, 'b_one': b_one, 'g_two': g_two, 'b_two': b_two, 'lam_off': lam_off}


def normalize(pre):
    mean_val = jnp.mean(pre, axis=0)
    var_val = jnp.mean(pre * pre, axis=0) - mean_val * mean_val
    inv_std = lax.rsqrt(var_val + NORM_EPS)
    return (pre - mean_val) * inv_std, inv_std


def normalize_back(grad_norm, normed, inv_std):
    centred = grad_norm - jnp.mean(grad_norm, axis=0)
    return inv_std * (centred - normed * jnp.mean(grad_norm * normed, axis=0))


def forward_view(feat, w_one, w_two, w_three, g_one, b_one, g_two, b_two):
    pre_one = jnp.dot(feat, w_one, preferred_element_type=jnp.float32)
    norm_one, inv_one = normalize(pre_one)
    aff_one = norm_one * g_one + b_one
    act_one = jnp.maximum(aff_one, 0.0).astype(jnp.bfloat16)
    pre_two = jnp.dot(act_one, w_two, preferred_element_type=jnp.float32)
    norm_two, inv_two = normalize(pre_two)
    aff_two = norm_two * g_two + b_two
    act_two = jnp.maximum(aff_two, 0.0).astype(jnp.bfloat16)
    proj_out = jnp.dot(act_two, w_three, preferred_element_type=jnp.float32)
    norm_out, inv_out = normalize(proj_out)
    return (act_one, act_two, norm_one, norm_two, aff_one, aff_two, norm_out, inv_one, inv_two, inv_out)


def backward_view(feat, grad_emb, saved, w_two, w_three, g_one, g_two):
    act_one, act_two, norm_one, norm_two, aff_one, aff_two, norm_out, inv_one, inv_two, inv_out = saved
    grad_proj = normalize_back(grad_emb, norm_out, inv_out).astype(jnp.bfloat16)
    dw_three = jnp.dot(act_two.T, grad_proj, preferred_element_type=jnp.float32)
    grad_act_two = jnp.dot(grad_proj, w_three.T, preferred_element_type=jnp.float32)
    grad_aff_two = jnp.where(aff_two > 0, grad_act_two, 0.0)
    dg_two = jnp.sum(grad_aff_two * norm_two, axis=0)
    db_two = jnp.sum(grad_aff_two, axis=0)
    grad_pre_two = normalize_back(grad_aff_two * g_two, norm_two, inv_two).astype(jnp.bfloat16)
    dw_two = jnp.dot(act_one.T, grad_pre_two, preferred_element_type=jnp.float32)
    grad_act_one = jnp.dot(grad_pre_two, w_two.T, preferred_element_type=jnp.float32)
    grad_aff_one = jnp.where(aff_one > 0, grad_act_one, 0.0)
    dg_one = jnp.sum(grad_aff_one * norm_one, axis=0)
    db_one = jnp.sum(grad_aff_one, axis=0)
    grad_pre_one = normalize_back(grad_aff_one * g_one, norm_one, inv_one).astype(jnp.bfloat16)
    dw_one = jnp.dot(feat.T, grad_pre_one, preferred_element_type=jnp.float32)
    return (dw_one, dw_two, dw_three, dg_one, db_one, dg_two, db_two)


def reference(feat_a, feat_b, w_one, w_two, w_three, g_one, b_one, g_two, b_two, lam_off):
    saved_a = forward_view(feat_a, w_one, w_two, w_three, g_one, b_one, g_two, b_two)
    saved_b = forward_view(feat_b, w_one, w_two, w_three, g_one, b_one, g_two, b_two)
    emb_a = saved_a[6].astype(jnp.bfloat16)
    emb_b = saved_b[6].astype(jnp.bfloat16)
    corr = jnp.dot(emb_a.T, emb_b, preferred_element_type=jnp.float32) / ROWS_ALL
    diag_c = jnp.diagonal(corr)
    loss_val = jnp.sum((1.0 - diag_c) ** 2) + lam_off * (jnp.sum(corr * corr) - jnp.sum(diag_c * diag_c))
    on_diag = jnp.arange(D)[:, None] == jnp.arange(D)[None, :]
    grad_c = jnp.where(on_diag, -2.0 * (1.0 - corr), 2.0 * lam_off * corr).astype(jnp.bfloat16)
    grad_a = jnp.dot(emb_b, grad_c.T, preferred_element_type=jnp.float32) / ROWS_ALL
    grad_b = jnp.dot(emb_a, grad_c, preferred_element_type=jnp.float32) / ROWS_ALL
    grads_a = backward_view(feat_a, grad_a, saved_a, w_two, w_three, g_one, g_two)
    grads_b = backward_view(feat_b, grad_b, saved_b, w_two, w_three, g_one, g_two)
    return (loss_val, grads_a[0] + grads_b[0], grads_a[1] + grads_b[1], grads_a[2] + grads_b[2], grads_a[3] + grads_b[3], grads_a[4] + grads_b[4], grads_a[5] + grads_b[5], grads_a[6] + grads_b[6])
```

```python
import functools

import jax
import jax.numpy as jnp
from jax import lax
from jax.experimental import pallas as pl
from jax.experimental.pallas import tpu as pltpu
from jax.sharding import PartitionSpec as P

NORM_EPS = 1e-5
AXIS = 'data'
MESH = pl.DeviceIdType.MESH
F32 = jnp.float32
BF16 = jnp.bfloat16
ONCE = pl.Buffered(1)
VMEM_LIMIT = 60 * 1024 * 1024


def dot(a, b, dims=((1,), (0,))):
    return lax.dot_general(a, b, (dims, ((), ())), preferred_element_type=F32)


def gather_kernel(n, fa_ref, fb_ref, out_ref, local_sem, send_sem, recv_sem):
    me = lax.axis_index(AXIS)
    rows = fa_ref.shape[0]
    barrier = pltpu.get_barrier_semaphore()
    for off in range(1, n):
        pl.semaphore_signal(barrier, inc=1, device_id=(lax.rem(me + off, n),), device_id_type=MESH)
    pl.semaphore_wait(barrier, n - 1)
    dst = out_ref.at[pl.ds(pl.multiple_of(me * rows, rows), rows), :]

    def each(view, src):
        @pl.when(lax.rem(me, 2) == view)
        def _():
            for off in range(1, n):
                if off % 2 == 0:
                    remote(src, off).start()
            pltpu.make_async_copy(src, dst, local_sem).start()

        @pl.when(lax.rem(me, 2) == 1 - view)
        def _():
            for off in range(1, n):
                if off % 2 == 1:
                    remote(src, off).start()

    def remote(src, off):
        return pltpu.make_async_remote_copy(
            src_ref=src, dst_ref=dst, send_sem=send_sem.at[off], recv_sem=recv_sem.at[off],
            device_id=(lax.rem(me + off, n),), device_id_type=MESH)

    each(0, fa_ref)
    each(1, fb_ref)
    pltpu.make_async_copy(fa_ref, dst, local_sem).wait()
    for off in range(1, n):
        remote(fa_ref, off).wait()


def gather_view(fa, fb, n):
    rows, width = fa.shape
    return pl.pallas_call(
        functools.partial(gather_kernel, n),
        out_shape=jax.ShapeDtypeStruct((rows * n, width), fa.dtype),
        in_specs=[pl.BlockSpec(memory_space=pltpu.VMEM)] * 2,
        out_specs=pl.BlockSpec(memory_space=pltpu.VMEM),
        scratch_shapes=[pltpu.SemaphoreType.DMA, pltpu.SemaphoreType.DMA((n,)), pltpu.SemaphoreType.DMA((n,))],
        compiler_params=pltpu.CompilerParams(collective_id=0, has_side_effects=True),
        name='gather_view',
    )(fa, fb)


def fwd_kernel(rows, tile, affine, x_ref, w_ref, g_ref, b_ref, norm_ref, inv_ref, act_ref):
    total = jnp.zeros((1, w_ref.shape[1]), F32)
    square = jnp.zeros((1, w_ref.shape[1]), F32)
    for r in range(0, rows, tile):
        pre = dot(x_ref[r:r + tile, :], w_ref[...])
        norm_ref[r:r + tile, :] = pre
        total += jnp.sum(pre, axis=0, keepdims=True)
        square += jnp.sum(pre * pre, axis=0, keepdims=True)
    mean = total / rows
    inv = lax.rsqrt(square / rows - mean * mean + NORM_EPS)
    inv_ref[...] = inv
    for r in range(0, rows, tile):
        norm = (norm_ref[r:r + tile, :] - mean) * inv
        norm_ref[r:r + tile, :] = norm
        if affine:
            norm = jnp.maximum(norm * g_ref[...] + b_ref[...], 0.0)
        act_ref[r:r + tile, :] = norm.astype(BF16)


def forward_layer(x, w, g, b, affine, bn=256, tile=512):
    rows, k = x.shape
    d = w.shape[1]
    col = pl.BlockSpec((1, bn), lambda j: (0, j))
    return pl.pallas_call(
        functools.partial(fwd_kernel, rows, tile, affine),
        grid=(d // bn,),
        in_specs=[pl.BlockSpec((rows, k), lambda j: (0, 0), pipeline_mode=ONCE), pl.BlockSpec((k, bn), lambda j: (0, j)), col, col],
        out_specs=[pl.BlockSpec((rows, bn), lambda j: (0, j)), col, pl.BlockSpec((rows, bn), lambda j: (0, j))],
        out_shape=[jax.ShapeDtypeStruct((rows, d), F32), jax.ShapeDtypeStruct((1, d), F32), jax.ShapeDtypeStruct((rows, d), BF16)],
        compiler_params=pltpu.CompilerParams(vmem_limit_bytes=VMEM_LIMIT),
        cost_estimate=pl.CostEstimate(flops=2 * rows * k * d, bytes_accessed=rows * d * 6 + rows * k * 2, transcendentals=0),
        name='forward_layer',
    )(x, w, g, b)


def loss_kernel(rows, tile, lam_ref, own_ref, other_ref, norm_ref, inv_ref, loss_ref, out_ref, grad, dn):
    j = pl.program_id(0)
    bn = own_ref.shape[1]
    d = other_ref.shape[1]
    lam = lam_ref[0, 0]
    own = own_ref[...]
    loss = jnp.zeros((1, tile), F32)
    for c in range(0, d, tile):
        corr = dot(own, other_ref[:, c:c + tile], ((0,), (0,))) * (1.0 / rows)
        row_id = lax.broadcasted_iota(jnp.int32, (bn, tile), 0) + j * bn
        col_id = lax.broadcasted_iota(jnp.int32, (bn, tile), 1) + c
        diag = row_id == col_id
        loss += jnp.sum(jnp.where(diag, (1.0 - corr) * (1.0 - corr), lam * (corr * corr)), axis=0, keepdims=True)
        grad[:, c:c + tile] = jnp.where(diag, -2.0 * (1.0 - corr), (2.0 * lam) * corr).astype(BF16)

    @pl.when(j == 0)
    def _():
        loss_ref[...] = jnp.zeros_like(loss_ref)

    loss_ref[...] += loss
    total = jnp.zeros((1, bn), F32)
    cross = jnp.zeros((1, bn), F32)
    for r in range(0, rows, tile):
        part = dot(other_ref[r:r + tile, :], grad[...], ((1,), (1,))) * (1.0 / rows)
        dn[r:r + tile, :] = part
        total += jnp.sum(part, axis=0, keepdims=True)
        cross += jnp.sum(part * norm_ref[r:r + tile, :], axis=0, keepdims=True)
    total, cross = total / rows, cross / rows
    for r in range(0, rows, tile):
        out_ref[r:r + tile, :] = (inv_ref[...] * (dn[r:r + tile, :] - total - norm_ref[r:r + tile, :] * cross)).astype(BF16)


def loss_layer(own, other, norm, inv, lam, bn=256, tile=512):
    rows, d = own.shape
    col = pl.BlockSpec((1, bn), lambda j: (0, j))
    blk = pl.BlockSpec((rows, bn), lambda j: (0, j))
    return pl.pallas_call(
        functools.partial(loss_kernel, rows, tile),
        grid=(d // bn,),
        in_specs=[pl.BlockSpec(memory_space=pltpu.SMEM), blk, pl.BlockSpec((rows, d), lambda j: (0, 0), pipeline_mode=ONCE), blk, col],
        out_specs=[pl.BlockSpec((1, tile), lambda j: (0, 0)), blk],
        out_shape=[jax.ShapeDtypeStruct((1, tile), F32), jax.ShapeDtypeStruct((rows, d), BF16)],
        scratch_shapes=[pltpu.VMEM((bn, d), BF16), pltpu.VMEM((rows, bn), F32)],
        compiler_params=pltpu.CompilerParams(vmem_limit_bytes=VMEM_LIMIT),
        cost_estimate=pl.CostEstimate(flops=4 * rows * d * d, bytes_accessed=rows * d * 10, transcendentals=0),
        name='loss_layer',
    )(lam, own, other, norm, inv)


def bwd_kernel(rows, tile, x_ref, w_ref, norm_ref, inv_ref, g_ref, b_ref, out_ref, dg_ref, db_ref, da):
    total = jnp.zeros((1, w_ref.shape[0]), F32)
    cross = jnp.zeros((1, w_ref.shape[0]), F32)
    g = g_ref[...]
    for r in range(0, rows, tile):
        part = dot(x_ref[r:r + tile, :], w_ref[...], ((1,), (1,)))
        norm = norm_ref[r:r + tile, :]
        part = jnp.where(norm * g + b_ref[...] > 0.0, part, 0.0)
        da[r:r + tile, :] = part
        total += jnp.sum(part, axis=0, keepdims=True)
        cross += jnp.sum(part * norm, axis=0, keepdims=True)
    dg_ref[...] = cross
    db_ref[...] = total
    total, cross = total * g / rows, cross * g / rows
    for r in range(0, rows, tile):
        out_ref[r:r + tile, :] = (inv_ref[...] * (da[r:r + tile, :] * g - total - norm_ref[r:r + tile, :] * cross)).astype(BF16)


def backward_layer(x, w, norm, inv, g, b, bn=256, tile=512):
    rows, k = x.shape
    d = w.shape[0]
    col = pl.BlockSpec((1, bn), lambda j: (0, j))
    blk = pl.BlockSpec((rows, bn), lambda j: (0, j))
    return pl.pallas_call(
        functools.partial(bwd_kernel, rows, tile),
        grid=(d // bn,),
        in_specs=[pl.BlockSpec((rows, k), lambda j: (0, 0), pipeline_mode=ONCE), pl.BlockSpec((bn, k), lambda j: (j, 0)), blk, col, col, col],
        out_specs=[blk, col, col],
        out_shape=[jax.ShapeDtypeStruct((rows, d), BF16), jax.ShapeDtypeStruct((1, d), F32), jax.ShapeDtypeStruct((1, d), F32)],
        scratch_shapes=[pltpu.VMEM((rows, bn), F32)],
        compiler_params=pltpu.CompilerParams(vmem_limit_bytes=VMEM_LIMIT),
        cost_estimate=pl.CostEstimate(flops=2 * rows * k * d, bytes_accessed=rows * d * 6 + rows * k * 2, transcendentals=0),
        name='backward_layer',
    )(x, w, norm, inv, g, b)


def dw_kernel(tile, x_ref, y_ref, out_ref):
    x = x_ref[...]
    for c in range(0, y_ref.shape[1], tile):
        out_ref[:, c:c + tile] = dot(x, y_ref[:, c:c + tile], ((0,), (0,)))


def weight_grad(x, y, bm=256, tile=512):
    rows, k = x.shape
    d = y.shape[1]
    return pl.pallas_call(
        functools.partial(dw_kernel, tile),
        grid=(k // bm,),
        in_specs=[pl.BlockSpec((rows, bm), lambda j: (0, j)), pl.BlockSpec((rows, d), lambda j: (0, 0), pipeline_mode=ONCE)],
        out_specs=pl.BlockSpec((bm, d), lambda j: (j, 0)),
        out_shape=jax.ShapeDtypeStruct((k, d), F32),
        compiler_params=pltpu.CompilerParams(vmem_limit_bytes=VMEM_LIMIT),
        cost_estimate=pl.CostEstimate(flops=2 * rows * k * d, bytes_accessed=k * d * 4 + rows * (k + d) * 2, transcendentals=0),
        name='weight_grad',
    )(x, y)


def solution(mesh):
    n = mesh.shape[AXIS]
    pair = [(i, i + 1 - 2 * (i % 2)) for i in range(n)]

    def swap(x):
        return lax.ppermute(x, AXIS, pair)

    def local_step(feat_a, feat_b, w_one, w_two, w_three, g_one, b_one, g_two, b_two, lam_off):
        width = w_two.shape[0]
        g1, b1, g2, b2 = (v.reshape(1, width) for v in (g_one, b_one, g_two, b_two))
        x = gather_view(feat_a, feat_b, n)
        norm1, inv1, act1 = forward_layer(x, w_one, g1, b1, True)
        norm2, inv2, act2 = forward_layer(act1, w_two, g2, b2, True)
        norm3, inv3, emb = forward_layer(act2, w_three, g2, b2, False)
        other = swap(emb)
        loss, d_out = loss_layer(emb, other, norm3, inv3, lam_off.reshape(1, 1))
        dw3 = weight_grad(act2, d_out)
        dw3_other = swap(dw3)
        d_pre2, dg2, db2 = backward_layer(d_out, w_three, norm2, inv2, g2, b2)
        dw2 = weight_grad(act1, d_pre2)
        dw2_other = swap(dw2)
        d_pre1, dg1, db1 = backward_layer(d_pre2, w_two, norm1, inv1, g1, b1)
        dw1 = weight_grad(x, d_pre1)
        dw1_other = swap(dw1)
        small = jnp.concatenate([dg1, db1, dg2, db2, loss], axis=1)
        small = small + swap(small)
        dg1, db1, dg2, db2 = (small[0, i * width:(i + 1) * width] for i in range(4))
        loss_val = jnp.sum(small[0, 4 * width:]) * 0.5
        return (loss_val, dw1 + dw1_other, dw2 + dw2_other, dw3 + dw3_other, dg1, db1, dg2, db2)

    row_spec = P(AXIS, None)
    return jax.shard_map(local_step, mesh=mesh, in_specs=(row_spec, row_spec) + (P(),) * 8, out_specs=(P(),) * 8, check_vma=False)
```

```python
import functools

import jax
import jax.numpy as jnp
from jax import lax
from jax.experimental import pallas as pl
from jax.experimental.pallas import tpu as pltpu
from jax.sharding import PartitionSpec as P

NORM_EPS = 1e-5
AXIS = 'data'
MESH = pl.DeviceIdType.MESH
F32 = jnp.float32
BF16 = jnp.bfloat16
ONCE = pl.Buffered(1)
VMEM_LIMIT = 60 * 1024 * 1024
TILE = 256
CHUNK = 64


def fold(v):
    return jnp.sum(v.reshape(v.shape[0] // 8, 8, v.shape[1]), axis=0)


def dot(a, b, dims=((1,), (0,))):
    return lax.dot_general(a, b, (dims, ((), ())), preferred_element_type=F32)


def forward_kernel(nb, rows, fa_ref, fb_ref, w1_ref, w2_ref, w3_ref, g1_ref, b1_ref, g2_ref, b2_ref,
                   n1_ref, n2_ref, n3_ref, i1_ref, i2_ref, i3_ref, x_hbm, act1_hbm, act2_hbm, emb_hbm, other_hbm,
                   xs, bufa, bufb, acc, copy_sem, feat_sem, send_sem, recv_sem, esend_sem, erecv_sem):
    j = pl.program_id(0)
    me = lax.axis_index(AXIS)
    core = lax.rem(me, 2)
    chip = me // 2
    x_pos, y_pos = lax.rem(chip, 2), chip // 2
    partner = me + 1 - 2 * core
    x_chip, y_chip = chip + 1 - 2 * x_pos, chip + 2 - 4 * y_pos
    piece = fa_ref.shape[0]
    bn = acc.shape[1]

    def remote(src, dst, send, recv, dev):
        return pltpu.make_async_remote_copy(src_ref=src, dst_ref=dst, send_sem=send, recv_sem=recv, device_id=(dev,), device_id_type=MESH)

    def part(dev):
        return xs.at[pl.ds(pl.multiple_of(dev * piece, piece), piece), :]

    def gather():
        barrier = pltpu.get_barrier_semaphore()
        for dev in (partner, 2 * x_chip, 2 * x_chip + 1, 2 * y_chip, 2 * y_chip + 1):
            pl.semaphore_signal(barrier, inc=1, device_id=(dev,), device_id_type=MESH)
        pl.semaphore_wait(barrier, 5)

        def sends(mine, mine_src, theirs_src):
            for view, src in ((mine, mine_src), (1 - mine, theirs_src)):
                remote(src, part(me), send_sem.at[1 + view], recv_sem.at[1 + mine], 2 * x_chip + view).start()
                remote(src, part(me), send_sem.at[3 + view], recv_sem.at[3 + mine], 2 * y_chip + view).start()
            remote(theirs_src, part(me), send_sem.at[0], recv_sem.at[0], partner).start()
            pltpu.make_async_copy(mine_src, part(me), feat_sem).start()

        pl.when(core == 0)(lambda: sends(0, fa_ref, fb_ref))
        pl.when(core == 1)(lambda: sends(1, fb_ref, fa_ref))
        remote(fa_ref, part(2 * x_chip), send_sem.at[1], recv_sem.at[1], me).wait_recv()
        relay_y = remote(part(2 * x_chip), part(2 * x_chip), send_sem.at[5], recv_sem.at[5], 2 * y_chip + core)
        relay_y.start()
        remote(fa_ref, part(2 * y_chip + 1), send_sem.at[4], recv_sem.at[4], me).wait_recv()
        relay_x = remote(part(2 * y_chip + 1), part(2 * y_chip + 1), send_sem.at[6], recv_sem.at[6], 2 * x_chip + core)
        relay_x.start()
        pltpu.make_async_copy(fa_ref, part(me), feat_sem).wait()
        remote(fa_ref, part(me), send_sem.at[0], recv_sem.at[0], me).wait()
        remote(fa_ref, part(me), send_sem.at[1], recv_sem.at[2], me).wait()
        remote(fa_ref, part(me), send_sem.at[2], recv_sem.at[3], me).wait()
        remote(fa_ref, part(me), send_sem.at[3], recv_sem.at[5], me).wait()
        remote(fa_ref, part(me), send_sem.at[4], recv_sem.at[6], me).wait()
        relay_y.wait_send()
        relay_x.wait_send()

    def fin(layer):
        norm_ref, inv_ref = ((n1_ref, i1_ref), (n2_ref, i2_ref), (n3_ref, i3_ref))[layer]
        buf = (bufa, bufb, bufa)[layer]
        base = pl.multiple_of((j - 1 - layer * nb) * bn, bn)
        total = jnp.zeros((8, bn), F32)
        square = jnp.zeros((8, bn), F32)
        for r in range(0, rows, CHUNK):
            pre = acc[r:r + CHUNK, :]
            total += fold(pre)
            square += fold(pre * pre)
        mean = jnp.sum(total, axis=0, keepdims=True) / rows
        inv = lax.rsqrt(jnp.sum(square, axis=0, keepdims=True) / rows - mean * mean + NORM_EPS)
        inv_ref[...] = inv
        if layer < 2:
            g_ref, b_ref = ((g1_ref, b1_ref), (g2_ref, b2_ref))[layer]
            g, b = g_ref[...], b_ref[...]
        for r in range(0, rows, CHUNK):
            norm = (acc[r:r + CHUNK, :] - mean) * inv
            norm_ref[r:r + CHUNK, :] = norm
            if layer < 2:
                norm = jnp.maximum(norm * g + b, 0.0)
            buf[r:r + CHUNK, pl.ds(base, bn)] = norm.astype(BF16)

    def mm(layer):
        x_ref, w_ref = ((xs, w1_ref), (bufa, w2_ref), (bufb, w3_ref))[layer]
        for r in range(0, rows, TILE):
            acc[r:r + TILE, :] = dot(x_ref[r:r + TILE, :], w_ref[...])

    def out_copy(layer, block):
        cols = pl.ds(pl.multiple_of(block * bn, bn), bn)
        src = (bufa, bufb, bufa)[layer].at[:, cols]
        dst = (act1_hbm, act2_hbm, emb_hbm)[layer].at[:, cols]
        return pltpu.make_async_copy(src, dst, copy_sem.at[layer * nb + block])

    def emb_copy(block):
        cols = pl.ds(pl.multiple_of(block * bn, bn), bn)
        return remote(bufa.at[:, cols], other_hbm.at[:, cols], esend_sem.at[block], erecv_sem.at[block], partner)

    @pl.when(j == 0)
    def _():
        gather()
        pltpu.make_async_copy(xs, x_hbm, feat_sem).start()
        mm(0)

    for layer in range(3):
        @pl.when((j >= layer * nb + 2) & (j < (layer + 1) * nb + 2))
        def _(layer=layer):
            block = j - 2 - layer * nb
            out_copy(layer, block).start()
            if layer == 2:
                emb_copy(block).start()

        @pl.when((j > layer * nb) & (j < (layer + 1) * nb))
        def _(layer=layer):
            fin(layer)
            mm(layer)

        @pl.when(j == (layer + 1) * nb)
        def _(layer=layer):
            if layer == 1:
                for block in range(nb):
                    out_copy(0, block).wait()
            fin(layer)
            if layer < 2:
                mm(layer + 1)

    @pl.when(j == 3 * nb + 1)
    def _():
        for layer in (1, 2):
            for block in range(nb):
                out_copy(layer, block).wait()
        pltpu.make_async_copy(xs, x_hbm, feat_sem).wait()
        for block in range(nb):
            emb_copy(block).wait()


def forward(fa, fb, w1, w2, w3, g1, b1, g2, b2, n, bn=256):
    piece, k = fa.shape
    rows, d = piece * n, w2.shape[1]
    nb = d // bn

    def at(layer, delay):
        return lambda j: (0, jnp.clip(j - layer * nb - delay, 0, nb - 1))

    whole = pl.BlockSpec((piece, k), lambda j: (0, 0), pipeline_mode=ONCE)
    any_spec = pl.BlockSpec(memory_space=pl.ANY)
    col = [pl.BlockSpec((1, bn), at(layer, 1)) for layer in range(3)]
    norm = [pl.BlockSpec((rows, bn), at(layer, 1)) for layer in range(3)]
    big = jax.ShapeDtypeStruct((rows, d), BF16)
    return pl.pallas_call(
        functools.partial(forward_kernel, nb, rows),
        grid=(3 * nb + 2,),
        in_specs=[whole, whole, pl.BlockSpec((k, bn), at(0, 0)), pl.BlockSpec((d, bn), at(1, 0)), pl.BlockSpec((d, bn), at(2, 0)),
                  col[0], col[0], col[1], col[1]],
        out_specs=norm + col + [any_spec] * 5,
        out_shape=[jax.ShapeDtypeStruct((rows, d), F32)] * 3 + [jax.ShapeDtypeStruct((1, d), F32)] * 3
        + [jax.ShapeDtypeStruct((rows, k), BF16)] + [big] * 4,
        scratch_shapes=[pltpu.VMEM((rows, k), BF16), pltpu.VMEM((rows, d), BF16), pltpu.VMEM((rows, d), BF16), pltpu.VMEM((rows, bn), F32),
                        pltpu.SemaphoreType.DMA((3 * nb,)), pltpu.SemaphoreType.DMA, pltpu.SemaphoreType.DMA((7,)), pltpu.SemaphoreType.DMA((7,)),
                        pltpu.SemaphoreType.DMA((nb,)), pltpu.SemaphoreType.DMA((nb,))],
        compiler_params=pltpu.CompilerParams(collective_id=0, has_side_effects=True, vmem_limit_bytes=VMEM_LIMIT),
        cost_estimate=pl.CostEstimate(flops=2 * rows * d * (k + 2 * d), bytes_accessed=rows * d * 20, transcendentals=0),
        name='forward',
    )(fa, fb, w1, w2, w3, g1, b1, g2, b2)


def loss_kernel(rows, tile, lam_ref, own_ref, other_ref, norm_ref, inv_ref, loss_ref, out_ref, grad, dn):
    j = pl.program_id(0)
    bn = own_ref.shape[1]
    d = other_ref.shape[1]
    lam = lam_ref[0, 0]
    own = own_ref[...]
    loss = jnp.zeros((1, tile), F32)
    for c in range(0, d, tile):
        corr = dot(own, other_ref[:, c:c + tile], ((0,), (0,))) * (1.0 / rows)
        row_id = lax.broadcasted_iota(jnp.int32, (bn, tile), 0) + j * bn
        col_id = lax.broadcasted_iota(jnp.int32, (bn, tile), 1) + c
        diag = row_id == col_id
        loss += jnp.sum(jnp.where(diag, (1.0 - corr) * (1.0 - corr), lam * (corr * corr)), axis=0, keepdims=True)
        grad[:, c:c + tile] = jnp.where(diag, -2.0 * (1.0 - corr), (2.0 * lam) * corr).astype(BF16)

    @pl.when(j == 0)
    def _():
        loss_ref[...] = jnp.zeros_like(loss_ref)

    loss_ref[...] += loss
    total = jnp.zeros((1, bn), F32)
    cross = jnp.zeros((1, bn), F32)
    for r in range(0, rows, tile):
        part = dot(other_ref[r:r + tile, :], grad[...], ((1,), (1,))) * (1.0 / rows)
        dn[r:r + tile, :] = part
        total += jnp.sum(part, axis=0, keepdims=True)
        cross += jnp.sum(part * norm_ref[r:r + tile, :], axis=0, keepdims=True)
    total, cross = total / rows, cross / rows
    for r in range(0, rows, tile):
        out_ref[r:r + tile, :] = (inv_ref[...] * (dn[r:r + tile, :] - total - norm_ref[r:r + tile, :] * cross)).astype(BF16)


def loss_layer(own, other, norm, inv, lam, bn=256, tile=512):
    rows, d = own.shape
    col = pl.BlockSpec((1, bn), lambda j: (0, j))
    blk = pl.BlockSpec((rows, bn), lambda j: (0, j))
    return pl.pallas_call(
        functools.partial(loss_kernel, rows, tile),
        grid=(d // bn,),
        in_specs=[pl.BlockSpec(memory_space=pltpu.SMEM), blk, pl.BlockSpec((rows, d), lambda j: (0, 0), pipeline_mode=ONCE), blk, col],
        out_specs=[pl.BlockSpec((1, tile), lambda j: (0, 0)), blk],
        out_shape=[jax.ShapeDtypeStruct((1, tile), F32), jax.ShapeDtypeStruct((rows, d), BF16)],
        scratch_shapes=[pltpu.VMEM((bn, d), BF16), pltpu.VMEM((rows, bn), F32)],
        compiler_params=pltpu.CompilerParams(vmem_limit_bytes=VMEM_LIMIT),
        cost_estimate=pl.CostEstimate(flops=4 * rows * d * d, bytes_accessed=rows * d * 10, transcendentals=0),
        name='loss_layer',
    )(lam, own, other, norm, inv)


def bwd_kernel(rows, tile, x_ref, w_ref, norm_ref, inv_ref, g_ref, b_ref, out_ref, dg_ref, db_ref, da):
    total = jnp.zeros((1, w_ref.shape[0]), F32)
    cross = jnp.zeros((1, w_ref.shape[0]), F32)
    g = g_ref[...]
    for r in range(0, rows, tile):
        part = dot(x_ref[r:r + tile, :], w_ref[...], ((1,), (1,)))
        norm = norm_ref[r:r + tile, :]
        part = jnp.where(norm * g + b_ref[...] > 0.0, part, 0.0)
        da[r:r + tile, :] = part
        total += jnp.sum(part, axis=0, keepdims=True)
        cross += jnp.sum(part * norm, axis=0, keepdims=True)
    dg_ref[...] = cross
    db_ref[...] = total
    total, cross = total * g / rows, cross * g / rows
    for r in range(0, rows, tile):
        out_ref[r:r + tile, :] = (inv_ref[...] * (da[r:r + tile, :] * g - total - norm_ref[r:r + tile, :] * cross)).astype(BF16)


def backward_layer(x, w, norm, inv, g, b, bn=256, tile=512):
    rows, k = x.shape
    d = w.shape[0]
    col = pl.BlockSpec((1, bn), lambda j: (0, j))
    blk = pl.BlockSpec((rows, bn), lambda j: (0, j))
    return pl.pallas_call(
        functools.partial(bwd_kernel, rows, tile),
        grid=(d // bn,),
        in_specs=[pl.BlockSpec((rows, k), lambda j: (0, 0), pipeline_mode=ONCE), pl.BlockSpec((bn, k), lambda j: (j, 0)), blk, col, col, col],
        out_specs=[blk, col, col],
        out_shape=[jax.ShapeDtypeStruct((rows, d), BF16), jax.ShapeDtypeStruct((1, d), F32), jax.ShapeDtypeStruct((1, d), F32)],
        scratch_shapes=[pltpu.VMEM((rows, bn), F32)],
        compiler_params=pltpu.CompilerParams(vmem_limit_bytes=VMEM_LIMIT),
        cost_estimate=pl.CostEstimate(flops=2 * rows * k * d, bytes_accessed=rows * d * 6 + rows * k * 2, transcendentals=0),
        name='backward_layer',
    )(x, w, norm, inv, g, b)


def dw_kernel(tile, x_ref, y_ref, out_ref):
    x = x_ref[...]
    for c in range(0, y_ref.shape[1], tile):
        out_ref[:, c:c + tile] = dot(x, y_ref[:, c:c + tile], ((0,), (0,)))


def weight_grad(x, y, bm=256, tile=512):
    rows, k = x.shape
    d = y.shape[1]
    return pl.pallas_call(
        functools.partial(dw_kernel, tile),
        grid=(k // bm,),
        in_specs=[pl.BlockSpec((rows, bm), lambda j: (0, j)), pl.BlockSpec((rows, d), lambda j: (0, 0), pipeline_mode=ONCE)],
        out_specs=pl.BlockSpec((bm, d), lambda j: (j, 0)),
        out_shape=jax.ShapeDtypeStruct((k, d), F32),
        compiler_params=pltpu.CompilerParams(vmem_limit_bytes=VMEM_LIMIT),
        cost_estimate=pl.CostEstimate(flops=2 * rows * k * d, bytes_accessed=k * d * 4 + rows * (k + d) * 2, transcendentals=0),
        name='weight_grad',
    )(x, y)


def solution(mesh):
    n = mesh.shape[AXIS]
    pair = [(i, i + 1 - 2 * (i % 2)) for i in range(n)]

    def swap(x):
        return lax.ppermute(x, AXIS, pair)

    def local_step(feat_a, feat_b, w_one, w_two, w_three, g_one, b_one, g_two, b_two, lam_off):
        width = w_two.shape[0]
        g1, b1, g2, b2 = (v.reshape(1, width) for v in (g_one, b_one, g_two, b_two))
        norm1, norm2, norm3, inv1, inv2, inv3, x, act1, act2, emb, other = forward(
            feat_a, feat_b, w_one, w_two, w_three, g1, b1, g2, b2, n)
        loss, d_out = loss_layer(emb, other, norm3, inv3, lam_off.reshape(1, 1))
        dw3 = weight_grad(act2, d_out)
        dw3_other = swap(dw3)
        d_pre2, dg2, db2 = backward_layer(d_out, w_three, norm2, inv2, g2, b2)
        dw2 = weight_grad(act1, d_pre2)
        dw2_other = swap(dw2)
        d_pre1, dg1, db1 = backward_layer(d_pre2, w_two, norm1, inv1, g1, b1)
        dw1 = weight_grad(x, d_pre1)
        dw1_other = swap(dw1)
        small = jnp.concatenate([dg1, db1, dg2, db2, loss], axis=1)
        small = small + swap(small)
        dg1, db1, dg2, db2 = (small[0, i * width:(i + 1) * width] for i in range(4))
        loss_val = jnp.sum(small[0, 4 * width:]) * 0.5
        return (loss_val, dw1 + dw1_other, dw2 + dw2_other, dw3 + dw3_other, dg1, db1, dg2, db2)

    row_spec = P(AXIS, None)
    return jax.shard_map(local_step, mesh=mesh, in_specs=(row_spec, row_spec) + (P(),) * 8, out_specs=(P(),) * 8, check_vma=False)
```

```python
import functools

import jax
import jax.numpy as jnp
from jax import lax
from jax.experimental import pallas as pl
from jax.experimental.pallas import tpu as pltpu
from jax.sharding import PartitionSpec as P

NORM_EPS = 1e-5
AXIS = 'data'
MESH = pl.DeviceIdType.MESH
F32 = jnp.float32
BF16 = jnp.bfloat16
ONCE = pl.Buffered(1)
VMEM_LIMIT = 60 * 1024 * 1024
TILE = 256
CHUNK = 64


def fold(v):
    return jnp.sum(v.reshape(v.shape[0] // 8, 8, v.shape[1]), axis=0)


def dot(a, b, dims=((1,), (0,))):
    return lax.dot_general(a, b, (dims, ((), ())), preferred_element_type=F32)


def forward_kernel(nb, rows, fa_ref, fb_ref, w1_ref, w2_ref, w3_ref, g1_ref, b1_ref, g2_ref, b2_ref,
                   n1_ref, n2_ref, n3_ref, i1_ref, i2_ref, i3_ref, x_hbm, act1_hbm, act2_hbm, emb_hbm, other_hbm,
                   xs, bufa, bufb, acc, copy_sem, feat_sem, send_sem, recv_sem, esend_sem, erecv_sem):
    j = pl.program_id(0)
    me = lax.axis_index(AXIS)
    core = lax.rem(me, 2)
    chip = me // 2
    x_pos, y_pos = lax.rem(chip, 2), chip // 2
    partner = me + 1 - 2 * core
    x_chip, y_chip = chip + 1 - 2 * x_pos, chip + 2 - 4 * y_pos
    piece = fa_ref.shape[0]
    bn = acc.shape[1]

    def remote(src, dst, send, recv, dev):
        return pltpu.make_async_remote_copy(src_ref=src, dst_ref=dst, send_sem=send, recv_sem=recv, device_id=(dev,), device_id_type=MESH)

    def part(dev):
        return xs.at[pl.ds(pl.multiple_of(dev * piece, piece), piece), :]

    def gather():
        barrier = pltpu.get_barrier_semaphore()
        for dev in (partner, 2 * x_chip, 2 * x_chip + 1, 2 * y_chip, 2 * y_chip + 1):
            pl.semaphore_signal(barrier, inc=1, device_id=(dev,), device_id_type=MESH)
        pl.semaphore_wait(barrier, 5)

        def sends(mine, mine_src, theirs_src):
            for view, src in ((mine, mine_src), (1 - mine, theirs_src)):
                remote(src, part(me), send_sem.at[1 + view], recv_sem.at[1 + mine], 2 * x_chip + view).start()
                remote(src, part(me), send_sem.at[3 + view], recv_sem.at[3 + mine], 2 * y_chip + view).start()
            remote(theirs_src, part(me), send_sem.at[0], recv_sem.at[0], partner).start()
            pltpu.make_async_copy(mine_src, part(me), feat_sem).start()

        pl.when(core == 0)(lambda: sends(0, fa_ref, fb_ref))
        pl.when(core == 1)(lambda: sends(1, fb_ref, fa_ref))
        remote(fa_ref, part(2 * x_chip), send_sem.at[1], recv_sem.at[1], me).wait_recv()
        relay_y = remote(part(2 * x_chip), part(2 * x_chip), send_sem.at[5], recv_sem.at[5], 2 * y_chip + core)
        relay_y.start()
        remote(fa_ref, part(2 * y_chip + 1), send_sem.at[4], recv_sem.at[4], me).wait_recv()
        relay_x = remote(part(2 * y_chip + 1), part(2 * y_chip + 1), send_sem.at[6], recv_sem.at[6], 2 * x_chip + core)
        relay_x.start()
        pltpu.make_async_copy(fa_ref, part(me), feat_sem).wait()
        remote(fa_ref, part(me), send_sem.at[0], recv_sem.at[0], me).wait()
        remote(fa_ref, part(me), send_sem.at[1], recv_sem.at[2], me).wait()
        remote(fa_ref, part(me), send_sem.at[2], recv_sem.at[3], me).wait()
        remote(fa_ref, part(me), send_sem.at[3], recv_sem.at[5], me).wait()
        remote(fa_ref, part(me), send_sem.at[4], recv_sem.at[6], me).wait()
        relay_y.wait_send()
        relay_x.wait_send()

    def fin(layer):
        norm_ref, inv_ref = ((n1_ref, i1_ref), (n2_ref, i2_ref), (n3_ref, i3_ref))[layer]
        buf = (bufa, bufb, bufa)[layer]
        base = pl.multiple_of(jnp.maximum(j - 1 - layer * nb, 0) * bn, bn)
        total = jnp.zeros((8, bn), F32)
        square = jnp.zeros((8, bn), F32)
        for r in range(0, rows, CHUNK):
            pre = acc[r:r + CHUNK, :]
            total += fold(pre)
            square += fold(pre * pre)
        mean = jnp.sum(total, axis=0, keepdims=True) / rows
        inv = lax.rsqrt(jnp.sum(square, axis=0, keepdims=True) / rows - mean * mean + NORM_EPS)
        inv_ref[...] = inv
        if layer < 2:
            g_ref, b_ref = ((g1_ref, b1_ref), (g2_ref, b2_ref))[layer]
            g, b = g_ref[...], b_ref[...]
        for r in range(0, rows, CHUNK):
            norm = (acc[r:r + CHUNK, :] - mean) * inv
            norm_ref[r:r + CHUNK, :] = norm
            if layer < 2:
                norm = jnp.maximum(norm * g + b, 0.0)
            buf[r:r + CHUNK, pl.ds(base, bn)] = norm.astype(BF16)

    def mm(layer):
        x_ref, w_ref = ((xs, w1_ref), (bufa, w2_ref), (bufb, w3_ref))[layer]
        for r in range(0, rows, TILE):
            acc[r:r + TILE, :] = dot(x_ref[r:r + TILE, :], w_ref[...])

    def out_copy(layer, block):
        cols = pl.ds(pl.multiple_of(block * bn, bn), bn)
        src = (bufa, bufb, bufa)[layer].at[:, cols]
        dst = (act1_hbm, act2_hbm, emb_hbm)[layer].at[:, cols]
        return pltpu.make_async_copy(src, dst, copy_sem.at[layer * nb + block])

    def emb_copy(block):
        cols = pl.ds(pl.multiple_of(block * bn, bn), bn)
        return remote(bufa.at[:, cols], other_hbm.at[:, cols], esend_sem.at[block], erecv_sem.at[block], partner)

    @pl.when(j == 0)
    def _():
        gather()
        pltpu.make_async_copy(xs, x_hbm, feat_sem).start()

    for layer in range(3):
        @pl.when((j >= layer * nb + 2) & (j < (layer + 1) * nb + 2))
        def _(layer=layer):
            block = j - 2 - layer * nb
            out_copy(layer, block).start()
            if layer == 2:
                emb_copy(block).start()

        @pl.when((j >= layer * nb) & (j < (layer + 1) * nb))
        def _(layer=layer):
            fin(layer)
            mm(layer)

        @pl.when(j == (layer + 1) * nb)
        def _(layer=layer):
            if layer == 1:
                for block in range(nb):
                    out_copy(0, block).wait()
            fin(layer)

    @pl.when(j == 3 * nb + 1)
    def _():
        for layer in (1, 2):
            for block in range(nb):
                out_copy(layer, block).wait()
        pltpu.make_async_copy(xs, x_hbm, feat_sem).wait()
        for block in range(nb):
            emb_copy(block).wait()


def forward(fa, fb, w1, w2, w3, g1, b1, g2, b2, n, bn=256):
    piece, k = fa.shape
    rows, d = piece * n, w2.shape[1]
    nb = d // bn

    def at(layer, delay):
        return lambda j: (0, jnp.clip(j - layer * nb - delay, 0, nb - 1))

    whole = pl.BlockSpec((piece, k), lambda j: (0, 0), pipeline_mode=ONCE)
    any_spec = pl.BlockSpec(memory_space=pl.ANY)
    col = [pl.BlockSpec((1, bn), at(layer, 1)) for layer in range(3)]
    norm = [pl.BlockSpec((rows, bn), at(layer, 1)) for layer in range(3)]
    big = jax.ShapeDtypeStruct((rows, d), BF16)
    return pl.pallas_call(
        functools.partial(forward_kernel, nb, rows),
        grid=(3 * nb + 2,),
        in_specs=[whole, whole, pl.BlockSpec((k, bn), at(0, 0)), pl.BlockSpec((d, bn), at(1, 0)), pl.BlockSpec((d, bn), at(2, 0)),
                  col[0], col[0], col[1], col[1]],
        out_specs=norm + col + [any_spec] * 5,
        out_shape=[jax.ShapeDtypeStruct((rows, d), F32)] * 3 + [jax.ShapeDtypeStruct((1, d), F32)] * 3
        + [jax.ShapeDtypeStruct((rows, k), BF16)] + [big] * 4,
        scratch_shapes=[pltpu.VMEM((rows, k), BF16), pltpu.VMEM((rows, d), BF16), pltpu.VMEM((rows, d), BF16), pltpu.VMEM((rows, bn), F32),
                        pltpu.SemaphoreType.DMA((3 * nb,)), pltpu.SemaphoreType.DMA, pltpu.SemaphoreType.DMA((7,)), pltpu.SemaphoreType.DMA((7,)),
                        pltpu.SemaphoreType.DMA((nb,)), pltpu.SemaphoreType.DMA((nb,))],
        compiler_params=pltpu.CompilerParams(collective_id=0, has_side_effects=True, vmem_limit_bytes=VMEM_LIMIT),
        cost_estimate=pl.CostEstimate(flops=2 * rows * d * (k + 2 * d), bytes_accessed=rows * d * 20, transcendentals=0),
        name='forward',
    )(fa, fb, w1, w2, w3, g1, b1, g2, b2)


def finish_back(rows, acc, norm_ref, inv, g, b, put):
    bn = acc.shape[1]
    total = jnp.zeros((8, bn), F32)
    cross = jnp.zeros((8, bn), F32)
    for r in range(0, rows, CHUNK):
        part = acc[r:r + CHUNK, :]
        norm = norm_ref[r:r + CHUNK, :]
        if b is not None:
            part = jnp.where(norm * g + b > 0.0, part, 0.0)
            acc[r:r + CHUNK, :] = part
        total += fold(part)
        cross += fold(part * norm)
    total = jnp.sum(total, axis=0, keepdims=True)
    cross = jnp.sum(cross, axis=0, keepdims=True)
    scale = inv if g is None else inv * g
    shift, slope = scale * (total / rows), scale * (cross / rows)
    for r in range(0, rows, CHUNK):
        put(r, (acc[r:r + CHUNK, :] * scale - shift - norm_ref[r:r + CHUNK, :] * slope).astype(BF16))
    return total, cross


def back_a_kernel(nb, rows, lam_ref, own_ref, other_ref, n3_ref, i3_ref, w3_ref, n2_ref, i2_ref, g2_ref, b2_ref, act2_ref,
                  loss_ref, dw3_ref, dpre_ref, dg_ref, db_ref, corr, grad, acc, dout):
    j = pl.program_id(0)
    bn = acc.shape[1]
    d = other_ref.shape[1]
    lam = lam_ref[0, 0]

    def fin_loss():
        base = pl.multiple_of(jnp.maximum(j - 1, 0) * bn, bn)

        def put(r, v):
            dout[r:r + CHUNK, pl.ds(base, bn)] = v

        finish_back(rows, acc, n3_ref, i3_ref[...], None, None, put)

    def mm_loss():
        own = own_ref[...]
        loss = jnp.zeros((8, bn), F32)
        for c in range(0, d, bn):
            part = dot(own, other_ref[:, c:c + bn], ((0,), (0,))) * (1.0 / rows)
            corr[:, c:c + bn] = part
            loss += fold(part * part)
            grad[:, c:c + bn] = ((2.0 * lam) * part).astype(BF16)
        here = pl.ds(pl.multiple_of(j * bn, bn), bn)
        part = corr[:, here]
        diag = lax.broadcasted_iota(jnp.int32, (bn, bn), 0) == lax.broadcasted_iota(jnp.int32, (bn, bn), 1)
        grad[:, here] = jnp.where(diag, -2.0 * (1.0 - part), (2.0 * lam) * part).astype(BF16)
        loss = lam * loss + fold(jnp.where(diag, (1.0 - part) * (1.0 - part) - lam * (part * part), 0.0))
        loss_ref[...] += jnp.sum(loss, axis=0, keepdims=True)
        for r in range(0, rows, TILE):
            acc[r:r + TILE, :] = dot(other_ref[r:r + TILE, :], grad[...], ((1,), (1,))) * (1.0 / rows)

    def fin_two():
        def put(r, v):
            dpre_ref[r:r + CHUNK, :] = v

        db_ref[...], dg_ref[...] = finish_back(rows, acc, n2_ref, i2_ref[...], g2_ref[...], b2_ref[...], put)

    def mm_two():
        for r in range(0, rows, TILE):
            acc[r:r + TILE, :] = dot(dout[r:r + TILE, :], w3_ref[...], ((1,), (1,)))
        act = act2_ref[...]
        for c in range(0, d, 2 * bn):
            dw3_ref[:, c:c + 2 * bn] = dot(act, dout[:, c:c + 2 * bn], ((0,), (0,)))

    @pl.when(j == 0)
    def _():
        loss_ref[...] = jnp.zeros_like(loss_ref)

    @pl.when(j < nb)
    def _():
        fin_loss()
        mm_loss()

    @pl.when(j == nb)
    def _():
        fin_loss()

    @pl.when((j >= nb) & (j < 2 * nb))
    def _():
        fin_two()
        mm_two()

    @pl.when(j == 2 * nb)
    def _():
        fin_two()


def back_a(lam, own, other, n3, i3, w3, n2, i2, g2, b2, act2, bn=256):
    rows, d = own.shape
    nb = d // bn

    def at(first):
        return lambda j: (0, jnp.clip(j - first, 0, nb - 1))

    def block(first):
        return pl.BlockSpec((rows, bn), at(first))

    def col(first):
        return pl.BlockSpec((1, bn), at(first))

    row = pl.BlockSpec((bn, d), lambda j: (jnp.clip(j - nb, 0, nb - 1), 0))
    vec = jax.ShapeDtypeStruct((1, d), F32)
    return pl.pallas_call(
        functools.partial(back_a_kernel, nb, rows),
        grid=(2 * nb + 1,),
        in_specs=[pl.BlockSpec(memory_space=pltpu.SMEM), block(0), pl.BlockSpec((rows, d), lambda j: (0, 0), pipeline_mode=ONCE),
                  block(1), col(1), row, block(nb + 1), col(nb + 1), col(nb + 1), col(nb + 1), block(nb)],
        out_specs=[pl.BlockSpec((1, bn), lambda j: (0, 0)), row, block(nb + 1), col(nb + 1), col(nb + 1)],
        out_shape=[jax.ShapeDtypeStruct((1, bn), F32), jax.ShapeDtypeStruct((d, d), F32), jax.ShapeDtypeStruct((rows, d), BF16), vec, vec],
        scratch_shapes=[pltpu.VMEM((bn, d), F32), pltpu.VMEM((bn, d), BF16), pltpu.VMEM((rows, bn), F32), pltpu.VMEM((rows, d), BF16)],
        compiler_params=pltpu.CompilerParams(vmem_limit_bytes=VMEM_LIMIT),
        cost_estimate=pl.CostEstimate(flops=8 * rows * d * d, bytes_accessed=rows * d * 24, transcendentals=0),
        name='back_a',
    )(lam, own, other, n3, i3, w3, n2, i2, g2, b2, act2)


def back_c_kernel(nb, rows, x_ref, feat_ref, w2_ref, n1_ref, i1_ref, g1_ref, b1_ref, p_ref, q_ref,
                  sum_ref, dw1_ref, dg_ref, db_ref, acc, dpre, featt):
    j = pl.program_id(0)

    def fin():
        def put(r, v):
            dpre[r:r + CHUNK, :] = v

        db_ref[...], dg_ref[...] = finish_back(rows, acc, n1_ref, i1_ref[...], g1_ref[...], b1_ref[...], put)

    def mm():
        for r in range(0, rows, TILE):
            acc[r:r + TILE, :] = dot(x_ref[r:r + TILE, :], w2_ref[...], ((1,), (1,)))
        for r in range(0, p_ref.shape[0], CHUNK // 2):
            sum_ref[r:r + CHUNK // 2, :] = p_ref[r:r + CHUNK // 2, :] + q_ref[r:r + CHUNK // 2, :]

    def dw():
        dw1_ref[...] = dot(featt[...], dpre[...])

    @pl.when(j == 0)
    def _():
        for r in range(0, rows, TILE):
            featt[:, r:r + TILE] = feat_ref[r:r + TILE, :].T

    @pl.when(j < nb)
    def _():
        fin()
        mm()
        dw()

    @pl.when(j == nb)
    def _():
        fin()
        dw()


def back_c(x, feat, w2, n1, i1, g1, b1, p, q, bn=256):
    rows, d = x.shape
    k = feat.shape[1]
    nb = d // bn

    def at(first):
        return lambda j: (0, jnp.clip(j - first, 0, nb - 1))

    col = pl.BlockSpec((1, bn), at(1))
    row = pl.BlockSpec((bn, d), lambda j: (jnp.minimum(j, nb - 1), 0))
    vec = jax.ShapeDtypeStruct((1, d), F32)
    return pl.pallas_call(
        functools.partial(back_c_kernel, nb, rows),
        grid=(nb + 1,),
        in_specs=[pl.BlockSpec((rows, d), lambda j: (0, 0), pipeline_mode=ONCE), pl.BlockSpec((rows, k), lambda j: (0, 0), pipeline_mode=ONCE),
                  row, pl.BlockSpec((rows, bn), at(1)), col, col, col, row, row],
        out_specs=[row, pl.BlockSpec((k, bn), at(1)), col, col],
        out_shape=[jax.ShapeDtypeStruct((d, d), F32), jax.ShapeDtypeStruct((k, d), F32), vec, vec],
        scratch_shapes=[pltpu.VMEM((rows, bn), F32), pltpu.VMEM((rows, bn), BF16), pltpu.VMEM((k, rows), BF16)],
        compiler_params=pltpu.CompilerParams(vmem_limit_bytes=VMEM_LIMIT),
        cost_estimate=pl.CostEstimate(flops=2 * rows * d * (k + d), bytes_accessed=rows * d * 20, transcendentals=0),
        name='back_c',
    )(x, feat, w2, n1, i1, g1, b1, p, q)


def dw_kernel(tile, x_ref, y_ref, out_ref):
    x = x_ref[...]
    for c in range(0, y_ref.shape[1], tile):
        out_ref[:, c:c + tile] = dot(x, y_ref[:, c:c + tile], ((0,), (0,)))


def weight_grad(x, y, bm=256, tile=512):
    rows, k = x.shape
    d = y.shape[1]
    return pl.pallas_call(
        functools.partial(dw_kernel, tile),
        grid=(k // bm,),
        in_specs=[pl.BlockSpec((rows, bm), lambda j: (0, j)), pl.BlockSpec((rows, d), lambda j: (0, 0), pipeline_mode=ONCE)],
        out_specs=pl.BlockSpec((bm, d), lambda j: (j, 0)),
        out_shape=jax.ShapeDtypeStruct((k, d), F32),
        compiler_params=pltpu.CompilerParams(vmem_limit_bytes=VMEM_LIMIT),
        cost_estimate=pl.CostEstimate(flops=2 * rows * k * d, bytes_accessed=k * d * 4 + rows * (k + d) * 2, transcendentals=0),
        name='weight_grad',
    )(x, y)


def solution(mesh):
    n = mesh.shape[AXIS]
    pair = [(i, i + 1 - 2 * (i % 2)) for i in range(n)]

    def swap(x):
        return lax.ppermute(x, AXIS, pair)

    def local_step(feat_a, feat_b, w_one, w_two, w_three, g_one, b_one, g_two, b_two, lam_off):
        width = w_two.shape[0]
        g1, b1, g2, b2 = (v.reshape(1, width) for v in (g_one, b_one, g_two, b_two))
        norm1, norm2, norm3, inv1, inv2, inv3, x, act1, act2, emb, other = forward(
            feat_a, feat_b, w_one, w_two, w_three, g1, b1, g2, b2, n)
        loss, dw3, d_pre2, dg2, db2 = back_a(lam_off.reshape(1, 1), emb, other, norm3, inv3, w_three, norm2, inv2, g2, b2, act2)
        dw3_other = swap(dw3)
        dw2 = weight_grad(act1, d_pre2)
        dw2_other = swap(dw2)
        dw3, dw1, dg1, db1 = back_c(d_pre2, x, w_two, norm1, inv1, g1, b1, dw3, dw3_other)
        dw1_other = swap(dw1)
        small = jnp.concatenate([dg1, db1, dg2, db2, loss], axis=1)
        small = small + swap(small)
        dg1, db1, dg2, db2 = (small[0, i * width:(i + 1) * width] for i in range(4))
        loss_val = jnp.sum(small[0, 4 * width:]) * 0.5
        return (loss_val, dw1 + dw1_other, dw2 + dw2_other, dw3, dg1, db1, dg2, db2)

    row_spec = P(AXIS, None)
    return jax.shard_map(local_step, mesh=mesh, in_specs=(row_spec, row_spec) + (P(),) * 8, out_specs=(P(),) * 8, check_vma=False)
```

```python
import functools

import jax
import jax.numpy as jnp
from jax import lax
from jax.experimental import pallas as pl
from jax.experimental.pallas import tpu as pltpu
from jax.sharding import PartitionSpec as P

NORM_EPS = 1e-5
AXIS = 'data'
MESH = pl.DeviceIdType.MESH
F32 = jnp.float32
BF16 = jnp.bfloat16
ONCE = pl.Buffered(1)
VMEM_LIMIT = 60 * 1024 * 1024
TILE = 256
CHUNK = 64


def fold(v):
    return jnp.sum(v.reshape(v.shape[0] // 8, 8, v.shape[1]), axis=0)


def dot(a, b, dims=((1,), (0,))):
    return lax.dot_general(a, b, (dims, ((), ())), preferred_element_type=F32)


def forward_kernel(nb, rows, fa_ref, fb_ref, w1_ref, w2_ref, w3_ref, g1_ref, b1_ref, g2_ref, b2_ref,
                   n1_ref, n2_ref, n3_ref, i1_ref, i2_ref, i3_ref, t1_ref, t2_ref, xt_ref, emb_hbm, other_hbm,
                   xs, bufa, bufb, acc, copy_sem, feat_sem, send_sem, recv_sem, esend_sem, erecv_sem):
    j = pl.program_id(0)
    me = lax.axis_index(AXIS)
    core = lax.rem(me, 2)
    chip = me // 2
    x_pos, y_pos = lax.rem(chip, 2), chip // 2
    partner = me + 1 - 2 * core
    x_chip, y_chip = chip + 1 - 2 * x_pos, chip + 2 - 4 * y_pos
    piece = fa_ref.shape[0]
    bn = acc.shape[1]

    def remote(src, dst, send, recv, dev):
        return pltpu.make_async_remote_copy(src_ref=src, dst_ref=dst, send_sem=send, recv_sem=recv, device_id=(dev,), device_id_type=MESH)

    def part(dev):
        return xs.at[pl.ds(pl.multiple_of(dev * piece, piece), piece), :]

    def gather():
        barrier = pltpu.get_barrier_semaphore()
        for dev in (partner, 2 * x_chip, 2 * x_chip + 1, 2 * y_chip, 2 * y_chip + 1):
            pl.semaphore_signal(barrier, inc=1, device_id=(dev,), device_id_type=MESH)
        pl.semaphore_wait(barrier, 5)

        def sends(mine, mine_src, theirs_src):
            for view, src in ((mine, mine_src), (1 - mine, theirs_src)):
                remote(src, part(me), send_sem.at[1 + view], recv_sem.at[1 + mine], 2 * x_chip + view).start()
                remote(src, part(me), send_sem.at[3 + view], recv_sem.at[3 + mine], 2 * y_chip + view).start()
            remote(theirs_src, part(me), send_sem.at[0], recv_sem.at[0], partner).start()
            pltpu.make_async_copy(mine_src, part(me), feat_sem).start()

        pl.when(core == 0)(lambda: sends(0, fa_ref, fb_ref))
        pl.when(core == 1)(lambda: sends(1, fb_ref, fa_ref))
        remote(fa_ref, part(2 * x_chip), send_sem.at[1], recv_sem.at[1], me).wait_recv()
        relay_y = remote(part(2 * x_chip), part(2 * x_chip), send_sem.at[5], recv_sem.at[5], 2 * y_chip + core)
        relay_y.start()
        remote(fa_ref, part(2 * y_chip + 1), send_sem.at[4], recv_sem.at[4], me).wait_recv()
        relay_x = remote(part(2 * y_chip + 1), part(2 * y_chip + 1), send_sem.at[6], recv_sem.at[6], 2 * x_chip + core)
        relay_x.start()
        pltpu.make_async_copy(fa_ref, part(me), feat_sem).wait()
        remote(fa_ref, part(me), send_sem.at[0], recv_sem.at[0], me).wait()
        remote(fa_ref, part(me), send_sem.at[1], recv_sem.at[2], me).wait()
        remote(fa_ref, part(me), send_sem.at[2], recv_sem.at[3], me).wait()
        remote(fa_ref, part(me), send_sem.at[3], recv_sem.at[5], me).wait()
        remote(fa_ref, part(me), send_sem.at[4], recv_sem.at[6], me).wait()
        relay_y.wait_send()
        relay_x.wait_send()

    def fin(layer):
        norm_ref, inv_ref = ((n1_ref, i1_ref), (n2_ref, i2_ref), (n3_ref, i3_ref))[layer]
        buf = (bufa, bufb, bufa)[layer]
        base = pl.multiple_of(jnp.maximum(j - 1 - layer * nb, 0) * bn, bn)
        total = jnp.zeros((8, bn), F32)
        square = jnp.zeros((8, bn), F32)
        for r in range(0, rows, CHUNK):
            pre = acc[r:r + CHUNK, :]
            total += fold(pre)
            square += fold(pre * pre)
        mean = jnp.sum(total, axis=0, keepdims=True) / rows
        inv = lax.rsqrt(jnp.sum(square, axis=0, keepdims=True) / rows - mean * mean + NORM_EPS)
        inv_ref[...] = inv
        if layer < 2:
            g_ref, b_ref = ((g1_ref, b1_ref), (g2_ref, b2_ref))[layer]
            g, b = g_ref[...], b_ref[...]
        for r in range(0, rows, CHUNK):
            norm = (acc[r:r + CHUNK, :] - mean) * inv
            norm_ref[r:r + CHUNK, :] = norm
            if layer < 2:
                norm = jnp.maximum(norm * g + b, 0.0)
            buf[r:r + CHUNK, pl.ds(base, bn)] = norm.astype(BF16)
        if layer < 2:
            t_ref = (t1_ref, t2_ref)[layer]
            for r in range(0, rows, TILE):
                t_ref[:, r:r + TILE] = buf[r:r + TILE, pl.ds(base, bn)].T

    def mm(layer):
        x_ref, w_ref = ((xs, w1_ref), (bufa, w2_ref), (bufb, w3_ref))[layer]
        for r in range(0, rows, TILE):
            acc[r:r + TILE, :] = dot(x_ref[r:r + TILE, :], w_ref[...])

    def out_copy(block):
        cols = pl.ds(pl.multiple_of(block * bn, bn), bn)
        return pltpu.make_async_copy(bufa.at[:, cols], emb_hbm.at[:, cols], copy_sem.at[block])

    def emb_copy(block):
        cols = pl.ds(pl.multiple_of(block * bn, bn), bn)
        return remote(bufa.at[:, cols], other_hbm.at[:, cols], esend_sem.at[block], erecv_sem.at[block], partner)

    @pl.when(j == 0)
    def _():
        gather()

    for layer in range(3):
        @pl.when((j >= layer * nb) & (j < (layer + 1) * nb))
        def _(layer=layer):
            fin(layer)
            mm(layer)

        @pl.when(j == (layer + 1) * nb)
        def _(layer=layer):
            fin(layer)

    @pl.when(j >= 2 * nb + 2)
    def _():
        block = j - 2 - 2 * nb
        out_copy(block).start()
        emb_copy(block).start()

    @pl.when(j == 3 * nb + 1)
    def _():
        for r in range(0, rows, TILE):
            xt_ref[:, r:r + TILE] = xs[r:r + TILE, :].T
        for block in range(nb):
            out_copy(block).wait()
            emb_copy(block).wait()


def forward(fa, fb, w1, w2, w3, g1, b1, g2, b2, n, bn=256):
    piece, k = fa.shape
    rows, d = piece * n, w2.shape[1]
    nb = d // bn

    def at(layer, delay):
        return lambda j: (0, jnp.clip(j - layer * nb - delay, 0, nb - 1))

    whole = pl.BlockSpec((piece, k), lambda j: (0, 0), pipeline_mode=ONCE)
    any_spec = pl.BlockSpec(memory_space=pl.ANY)
    col = [pl.BlockSpec((1, bn), at(layer, 1)) for layer in range(3)]
    norm = [pl.BlockSpec((rows, bn), at(layer, 1)) for layer in range(3)]
    big = jax.ShapeDtypeStruct((rows, d), BF16)
    return pl.pallas_call(
        functools.partial(forward_kernel, nb, rows),
        grid=(3 * nb + 2,),
        in_specs=[whole, whole, pl.BlockSpec((k, bn), at(0, 0)), pl.BlockSpec((d, bn), at(1, 0)), pl.BlockSpec((d, bn), at(2, 0)),
                  col[0], col[0], col[1], col[1]],
        out_specs=norm + col + [pl.BlockSpec((bn, rows), lambda j, f=at(layer, 1): f(j)[::-1]) for layer in range(2)]
        + [pl.BlockSpec((k, rows), lambda j: (0, 0), pipeline_mode=ONCE)] + [any_spec] * 2,
        out_shape=[jax.ShapeDtypeStruct((rows, d), F32)] * 3 + [jax.ShapeDtypeStruct((1, d), F32)] * 3
        + [jax.ShapeDtypeStruct((d, rows), BF16)] * 2 + [jax.ShapeDtypeStruct((k, rows), BF16)] + [big] * 2,
        scratch_shapes=[pltpu.VMEM((rows, k), BF16), pltpu.VMEM((rows, d), BF16), pltpu.VMEM((rows, d), BF16), pltpu.VMEM((rows, bn), F32),
                        pltpu.SemaphoreType.DMA((nb,)), pltpu.SemaphoreType.DMA, pltpu.SemaphoreType.DMA((7,)), pltpu.SemaphoreType.DMA((7,)),
                        pltpu.SemaphoreType.DMA((nb,)), pltpu.SemaphoreType.DMA((nb,))],
        compiler_params=pltpu.CompilerParams(collective_id=0, has_side_effects=True, vmem_limit_bytes=VMEM_LIMIT),
        cost_estimate=pl.CostEstimate(flops=2 * rows * d * (k + 2 * d), bytes_accessed=rows * d * 20, transcendentals=0),
        name='forward',
    )(fa, fb, w1, w2, w3, g1, b1, g2, b2)


def finish_back(rows, acc, norm_ref, inv, g, b, put):
    bn = acc.shape[1]
    total = jnp.zeros((8, bn), F32)
    cross = jnp.zeros((8, bn), F32)
    for r in range(0, rows, CHUNK):
        part = acc[r:r + CHUNK, :]
        norm = norm_ref[r:r + CHUNK, :]
        if b is not None:
            part = jnp.where(norm * g + b > 0.0, part, 0.0)
            acc[r:r + CHUNK, :] = part
        total += fold(part)
        cross += fold(part * norm)
    total = jnp.sum(total, axis=0, keepdims=True)
    cross = jnp.sum(cross, axis=0, keepdims=True)
    scale = inv if g is None else inv * g
    shift, slope = scale * (total / rows), scale * (cross / rows)
    for r in range(0, rows, CHUNK):
        put(r, (acc[r:r + CHUNK, :] * scale - shift - norm_ref[r:r + CHUNK, :] * slope).astype(BF16))
    return total, cross


def back_ab_kernel(nb, rows, lam_ref, own_ref, other_hbm, n3_ref, i3_ref, w3_ref, n2_ref, i2_ref, g2_ref, b2_ref, t2_ref, t1_hbm,
                   loss_ref, dpre_ref, dg_ref, db_ref, dw3_hbm, dw2_hbm,
                   big, corr, grad, acc, dout, send3, recv3, send2, recv2, load_sem, ssem, rsem, osem, free3, free2):
    j = pl.program_id(0)
    me = lax.axis_index(AXIS)
    partner = me + 1 - 2 * lax.rem(me, 2)
    bn = acc.shape[1]
    d = big.shape[1]
    lam = lam_ref[0, 0]
    other_ref = big

    def pair(e):
        return ((send3, recv3, free3, nb), (send2, recv2, free2, nb + 1))[e]

    def swap_copy(e, b):
        send, recv, _, _ = pair(e)
        return pltpu.make_async_remote_copy(
            src_ref=send.at[lax.rem(b, 2)], dst_ref=recv.at[lax.rem(b, 3)], send_sem=ssem.at[e, lax.rem(b, 2)],
            recv_sem=rsem.at[e, lax.rem(b, 3)], device_id=(partner,), device_id_type=MESH)

    def sum_copy(e, b):
        span = pl.ds(pl.multiple_of(b * bn, bn), bn)
        dst = dw3_hbm.at[span, :] if e == 0 else dw2_hbm.at[:, span]
        return pltpu.make_async_copy(pair(e)[1].at[lax.rem(b, 3)], dst, osem.at[e, lax.rem(b, 3)])

    def exchange(e):
        send, recv, free, first = pair(e)

        @pl.when((j >= first + 3) & (j < first + 3 + nb))
        def _():
            b = j - first - 3
            sum_copy(e, b).wait()

            @pl.when(b < nb - 3)
            def _():
                pl.semaphore_signal(free, inc=1, device_id=(partner,), device_id_type=MESH)

        @pl.when((j >= first + 2) & (j < first + 2 + nb))
        def _():
            b = j - first - 2
            swap_copy(e, b).wait()
            mine, theirs = lax.rem(b, 2), lax.rem(b, 3)
            for r in range(0, send.shape[1], send.shape[1] // 32):
                part = pl.ds(r, send.shape[1] // 32)
                recv[theirs, part, :] = recv[theirs, part, :] + send[mine, part, :]
            sum_copy(e, b).start()

        @pl.when((j >= first + 1) & (j < first + 1 + nb))
        def _():
            b = j - first - 1

            @pl.when(b >= 3)
            def _():
                pl.semaphore_wait(free, 1)

            swap_copy(e, b).start()

    def fin_loss():
        base = pl.multiple_of(jnp.maximum(j - 1, 0) * bn, bn)

        def put(r, v):
            dout[r:r + CHUNK, pl.ds(base, bn)] = v

        finish_back(rows, acc, n3_ref, i3_ref[...], None, None, put)

    def mm_loss():
        own = own_ref[...]
        loss = jnp.zeros((8, bn), F32)
        for c in range(0, d, bn):
            part = dot(own, other_ref[:, c:c + bn], ((0,), (0,))) * (1.0 / rows)
            corr[:, c:c + bn] = part
            loss += fold(part * part)
            grad[:, c:c + bn] = ((2.0 * lam) * part).astype(BF16)
        here = pl.ds(pl.multiple_of(j * bn, bn), bn)
        part = corr[:, here]
        diag = lax.broadcasted_iota(jnp.int32, (bn, bn), 0) == lax.broadcasted_iota(jnp.int32, (bn, bn), 1)
        grad[:, here] = jnp.where(diag, -2.0 * (1.0 - part), (2.0 * lam) * part).astype(BF16)
        loss = lam * loss + fold(jnp.where(diag, (1.0 - part) * (1.0 - part) - lam * (part * part), 0.0))
        loss_ref[...] += jnp.sum(loss, axis=0, keepdims=True)
        for r in range(0, rows, TILE):
            acc[r:r + TILE, :] = dot(other_ref[r:r + TILE, :], grad[...], ((1,), (1,))) * (1.0 / rows)

    def fin_two():
        def put(r, v):
            dpre_ref[r:r + CHUNK, :] = v

        db_ref[...], dg_ref[...] = finish_back(rows, acc, n2_ref, i2_ref[...], g2_ref[...], b2_ref[...], put)

    def mm_two():
        for r in range(0, rows, TILE):
            acc[r:r + TILE, :] = dot(dout[r:r + TILE, :], w3_ref[...], ((1,), (1,)))
        act = t2_ref[...]
        slot = lax.rem(j - nb, 2)
        for c in range(0, d, 2 * bn):
            send3[slot, :, c:c + 2 * bn] = dot(act, dout[:, c:c + 2 * bn])

    def mm_dw2():
        slot = lax.rem(j - nb - 1, 2)
        for r in range(0, d, TILE):
            send2[slot, r:r + TILE, :] = dot(big[r:r + TILE, :], dpre_ref[...])

    @pl.when(j == 0)
    def _():
        load = pltpu.make_async_copy(other_hbm, big, load_sem)
        load.start()
        loss_ref[...] = jnp.zeros_like(loss_ref)
        barrier = pltpu.get_barrier_semaphore()
        pl.semaphore_signal(barrier, inc=1, device_id=(partner,), device_id_type=MESH)
        pl.semaphore_wait(barrier, 1)
        load.wait()

    @pl.when(j == nb)
    def _():
        pltpu.make_async_copy(t1_hbm, big, load_sem).start()

    exchange(0)
    exchange(1)

    @pl.when(j < nb)
    def _():
        fin_loss()
        mm_loss()

    @pl.when(j == nb)
    def _():
        fin_loss()

    @pl.when((j >= nb) & (j < 2 * nb))
    def _():
        fin_two()
        mm_two()

    @pl.when(j == 2 * nb)
    def _():
        fin_two()

    @pl.when(j == nb + 1)
    def _():
        pltpu.make_async_copy(t1_hbm, big, load_sem).wait()

    @pl.when((j > nb) & (j <= 2 * nb))
    def _():
        mm_dw2()


def back_ab(lam, own, other, n3, i3, w3, n2, i2, g2, b2, t2, t1, bn=256):
    rows, d = own.shape
    nb = d // bn

    def at(first):
        return lambda j: (0, jnp.clip(j - first, 0, nb - 1))

    def block(first):
        return pl.BlockSpec((rows, bn), at(first))

    def col(first):
        return pl.BlockSpec((1, bn), at(first))

    row = pl.BlockSpec((bn, d), lambda j: (jnp.clip(j - nb, 0, nb - 1), 0))
    vec = jax.ShapeDtypeStruct((1, d), F32)
    any_spec = pl.BlockSpec(memory_space=pl.ANY)
    return pl.pallas_call(
        functools.partial(back_ab_kernel, nb, rows),
        grid=(2 * nb + 4,),
        in_specs=[pl.BlockSpec(memory_space=pltpu.SMEM), block(0), any_spec,
                  block(1), col(1), row, block(nb + 1), col(nb + 1), col(nb + 1), col(nb + 1), row, any_spec],
        out_specs=[pl.BlockSpec((1, bn), lambda j: (0, 0)), block(nb + 1), col(nb + 1), col(nb + 1), any_spec, any_spec],
        out_shape=[jax.ShapeDtypeStruct((1, bn), F32), jax.ShapeDtypeStruct((rows, d), BF16), vec, vec]
        + [jax.ShapeDtypeStruct((d, d), F32)] * 2,
        scratch_shapes=[pltpu.VMEM((rows, d), BF16), pltpu.VMEM((bn, d), F32), pltpu.VMEM((bn, d), BF16), pltpu.VMEM((rows, bn), F32),
                        pltpu.VMEM((rows, d), BF16), pltpu.VMEM((2, bn, d), F32), pltpu.VMEM((3, bn, d), F32),
                        pltpu.VMEM((2, d, bn), F32), pltpu.VMEM((3, d, bn), F32), pltpu.SemaphoreType.DMA,
                        pltpu.SemaphoreType.DMA((2, 2)), pltpu.SemaphoreType.DMA((2, 3)), pltpu.SemaphoreType.DMA((2, 3)),
                        pltpu.SemaphoreType.REGULAR, pltpu.SemaphoreType.REGULAR],
        compiler_params=pltpu.CompilerParams(collective_id=1, has_side_effects=True, vmem_limit_bytes=63 * 1024 * 1024),
        cost_estimate=pl.CostEstimate(flops=10 * rows * d * d, bytes_accessed=rows * d * 24, transcendentals=0),
        name='back_ab',
    )(lam, own, other, n3, i3, w3, n2, i2, g2, b2, t2, t1)


def back_c_kernel(nb, rows, x_ref, featt, w2_ref, n1_ref, i1_ref, g1_ref, b1_ref, p_ref, q_ref,
                  p_out, q_out, dw1_ref, dg_ref, db_ref, acc, dpre):
    j = pl.program_id(0)

    def fin():
        def put(r, v):
            dpre[r:r + CHUNK, :] = v

        db_ref[...], dg_ref[...] = finish_back(rows, acc, n1_ref, i1_ref[...], g1_ref[...], b1_ref[...], put)

    def mm():
        for r in range(0, rows, TILE):
            acc[r:r + TILE, :] = dot(x_ref[r:r + TILE, :], w2_ref[...], ((1,), (1,)))
        for r in range(0, p_ref.shape[0], CHUNK // 2):
            p_out[r:r + CHUNK // 2, :] = p_ref[r:r + CHUNK // 2, :]
            q_out[r:r + CHUNK // 2, :] = q_ref[r:r + CHUNK // 2, :]

    def dw():
        dw1_ref[...] = dot(featt[...], dpre[...])

    @pl.when(j < nb)
    def _():
        fin()
        mm()
        dw()

    @pl.when(j == nb)
    def _():
        fin()
        dw()


def back_c(x, featt, w2, n1, i1, g1, b1, p, q, bn=256):
    rows, d = x.shape
    k = featt.shape[0]
    nb = d // bn

    def at(first):
        return lambda j: (0, jnp.clip(j - first, 0, nb - 1))

    col = pl.BlockSpec((1, bn), at(1))
    row = pl.BlockSpec((bn, d), lambda j: (jnp.minimum(j, nb - 1), 0))
    vec = jax.ShapeDtypeStruct((1, d), F32)
    return pl.pallas_call(
        functools.partial(back_c_kernel, nb, rows),
        grid=(nb + 1,),
        in_specs=[pl.BlockSpec((rows, d), lambda j: (0, 0), pipeline_mode=ONCE), pl.BlockSpec((k, rows), lambda j: (0, 0), pipeline_mode=ONCE),
                  row, pl.BlockSpec((rows, bn), at(1)), col, col, col, row, row],
        out_specs=[row, row, pl.BlockSpec((k, bn), at(1)), col, col],
        out_shape=[jax.ShapeDtypeStruct((d, d), F32)] * 2 + [jax.ShapeDtypeStruct((k, d), F32), vec, vec],
        scratch_shapes=[pltpu.VMEM((rows, bn), F32), pltpu.VMEM((rows, bn), BF16)],
        compiler_params=pltpu.CompilerParams(vmem_limit_bytes=VMEM_LIMIT),
        cost_estimate=pl.CostEstimate(flops=2 * rows * d * (k + d), bytes_accessed=rows * d * 20, transcendentals=0),
        name='back_c',
    )(x, featt, w2, n1, i1, g1, b1, p, q)


def solution(mesh):
    n = mesh.shape[AXIS]
    pair = [(i, i + 1 - 2 * (i % 2)) for i in range(n)]

    def swap(x):
        return lax.ppermute(x, AXIS, pair)

    def local_step(feat_a, feat_b, w_one, w_two, w_three, g_one, b_one, g_two, b_two, lam_off):
        width = w_two.shape[0]
        g1, b1, g2, b2 = (v.reshape(1, width) for v in (g_one, b_one, g_two, b_two))
        norm1, norm2, norm3, inv1, inv2, inv3, act1t, act2t, xt, emb, other = forward(
            feat_a, feat_b, w_one, w_two, w_three, g1, b1, g2, b2, n)
        loss, d_pre2, dg2, db2, dw3, dw2 = back_ab(
            lam_off.reshape(1, 1), emb, other, norm3, inv3, w_three, norm2, inv2, g2, b2, act2t, act1t)
        dw3, dw2, dw1, dg1, db1 = back_c(d_pre2, xt, w_two, norm1, inv1, g1, b1, dw3, dw2)
        dw1_other = swap(dw1)
        small = jnp.concatenate([dg1, db1, dg2, db2, loss], axis=1)
        small = small + swap(small)
        dg1, db1, dg2, db2 = (small[0, i * width:(i + 1) * width] for i in range(4))
        loss_val = jnp.sum(small[0, 4 * width:]) * 0.5
        return (loss_val, dw1 + dw1_other, dw2, dw3, dg1, db1, dg2, db2)

    row_spec = P(AXIS, None)
    return jax.shard_map(local_step, mesh=mesh, in_specs=(row_spec, row_spec) + (P(),) * 8, out_specs=(P(),) * 8, check_vma=False)
```

```python
import functools

import jax
import jax.numpy as jnp
from jax import lax
from jax.experimental import pallas as pl
from jax.experimental.pallas import tpu as pltpu
from jax.sharding import PartitionSpec as P

NORM_EPS = 1e-5
AXIS = 'data'
MESH = pl.DeviceIdType.MESH
F32 = jnp.float32
BF16 = jnp.bfloat16
ONCE = pl.Buffered(1)
VMEM_LIMIT = 60 * 1024 * 1024
TILE = 256
CHUNK = 64


def fold(v):
    return jnp.sum(v.reshape(v.shape[0] // 8, 8, v.shape[1]), axis=0)


def dot(a, b, dims=((1,), (0,))):
    return lax.dot_general(a, b, (dims, ((), ())), preferred_element_type=F32)


def forward_kernel(nb, rows, fa_ref, fb_ref, w1_ref, w2_ref, w3_ref, g1_ref, b1_ref, g2_ref, b2_ref,
                   n1_ref, n2_ref, n3_ref, i1_ref, i2_ref, i3_ref, t1_ref, t2_ref, xt_ref, emb_hbm, other_hbm,
                   xs, bufa, bufb, acc, copy_sem, feat_sem, send_sem, recv_sem, esend_sem, erecv_sem):
    j = pl.program_id(0)
    me = lax.axis_index(AXIS)
    core = lax.rem(me, 2)
    chip = me // 2
    x_pos, y_pos = lax.rem(chip, 2), chip // 2
    partner = me + 1 - 2 * core
    x_chip, y_chip = chip + 1 - 2 * x_pos, chip + 2 - 4 * y_pos
    piece = fa_ref.shape[0]
    bn = acc.shape[1]

    def remote(src, dst, send, recv, dev):
        return pltpu.make_async_remote_copy(src_ref=src, dst_ref=dst, send_sem=send, recv_sem=recv, device_id=(dev,), device_id_type=MESH)

    def part(dev):
        return xs.at[pl.ds(pl.multiple_of(dev * piece, piece), piece), :]

    def gather():
        barrier = pltpu.get_barrier_semaphore()
        for dev in (partner, 2 * x_chip, 2 * x_chip + 1, 2 * y_chip, 2 * y_chip + 1):
            pl.semaphore_signal(barrier, inc=1, device_id=(dev,), device_id_type=MESH)
        pl.semaphore_wait(barrier, 5)

        def sends(mine, mine_src, theirs_src):
            for view, src in ((mine, mine_src), (1 - mine, theirs_src)):
                remote(src, part(me), send_sem.at[1 + view], recv_sem.at[1 + mine], 2 * x_chip + view).start()
                remote(src, part(me), send_sem.at[3 + view], recv_sem.at[3 + mine], 2 * y_chip + view).start()
            remote(theirs_src, part(me), send_sem.at[0], recv_sem.at[0], partner).start()
            pltpu.make_async_copy(mine_src, part(me), feat_sem).start()

        pl.when(core == 0)(lambda: sends(0, fa_ref, fb_ref))
        pl.when(core == 1)(lambda: sends(1, fb_ref, fa_ref))
        remote(fa_ref, part(2 * x_chip), send_sem.at[1], recv_sem.at[1], me).wait_recv()
        relay_y = remote(part(2 * x_chip), part(2 * x_chip), send_sem.at[5], recv_sem.at[5], 2 * y_chip + core)
        relay_y.start()
        remote(fa_ref, part(2 * y_chip + 1), send_sem.at[4], recv_sem.at[4], me).wait_recv()
        relay_x = remote(part(2 * y_chip + 1), part(2 * y_chip + 1), send_sem.at[6], recv_sem.at[6], 2 * x_chip + core)
        relay_x.start()
        pltpu.make_async_copy(fa_ref, part(me), feat_sem).wait()
        remote(fa_ref, part(me), send_sem.at[0], recv_sem.at[0], me).wait()
        remote(fa_ref, part(me), send_sem.at[1], recv_sem.at[2], me).wait()
        remote(fa_ref, part(me), send_sem.at[2], recv_sem.at[3], me).wait()
        remote(fa_ref, part(me), send_sem.at[3], recv_sem.at[5], me).wait()
        remote(fa_ref, part(me), send_sem.at[4], recv_sem.at[6], me).wait()
        relay_y.wait_send()
        relay_x.wait_send()

    def fin(layer):
        norm_ref, inv_ref = ((n1_ref, i1_ref), (n2_ref, i2_ref), (n3_ref, i3_ref))[layer]
        buf = (bufa, bufb, bufa)[layer]
        base = pl.multiple_of(jnp.maximum(j - 1 - layer * nb, 0) * bn, bn)
        total = jnp.zeros((8, bn), F32)
        square = jnp.zeros((8, bn), F32)
        for r in range(0, rows, CHUNK):
            pre = acc[r:r + CHUNK, :]
            total += fold(pre)
            square += fold(pre * pre)
        mean = jnp.sum(total, axis=0, keepdims=True) / rows
        inv = lax.rsqrt(jnp.sum(square, axis=0, keepdims=True) / rows - mean * mean + NORM_EPS)
        inv_ref[...] = inv
        if layer < 2:
            g_ref, b_ref = ((g1_ref, b1_ref), (g2_ref, b2_ref))[layer]
            g, b = g_ref[...], b_ref[...]
        for r in range(0, rows, CHUNK):
            norm = (acc[r:r + CHUNK, :] - mean) * inv
            norm_ref[r:r + CHUNK, :] = norm
            if layer < 2:
                norm = jnp.maximum(norm * g + b, 0.0)
            buf[r:r + CHUNK, pl.ds(base, bn)] = norm.astype(BF16)
        if layer < 2:
            t_ref = (t1_ref, t2_ref)[layer]
            for r in range(0, rows, TILE):
                t_ref[:, r:r + TILE] = buf[r:r + TILE, pl.ds(base, bn)].T

    def mm(layer):
        x_ref, w_ref = ((xs, w1_ref), (bufa, w2_ref), (bufb, w3_ref))[layer]
        for r in range(0, rows, TILE):
            acc[r:r + TILE, :] = dot(x_ref[r:r + TILE, :], w_ref[...])

    def out_copy(block):
        cols = pl.ds(pl.multiple_of(block * bn, bn), bn)
        return pltpu.make_async_copy(bufa.at[:, cols], emb_hbm.at[:, cols], copy_sem.at[block])

    def emb_copy(block):
        cols = pl.ds(pl.multiple_of(block * bn, bn), bn)
        return remote(bufa.at[:, cols], other_hbm.at[:, cols], esend_sem.at[block], erecv_sem.at[block], partner)

    @pl.when(j == 0)
    def _():
        gather()

    for layer in range(3):
        @pl.when((j >= layer * nb) & (j < (layer + 1) * nb))
        def _(layer=layer):
            fin(layer)
            mm(layer)

        @pl.when(j == (layer + 1) * nb)
        def _(layer=layer):
            fin(layer)

    @pl.when(j >= 2 * nb + 2)
    def _():
        block = j - 2 - 2 * nb
        out_copy(block).start()
        emb_copy(block).start()

    @pl.when(j == 3 * nb + 1)
    def _():
        for r in range(0, rows, TILE):
            xt_ref[:, r:r + TILE] = xs[r:r + TILE, :].T
        for block in range(nb):
            out_copy(block).wait()
            emb_copy(block).wait()


def forward(fa, fb, w1, w2, w3, g1, b1, g2, b2, n, bn=256):
    piece, k = fa.shape
    rows, d = piece * n, w2.shape[1]
    nb = d // bn

    def at(layer, delay):
        return lambda j: (0, jnp.clip(j - layer * nb - delay, 0, nb - 1))

    whole = pl.BlockSpec((piece, k), lambda j: (0, 0), pipeline_mode=ONCE)
    any_spec = pl.BlockSpec(memory_space=pl.ANY)
    col = [pl.BlockSpec((1, bn), at(layer, 1)) for layer in range(3)]
    norm = [pl.BlockSpec((rows, bn), at(layer, 1)) for layer in range(3)]
    big = jax.ShapeDtypeStruct((rows, d), BF16)
    return pl.pallas_call(
        functools.partial(forward_kernel, nb, rows),
        grid=(3 * nb + 2,),
        in_specs=[whole, whole, pl.BlockSpec((k, bn), at(0, 0)), pl.BlockSpec((d, bn), at(1, 0)), pl.BlockSpec((d, bn), at(2, 0)),
                  col[0], col[0], col[1], col[1]],
        out_specs=norm + col + [pl.BlockSpec((bn, rows), lambda j, f=at(layer, 1): f(j)[::-1]) for layer in range(2)]
        + [pl.BlockSpec((k, rows), lambda j: (0, 0), pipeline_mode=ONCE)] + [any_spec] * 2,
        out_shape=[jax.ShapeDtypeStruct((rows, d), F32)] * 3 + [jax.ShapeDtypeStruct((1, d), F32)] * 3
        + [jax.ShapeDtypeStruct((d, rows), BF16)] * 2 + [jax.ShapeDtypeStruct((k, rows), BF16)] + [big] * 2,
        scratch_shapes=[pltpu.VMEM((rows, k), BF16), pltpu.VMEM((rows, d), BF16), pltpu.VMEM((rows, d), BF16), pltpu.VMEM((rows, bn), F32),
                        pltpu.SemaphoreType.DMA((nb,)), pltpu.SemaphoreType.DMA, pltpu.SemaphoreType.DMA((7,)), pltpu.SemaphoreType.DMA((7,)),
                        pltpu.SemaphoreType.DMA((nb,)), pltpu.SemaphoreType.DMA((nb,))],
        compiler_params=pltpu.CompilerParams(collective_id=0, has_side_effects=True, vmem_limit_bytes=VMEM_LIMIT),
        cost_estimate=pl.CostEstimate(flops=2 * rows * d * (k + 2 * d), bytes_accessed=rows * d * 20, transcendentals=0),
        name='forward',
    )(fa, fb, w1, w2, w3, g1, b1, g2, b2)


def finish_back(rows, acc, norm_ref, inv, g, b, put):
    bn = acc.shape[1]
    total = jnp.zeros((8, bn), F32)
    cross = jnp.zeros((8, bn), F32)
    for r in range(0, rows, CHUNK):
        part = acc[r:r + CHUNK, :]
        norm = norm_ref[r:r + CHUNK, :]
        if b is not None:
            part = jnp.where(norm * g + b > 0.0, part, 0.0)
            acc[r:r + CHUNK, :] = part
        total += fold(part)
        cross += fold(part * norm)
    total = jnp.sum(total, axis=0, keepdims=True)
    cross = jnp.sum(cross, axis=0, keepdims=True)
    scale = inv if g is None else inv * g
    shift, slope = scale * (total / rows), scale * (cross / rows)
    for r in range(0, rows, CHUNK):
        put(r, (acc[r:r + CHUNK, :] * scale - shift - norm_ref[r:r + CHUNK, :] * slope).astype(BF16))
    return total, cross


def back_ab_kernel(nb, rows, lam_ref, own_ref, other_hbm, n3_ref, i3_ref, w3_ref, n2_ref, i2_ref, g2_ref, b2_ref, t2_ref, t1_hbm,
                   loss_ref, dpre_ref, dg_ref, db_ref, dw3_hbm, dw2_hbm,
                   big, corr, grad, acc, dout, send3, recv3, send2, recv2, load_sem, ssem, rsem, osem, free3, free2):
    j = pl.program_id(0)
    me = lax.axis_index(AXIS)
    partner = me + 1 - 2 * lax.rem(me, 2)
    bn = acc.shape[1]
    d = big.shape[1]
    lam = lam_ref[0, 0]
    other_ref = big

    def pair(e):
        return ((send3, recv3, free3, nb), (send2, recv2, free2, nb + 1))[e]

    def swap_copy(e, b):
        send, recv, _, _ = pair(e)
        return pltpu.make_async_remote_copy(
            src_ref=send.at[lax.rem(b, 2)], dst_ref=recv.at[lax.rem(b, 3)], send_sem=ssem.at[e, lax.rem(b, 2)],
            recv_sem=rsem.at[e, lax.rem(b, 3)], device_id=(partner,), device_id_type=MESH)

    def sum_copy(e, b):
        span = pl.ds(pl.multiple_of(b * bn, bn), bn)
        dst = dw3_hbm.at[span, :] if e == 0 else dw2_hbm.at[:, span]
        return pltpu.make_async_copy(pair(e)[1].at[lax.rem(b, 3)], dst, osem.at[e, lax.rem(b, 3)])

    def exchange(e):
        send, recv, free, first = pair(e)

        @pl.when((j >= first + 3) & (j < first + 3 + nb))
        def _():
            b = j - first - 3
            sum_copy(e, b).wait()

            @pl.when(b < nb - 3)
            def _():
                pl.semaphore_signal(free, inc=1, device_id=(partner,), device_id_type=MESH)

        @pl.when((j >= first + 2) & (j < first + 2 + nb))
        def _():
            b = j - first - 2
            swap_copy(e, b).wait()
            mine, theirs = lax.rem(b, 2), lax.rem(b, 3)
            for r in range(0, send.shape[1], send.shape[1] // 32):
                part = pl.ds(r, send.shape[1] // 32)
                recv[theirs, part, :] = recv[theirs, part, :] + send[mine, part, :]
            sum_copy(e, b).start()

        @pl.when((j >= first + 1) & (j < first + 1 + nb))
        def _():
            b = j - first - 1

            @pl.when(b >= 3)
            def _():
                pl.semaphore_wait(free, 1)

            swap_copy(e, b).start()

    def fin_loss():
        base = pl.multiple_of(jnp.maximum(j - 1, 0) * bn, bn)

        def put(r, v):
            dout[r:r + CHUNK, pl.ds(base, bn)] = v

        finish_back(rows, acc, n3_ref, i3_ref[...], None, None, put)

    def mm_loss():
        own = own_ref[...]
        loss = jnp.zeros((8, bn), F32)
        for c in range(0, d, bn):
            part = dot(own, other_ref[:, c:c + bn], ((0,), (0,))) * (1.0 / rows)
            corr[:, c:c + bn] = part
            loss += fold(part * part)
            grad[:, c:c + bn] = ((2.0 * lam) * part).astype(BF16)
        here = pl.ds(pl.multiple_of(j * bn, bn), bn)
        part = corr[:, here]
        diag = lax.broadcasted_iota(jnp.int32, (bn, bn), 0) == lax.broadcasted_iota(jnp.int32, (bn, bn), 1)
        grad[:, here] = jnp.where(diag, -2.0 * (1.0 - part), (2.0 * lam) * part).astype(BF16)
        loss = lam * loss + fold(jnp.where(diag, (1.0 - part) * (1.0 - part) - lam * (part * part), 0.0))
        loss_ref[...] += jnp.sum(loss, axis=0, keepdims=True)
        for r in range(0, rows, TILE):
            acc[r:r + TILE, :] = dot(other_ref[r:r + TILE, :], grad[...], ((1,), (1,))) * (1.0 / rows)

    def fin_two():
        def put(r, v):
            dpre_ref[r:r + CHUNK, :] = v

        db_ref[...], dg_ref[...] = finish_back(rows, acc, n2_ref, i2_ref[...], g2_ref[...], b2_ref[...], put)

    def mm_two():
        for r in range(0, rows, TILE):
            acc[r:r + TILE, :] = dot(dout[r:r + TILE, :], w3_ref[...], ((1,), (1,)))
        act = t2_ref[...]
        slot = lax.rem(j - nb, 2)
        for c in range(0, d, 2 * bn):
            send3[slot, :, c:c + 2 * bn] = dot(act, dout[:, c:c + 2 * bn])

    def mm_dw2():
        slot = lax.rem(j - nb - 1, 2)
        for r in range(0, d, TILE):
            send2[slot, r:r + TILE, :] = dot(big[r:r + TILE, :], dpre_ref[...])

    @pl.when(j == 0)
    def _():
        load = pltpu.make_async_copy(other_hbm, big, load_sem)
        load.start()
        loss_ref[...] = jnp.zeros_like(loss_ref)
        barrier = pltpu.get_barrier_semaphore()
        pl.semaphore_signal(barrier, inc=1, device_id=(partner,), device_id_type=MESH)
        pl.semaphore_wait(barrier, 1)
        load.wait()

    @pl.when(j == nb)
    def _():
        pltpu.make_async_copy(t1_hbm, big, load_sem).start()

    exchange(0)
    exchange(1)

    @pl.when(j < nb)
    def _():
        fin_loss()
        mm_loss()

    @pl.when(j == nb)
    def _():
        fin_loss()

    @pl.when((j >= nb) & (j < 2 * nb))
    def _():
        fin_two()
        mm_two()

    @pl.when(j == 2 * nb)
    def _():
        fin_two()

    @pl.when(j == nb + 1)
    def _():
        pltpu.make_async_copy(t1_hbm, big, load_sem).wait()

    @pl.when((j > nb) & (j <= 2 * nb))
    def _():
        mm_dw2()


def back_ab(lam, own, other, n3, i3, w3, n2, i2, g2, b2, t2, t1, bn=256):
    rows, d = own.shape
    nb = d // bn

    def at(first):
        return lambda j: (0, jnp.clip(j - first, 0, nb - 1))

    def block(first):
        return pl.BlockSpec((rows, bn), at(first))

    def col(first):
        return pl.BlockSpec((1, bn), at(first))

    row = pl.BlockSpec((bn, d), lambda j: (jnp.clip(j - nb, 0, nb - 1), 0))
    vec = jax.ShapeDtypeStruct((1, d), F32)
    any_spec = pl.BlockSpec(memory_space=pl.ANY)
    return pl.pallas_call(
        functools.partial(back_ab_kernel, nb, rows),
        grid=(2 * nb + 4,),
        in_specs=[pl.BlockSpec(memory_space=pltpu.SMEM), block(0), any_spec,
                  block(1), col(1), row, block(nb + 1), col(nb + 1), col(nb + 1), col(nb + 1), row, any_spec],
        out_specs=[pl.BlockSpec((1, bn), lambda j: (0, 0)), block(nb + 1), col(nb + 1), col(nb + 1), any_spec, any_spec],
        out_shape=[jax.ShapeDtypeStruct((1, bn), F32), jax.ShapeDtypeStruct((rows, d), BF16), vec, vec]
        + [jax.ShapeDtypeStruct((d, d), F32)] * 2,
        scratch_shapes=[pltpu.VMEM((rows, d), BF16), pltpu.VMEM((bn, d), F32), pltpu.VMEM((bn, d), BF16), pltpu.VMEM((rows, bn), F32),
                        pltpu.VMEM((rows, d), BF16), pltpu.VMEM((2, bn, d), F32), pltpu.VMEM((3, bn, d), F32),
                        pltpu.VMEM((2, d, bn), F32), pltpu.VMEM((3, d, bn), F32), pltpu.SemaphoreType.DMA,
                        pltpu.SemaphoreType.DMA((2, 2)), pltpu.SemaphoreType.DMA((2, 3)), pltpu.SemaphoreType.DMA((2, 3)),
                        pltpu.SemaphoreType.REGULAR, pltpu.SemaphoreType.REGULAR],
        compiler_params=pltpu.CompilerParams(collective_id=1, has_side_effects=True, vmem_limit_bytes=63 * 1024 * 1024),
        cost_estimate=pl.CostEstimate(flops=10 * rows * d * d, bytes_accessed=rows * d * 24, transcendentals=0),
        name='back_ab',
    )(lam, own, other, n3, i3, w3, n2, i2, g2, b2, t2, t1)


def back_c_kernel(nb, rows, x_ref, featt, w2_ref, n1_ref, i1_ref, g1_ref, b1_ref, dg2_ref, db2_ref, loss_ref, p_ref, q_ref,
                  p_out, q_out, dw1_ref, small_ref, acc, dpre, ring, load_sem, store_sem):
    j = pl.program_id(0)
    bn = acc.shape[1]

    def moves(b):
        span = pl.ds(pl.multiple_of(b * bn, bn), bn)
        slot = lax.rem(b, 2)
        return [(pltpu.make_async_copy(src.at[span, :], ring.at[slot, i], load_sem.at[slot, i]),
                 pltpu.make_async_copy(ring.at[slot, i], dst.at[span, :], store_sem.at[slot, i]))
                for i, (src, dst) in enumerate(((p_ref, p_out), (q_ref, q_out)))]

    @pl.when(j >= 2)
    def _():
        for _, store in moves(j - 2):
            store.wait()

    @pl.when(j < nb)
    def _():
        for load, _ in moves(j):
            load.start()

    @pl.when((j >= 1) & (j <= nb))
    def _():
        for load, store in moves(j - 1):
            load.wait()
            store.start()

    def fin():
        def put(r, v):
            dpre[r:r + CHUNK, :] = v

        db, dg = finish_back(rows, acc, n1_ref, i1_ref[...], g1_ref[...], b1_ref[...], put)
        small_ref[0:1, :] = dg
        small_ref[1:2, :] = db
        small_ref[2:3, :] = dg2_ref[...]
        small_ref[3:4, :] = db2_ref[...]
        small_ref[4:5, :] = loss_ref[...]

    def mm():
        for r in range(0, rows, TILE):
            acc[r:r + TILE, :] = dot(x_ref[r:r + TILE, :], w2_ref[...], ((1,), (1,)))

    def dw():
        dw1_ref[...] = dot(featt[...], dpre[...])

    @pl.when(j < nb)
    def _():
        fin()
        mm()
        dw()

    @pl.when(j == nb)
    def _():
        fin()
        dw()


def back_c(x, featt, w2, n1, i1, g1, b1, dg2, db2, loss, p, q, bn=256):
    rows, d = x.shape
    k = featt.shape[0]
    nb = d // bn

    def at(first):
        return lambda j: (0, jnp.clip(j - first, 0, nb - 1))

    col = pl.BlockSpec((1, bn), at(1))
    row = pl.BlockSpec((bn, d), lambda j: (jnp.minimum(j, nb - 1), 0))
    any_spec = pl.BlockSpec(memory_space=pl.ANY)
    return pl.pallas_call(
        functools.partial(back_c_kernel, nb, rows),
        grid=(nb + 2,),
        in_specs=[pl.BlockSpec((rows, d), lambda j: (0, 0), pipeline_mode=ONCE), pl.BlockSpec((k, rows), lambda j: (0, 0), pipeline_mode=ONCE),
                  row, pl.BlockSpec((rows, bn), at(1)), col, col, col, col, col, pl.BlockSpec((1, bn), lambda j: (0, 0)), any_spec, any_spec],
        out_specs=[any_spec, any_spec, pl.BlockSpec((k, bn), at(1)), pl.BlockSpec((8, bn), at(1))],
        out_shape=[jax.ShapeDtypeStruct((d, d), F32)] * 2 + [jax.ShapeDtypeStruct((k, d), F32), jax.ShapeDtypeStruct((8, d), F32)],
        scratch_shapes=[pltpu.VMEM((rows, bn), F32), pltpu.VMEM((rows, bn), BF16), pltpu.VMEM((2, 2, bn, d), F32),
                        pltpu.SemaphoreType.DMA((2, 2)), pltpu.SemaphoreType.DMA((2, 2))],
        compiler_params=pltpu.CompilerParams(vmem_limit_bytes=VMEM_LIMIT),
        cost_estimate=pl.CostEstimate(flops=2 * rows * d * (k + d), bytes_accessed=rows * d * 20, transcendentals=0),
        name='back_c',
    )(x, featt, w2, n1, i1, g1, b1, dg2, db2, loss, p, q)


def solution(mesh):
    n = mesh.shape[AXIS]
    pair = [(i, i + 1 - 2 * (i % 2)) for i in range(n)]

    def swap(x):
        return lax.ppermute(x, AXIS, pair)

    def local_step(feat_a, feat_b, w_one, w_two, w_three, g_one, b_one, g_two, b_two, lam_off):
        width = w_two.shape[0]
        g1, b1, g2, b2 = (v.reshape(1, width) for v in (g_one, b_one, g_two, b_two))
        norm1, norm2, norm3, inv1, inv2, inv3, act1t, act2t, xt, emb, other = forward(
            feat_a, feat_b, w_one, w_two, w_three, g1, b1, g2, b2, n)
        loss, d_pre2, dg2, db2, dw3, dw2 = back_ab(
            lam_off.reshape(1, 1), emb, other, norm3, inv3, w_three, norm2, inv2, g2, b2, act2t, act1t)
        dw3, dw2, dw1, small = back_c(d_pre2, xt, w_two, norm1, inv1, g1, b1, dg2, db2, loss, dw3, dw2)
        dw1_other = swap(dw1)
        small = small + swap(small)
        dg1, db1, dg2, db2 = (small[i] for i in range(4))
        loss_val = jnp.sum(small[4, :loss.shape[1]]) * 0.5
        return (loss_val, dw1 + dw1_other, dw2, dw3, dg1, db1, dg2, db2)

    row_spec = P(AXIS, None)
    return jax.shard_map(local_step, mesh=mesh, in_specs=(row_spec, row_spec) + (P(),) * 8, out_specs=(P(),) * 8, check_vma=False)
```

```python
import functools

import jax
import jax.numpy as jnp
from jax import lax
from jax.experimental import pallas as pl
from jax.experimental.pallas import tpu as pltpu
from jax.sharding import PartitionSpec as P

NORM_EPS = 1e-5
AXIS = 'data'
MESH = pl.DeviceIdType.MESH
F32 = jnp.float32
BF16 = jnp.bfloat16
ONCE = pl.Buffered(1)
VMEM_LIMIT = 60 * 1024 * 1024
TILE = 256
CHUNK = 64


def fold(v):
    return jnp.sum(v.reshape(v.shape[0] // 8, 8, v.shape[1]), axis=0)


def dot(a, b, dims=((1,), (0,))):
    return lax.dot_general(a, b, (dims, ((), ())), preferred_element_type=F32)


def forward_kernel(nb, rows, fa_ref, fb_ref, w1_ref, w2_ref, w3_ref, g1_ref, b1_ref, g2_ref, b2_ref,
                   n1_ref, n2_ref, n3_ref, i1_ref, i2_ref, i3_ref, t1_ref, t2_ref, xt_ref, emb_hbm, other_hbm,
                   xs, bufa, bufb, acc, copy_sem, feat_sem, send_sem, recv_sem, esend_sem, erecv_sem):
    j = pl.program_id(0)
    me = lax.axis_index(AXIS)
    core = lax.rem(me, 2)
    chip = me // 2
    x_pos, y_pos = lax.rem(chip, 2), chip // 2
    partner = me + 1 - 2 * core
    x_chip, y_chip = chip + 1 - 2 * x_pos, chip + 2 - 4 * y_pos
    piece = fa_ref.shape[0]
    bn = acc.shape[1]

    def remote(src, dst, send, recv, dev):
        return pltpu.make_async_remote_copy(src_ref=src, dst_ref=dst, send_sem=send, recv_sem=recv, device_id=(dev,), device_id_type=MESH)

    def part(dev):
        return xs.at[pl.ds(pl.multiple_of(dev * piece, piece), piece), :]

    def gather():
        barrier = pltpu.get_barrier_semaphore()
        for dev in (partner, 2 * x_chip, 2 * x_chip + 1, 2 * y_chip, 2 * y_chip + 1):
            pl.semaphore_signal(barrier, inc=1, device_id=(dev,), device_id_type=MESH)
        pl.semaphore_wait(barrier, 5)

        def sends(mine, mine_src, theirs_src):
            for view, src in ((mine, mine_src), (1 - mine, theirs_src)):
                remote(src, part(me), send_sem.at[1 + view], recv_sem.at[1 + mine], 2 * x_chip + view).start()
                remote(src, part(me), send_sem.at[3 + view], recv_sem.at[3 + mine], 2 * y_chip + view).start()
            remote(theirs_src, part(me), send_sem.at[0], recv_sem.at[0], partner).start()
            pltpu.make_async_copy(mine_src, part(me), feat_sem).start()

        pl.when(core == 0)(lambda: sends(0, fa_ref, fb_ref))
        pl.when(core == 1)(lambda: sends(1, fb_ref, fa_ref))
        remote(fa_ref, part(2 * x_chip), send_sem.at[1], recv_sem.at[1], me).wait_recv()
        relay_y = remote(part(2 * x_chip), part(2 * x_chip), send_sem.at[5], recv_sem.at[5], 2 * y_chip + core)
        relay_y.start()
        remote(fa_ref, part(2 * y_chip + 1), send_sem.at[4], recv_sem.at[4], me).wait_recv()
        relay_x = remote(part(2 * y_chip + 1), part(2 * y_chip + 1), send_sem.at[6], recv_sem.at[6], 2 * x_chip + core)
        relay_x.start()
        pltpu.make_async_copy(fa_ref, part(me), feat_sem).wait()
        remote(fa_ref, part(me), send_sem.at[0], recv_sem.at[0], me).wait()
        remote(fa_ref, part(me), send_sem.at[1], recv_sem.at[2], me).wait()
        remote(fa_ref, part(me), send_sem.at[2], recv_sem.at[3], me).wait()
        remote(fa_ref, part(me), send_sem.at[3], recv_sem.at[5], me).wait()
        remote(fa_ref, part(me), send_sem.at[4], recv_sem.at[6], me).wait()
        relay_y.wait_send()
        relay_x.wait_send()

    def fin(layer):
        norm_ref, inv_ref = ((n1_ref, i1_ref), (n2_ref, i2_ref), (n3_ref, i3_ref))[layer]
        buf = (bufa, bufb, bufa)[layer]
        base = pl.multiple_of(jnp.maximum(j - 1 - layer * nb, 0) * bn, bn)
        total = jnp.zeros((8, bn), F32)
        square = jnp.zeros((8, bn), F32)
        for r in range(0, rows, CHUNK):
            pre = acc[r:r + CHUNK, :]
            total += fold(pre)
            square += fold(pre * pre)
        mean = jnp.sum(total, axis=0, keepdims=True) / rows
        inv = lax.rsqrt(jnp.sum(square, axis=0, keepdims=True) / rows - mean * mean + NORM_EPS)
        inv_ref[...] = inv
        if layer < 2:
            g_ref, b_ref = ((g1_ref, b1_ref), (g2_ref, b2_ref))[layer]
            g, b = g_ref[...], b_ref[...]
        for r in range(0, rows, CHUNK):
            norm = (acc[r:r + CHUNK, :] - mean) * inv
            norm_ref[r:r + CHUNK, :] = norm
            if layer < 2:
                norm = jnp.maximum(norm * g + b, 0.0)
            buf[r:r + CHUNK, pl.ds(base, bn)] = norm.astype(BF16)
        if layer < 2:
            t_ref = (t1_ref, t2_ref)[layer]
            for r in range(0, rows, TILE):
                t_ref[:, r:r + TILE] = buf[r:r + TILE, pl.ds(base, bn)].T

    def mm(layer):
        x_ref, w_ref = ((xs, w1_ref), (bufa, w2_ref), (bufb, w3_ref))[layer]
        for r in range(0, rows, TILE):
            acc[r:r + TILE, :] = dot(x_ref[r:r + TILE, :], w_ref[...])

    def out_copy(block):
        cols = pl.ds(pl.multiple_of(block * bn, bn), bn)
        return pltpu.make_async_copy(bufa.at[:, cols], emb_hbm.at[:, cols], copy_sem.at[block])

    def emb_copy(block):
        cols = pl.ds(pl.multiple_of(block * bn, bn), bn)
        return remote(bufa.at[:, cols], other_hbm.at[:, cols], esend_sem.at[block], erecv_sem.at[block], partner)

    @pl.when(j == 0)
    def _():
        gather()

    for layer in range(3):
        @pl.when((j >= layer * nb) & (j < (layer + 1) * nb))
        def _(layer=layer):
            fin(layer)
            mm(layer)

        @pl.when(j == (layer + 1) * nb)
        def _(layer=layer):
            fin(layer)

    @pl.when(j >= 2 * nb + 2)
    def _():
        block = j - 2 - 2 * nb
        out_copy(block).start()
        emb_copy(block).start()

    @pl.when(j == 3 * nb + 1)
    def _():
        for r in range(0, rows, TILE):
            xt_ref[:, r:r + TILE] = xs[r:r + TILE, :].T
        for block in range(nb):
            out_copy(block).wait()
            emb_copy(block).wait()


def forward(fa, fb, w1, w2, w3, g1, b1, g2, b2, n, bn=256):
    piece, k = fa.shape
    rows, d = piece * n, w2.shape[1]
    nb = d // bn

    def at(layer, delay):
        return lambda j: (0, jnp.clip(j - layer * nb - delay, 0, nb - 1))

    whole = pl.BlockSpec((piece, k), lambda j: (0, 0), pipeline_mode=ONCE)
    any_spec = pl.BlockSpec(memory_space=pl.ANY)
    col = [pl.BlockSpec((1, bn), at(layer, 1)) for layer in range(3)]
    norm = [pl.BlockSpec((rows, bn), at(layer, 1)) for layer in range(3)]
    big = jax.ShapeDtypeStruct((rows, d), BF16)
    return pl.pallas_call(
        functools.partial(forward_kernel, nb, rows),
        grid=(3 * nb + 2,),
        in_specs=[whole, whole, pl.BlockSpec((k, bn), at(0, 0)), pl.BlockSpec((d, bn), at(1, 0)), pl.BlockSpec((d, bn), at(2, 0)),
                  col[0], col[0], col[1], col[1]],
        out_specs=norm + col + [pl.BlockSpec((bn, rows), lambda j, f=at(layer, 1): f(j)[::-1]) for layer in range(2)]
        + [pl.BlockSpec((k, rows), lambda j: (0, 0), pipeline_mode=ONCE)] + [any_spec] * 2,
        out_shape=[jax.ShapeDtypeStruct((rows, d), F32)] * 3 + [jax.ShapeDtypeStruct((1, d), F32)] * 3
        + [jax.ShapeDtypeStruct((d, rows), BF16)] * 2 + [jax.ShapeDtypeStruct((k, rows), BF16)] + [big] * 2,
        scratch_shapes=[pltpu.VMEM((rows, k), BF16), pltpu.VMEM((rows, d), BF16), pltpu.VMEM((rows, d), BF16), pltpu.VMEM((rows, bn), F32),
                        pltpu.SemaphoreType.DMA((nb,)), pltpu.SemaphoreType.DMA, pltpu.SemaphoreType.DMA((7,)), pltpu.SemaphoreType.DMA((7,)),
                        pltpu.SemaphoreType.DMA((nb,)), pltpu.SemaphoreType.DMA((nb,))],
        compiler_params=pltpu.CompilerParams(collective_id=0, has_side_effects=True, vmem_limit_bytes=VMEM_LIMIT),
        cost_estimate=pl.CostEstimate(flops=2 * rows * d * (k + 2 * d), bytes_accessed=rows * d * 20, transcendentals=0),
        name='forward',
    )(fa, fb, w1, w2, w3, g1, b1, g2, b2)


def finish_back(rows, acc, norm_ref, inv, g, b, put):
    bn = acc.shape[1]
    total = jnp.zeros((8, bn), F32)
    cross = jnp.zeros((8, bn), F32)
    for r in range(0, rows, CHUNK):
        part = acc[r:r + CHUNK, :]
        norm = norm_ref[r:r + CHUNK, :]
        if b is not None:
            part = jnp.where(norm * g + b > 0.0, part, 0.0)
            acc[r:r + CHUNK, :] = part
        total += fold(part)
        cross += fold(part * norm)
    total = jnp.sum(total, axis=0, keepdims=True)
    cross = jnp.sum(cross, axis=0, keepdims=True)
    scale = inv if g is None else inv * g
    shift, slope = scale * (total / rows), scale * (cross / rows)
    for r in range(0, rows, CHUNK):
        put(r, (acc[r:r + CHUNK, :] * scale - shift - norm_ref[r:r + CHUNK, :] * slope).astype(BF16))
    return total, cross


def back_ab_kernel(nb, rows, lam_ref, own_ref, other_hbm, n3_ref, i3_ref, w3_ref, n2_ref, i2_ref, g2_ref, b2_ref, t2_ref, t1_hbm,
                   loss_ref, dpre_ref, dg_ref, db_ref, dw3_hbm, dw2_hbm,
                   big, corr, grad, acc, dout, send3, recv3, send2, recv2, load_sem, ssem, rsem, osem, free3, free2):
    j = pl.program_id(0)
    me = lax.axis_index(AXIS)
    partner = me + 1 - 2 * lax.rem(me, 2)
    bn = acc.shape[1]
    d = big.shape[1]
    lam = lam_ref[0, 0]
    other_ref = big

    def pair(e):
        return ((send3, recv3, free3, nb), (send2, recv2, free2, nb + 1))[e]

    def swap_copy(e, b):
        send, recv, _, _ = pair(e)
        return pltpu.make_async_remote_copy(
            src_ref=send.at[lax.rem(b, 2)], dst_ref=recv.at[lax.rem(b, 3)], send_sem=ssem.at[e, lax.rem(b, 2)],
            recv_sem=rsem.at[e, lax.rem(b, 3)], device_id=(partner,), device_id_type=MESH)

    def sum_copy(e, b):
        span = pl.ds(pl.multiple_of(b * bn, bn), bn)
        dst = dw3_hbm.at[span, :] if e == 0 else dw2_hbm.at[:, span]
        return pltpu.make_async_copy(pair(e)[1].at[lax.rem(b, 3)], dst, osem.at[e, lax.rem(b, 3)])

    def exchange(e):
        send, recv, free, first = pair(e)

        @pl.when((j >= first + 3) & (j < first + 3 + nb))
        def _():
            b = j - first - 3
            sum_copy(e, b).wait()

            @pl.when(b < nb - 3)
            def _():
                pl.semaphore_signal(free, inc=1, device_id=(partner,), device_id_type=MESH)

        @pl.when((j >= first + 2) & (j < first + 2 + nb))
        def _():
            b = j - first - 2
            swap_copy(e, b).wait()
            mine, theirs = lax.rem(b, 2), lax.rem(b, 3)
            for r in range(0, send.shape[1], send.shape[1] // 32):
                part = pl.ds(r, send.shape[1] // 32)
                recv[theirs, part, :] = recv[theirs, part, :] + send[mine, part, :]
            sum_copy(e, b).start()

        @pl.when((j >= first + 1) & (j < first + 1 + nb))
        def _():
            b = j - first - 1

            @pl.when(b >= 3)
            def _():
                pl.semaphore_wait(free, 1)

            swap_copy(e, b).start()

    def fin_loss():
        base = pl.multiple_of(jnp.maximum(j - 1, 0) * bn, bn)

        def put(r, v):
            dout[r:r + CHUNK, pl.ds(base, bn)] = v

        finish_back(rows, acc, n3_ref, i3_ref[...], None, None, put)

    def mm_loss():
        own = own_ref[...]
        loss = jnp.zeros((8, bn), F32)
        for c in range(0, d, bn):
            part = dot(own, other_ref[:, c:c + bn], ((0,), (0,))) * (1.0 / rows)
            corr[:, c:c + bn] = part
            loss += fold(part * part)
            grad[:, c:c + bn] = ((2.0 * lam) * part).astype(BF16)
        here = pl.ds(pl.multiple_of(j * bn, bn), bn)
        part = corr[:, here]
        diag = lax.broadcasted_iota(jnp.int32, (bn, bn), 0) == lax.broadcasted_iota(jnp.int32, (bn, bn), 1)
        grad[:, here] = jnp.where(diag, -2.0 * (1.0 - part), (2.0 * lam) * part).astype(BF16)
        loss = lam * loss + fold(jnp.where(diag, (1.0 - part) * (1.0 - part) - lam * (part * part), 0.0))
        loss_ref[...] += jnp.sum(loss, axis=0, keepdims=True)
        for r in range(0, rows, TILE):
            acc[r:r + TILE, :] = dot(other_ref[r:r + TILE, :], grad[...], ((1,), (1,))) * (1.0 / rows)

    def fin_two():
        def put(r, v):
            dpre_ref[r:r + CHUNK, :] = v

        db_ref[...], dg_ref[...] = finish_back(rows, acc, n2_ref, i2_ref[...], g2_ref[...], b2_ref[...], put)

    def mm_two():
        for r in range(0, rows, TILE):
            acc[r:r + TILE, :] = dot(dout[r:r + TILE, :], w3_ref[...], ((1,), (1,)))
        act = t2_ref[...]
        slot = lax.rem(j - nb, 2)
        for c in range(0, d, 2 * bn):
            send3[slot, :, c:c + 2 * bn] = dot(act, dout[:, c:c + 2 * bn])

    def mm_dw2():
        slot = lax.rem(j - nb - 1, 2)
        for r in range(0, d, TILE):
            send2[slot, r:r + TILE, :] = dot(big[r:r + TILE, :], dpre_ref[...])

    @pl.when(j == 0)
    def _():
        load = pltpu.make_async_copy(other_hbm, big, load_sem)
        load.start()
        loss_ref[...] = jnp.zeros_like(loss_ref)
        barrier = pltpu.get_barrier_semaphore()
        pl.semaphore_signal(barrier, inc=1, device_id=(partner,), device_id_type=MESH)
        pl.semaphore_wait(barrier, 1)
        load.wait()

    @pl.when(j == nb)
    def _():
        pltpu.make_async_copy(t1_hbm, big, load_sem).start()

    exchange(0)
    exchange(1)

    @pl.when(j < nb)
    def _():
        fin_loss()
        mm_loss()

    @pl.when(j == nb)
    def _():
        fin_loss()

    @pl.when((j >= nb) & (j < 2 * nb))
    def _():
        fin_two()
        mm_two()

    @pl.when(j == 2 * nb)
    def _():
        fin_two()

    @pl.when(j == nb + 1)
    def _():
        pltpu.make_async_copy(t1_hbm, big, load_sem).wait()

    @pl.when((j > nb) & (j <= 2 * nb))
    def _():
        mm_dw2()


def back_ab(lam, own, other, n3, i3, w3, n2, i2, g2, b2, t2, t1, bn=256):
    rows, d = own.shape
    nb = d // bn

    def at(first):
        return lambda j: (0, jnp.clip(j - first, 0, nb - 1))

    def block(first):
        return pl.BlockSpec((rows, bn), at(first))

    def col(first):
        return pl.BlockSpec((1, bn), at(first))

    row = pl.BlockSpec((bn, d), lambda j: (jnp.clip(j - nb, 0, nb - 1), 0))
    vec = jax.ShapeDtypeStruct((1, d), F32)
    any_spec = pl.BlockSpec(memory_space=pl.ANY)
    return pl.pallas_call(
        functools.partial(back_ab_kernel, nb, rows),
        grid=(2 * nb + 4,),
        in_specs=[pl.BlockSpec(memory_space=pltpu.SMEM), block(0), any_spec,
                  block(1), col(1), row, block(nb + 1), col(nb + 1), col(nb + 1), col(nb + 1), row, any_spec],
        out_specs=[pl.BlockSpec((1, bn), lambda j: (0, 0)), block(nb + 1), col(nb + 1), col(nb + 1), any_spec, any_spec],
        out_shape=[jax.ShapeDtypeStruct((1, bn), F32), jax.ShapeDtypeStruct((rows, d), BF16), vec, vec]
        + [jax.ShapeDtypeStruct((d, d), F32)] * 2,
        scratch_shapes=[pltpu.VMEM((rows, d), BF16), pltpu.VMEM((bn, d), F32), pltpu.VMEM((bn, d), BF16), pltpu.VMEM((rows, bn), F32),
                        pltpu.VMEM((rows, d), BF16), pltpu.VMEM((2, bn, d), F32), pltpu.VMEM((3, bn, d), F32),
                        pltpu.VMEM((2, d, bn), F32), pltpu.VMEM((3, d, bn), F32), pltpu.SemaphoreType.DMA,
                        pltpu.SemaphoreType.DMA((2, 2)), pltpu.SemaphoreType.DMA((2, 3)), pltpu.SemaphoreType.DMA((2, 3)),
                        pltpu.SemaphoreType.REGULAR, pltpu.SemaphoreType.REGULAR],
        compiler_params=pltpu.CompilerParams(collective_id=1, has_side_effects=True, vmem_limit_bytes=63 * 1024 * 1024),
        cost_estimate=pl.CostEstimate(flops=10 * rows * d * d, bytes_accessed=rows * d * 24, transcendentals=0),
        name='back_ab',
    )(lam, own, other, n3, i3, w3, n2, i2, g2, b2, t2, t1)


def back_c_kernel(nb, rows, x_ref, featt, w2_ref, n1_ref, i1_ref, g1_ref, b1_ref, dg2_ref, db2_ref, loss_ref, p_ref, q_ref,
                  p_out, q_out, dw1_ref, small_ref, acc, dpre, ring, load_sem, store_sem):
    j = pl.program_id(0)
    bn = acc.shape[1]

    def fin():
        def put(r, v):
            dpre[r:r + CHUNK, :] = v

        db, dg = finish_back(rows, acc, n1_ref, i1_ref[...], g1_ref[...], b1_ref[...], put)
        small_ref[0:1, :] = dg
        small_ref[1:2, :] = db
        small_ref[2:3, :] = dg2_ref[...]
        small_ref[3:4, :] = db2_ref[...]
        small_ref[4:5, :] = loss_ref[...]

    def mm():
        for r in range(0, rows, TILE):
            acc[r:r + TILE, :] = dot(x_ref[r:r + TILE, :], w2_ref[...], ((1,), (1,)))

    def dw():
        dw1_ref[...] = dot(featt[...], dpre[...])

    @pl.when(j < nb)
    def _():
        fin()
        mm()
        dw()

    @pl.when(j == nb)
    def _():
        fin()
        dw()


def back_c(x, featt, w2, n1, i1, g1, b1, dg2, db2, loss, p, q, bn=256):
    rows, d = x.shape
    k = featt.shape[0]
    nb = d // bn

    def at(first):
        return lambda j: (0, jnp.clip(j - first, 0, nb - 1))

    col = pl.BlockSpec((1, bn), at(1))
    row = pl.BlockSpec((bn, d), lambda j: (jnp.minimum(j, nb - 1), 0))
    any_spec = pl.BlockSpec(memory_space=pl.ANY)
    return pl.pallas_call(
        functools.partial(back_c_kernel, nb, rows),
        grid=(nb + 2,),
        in_specs=[pl.BlockSpec((rows, d), lambda j: (0, 0), pipeline_mode=ONCE), pl.BlockSpec((k, rows), lambda j: (0, 0), pipeline_mode=ONCE),
                  row, pl.BlockSpec((rows, bn), at(1)), col, col, col, col, col, pl.BlockSpec((1, bn), lambda j: (0, 0)), any_spec, any_spec],
        input_output_aliases={10: 0, 11: 1},
        out_specs=[any_spec, any_spec, pl.BlockSpec((k, bn), at(1)), pl.BlockSpec((8, bn), at(1))],
        out_shape=[jax.ShapeDtypeStruct((d, d), F32)] * 2 + [jax.ShapeDtypeStruct((k, d), F32), jax.ShapeDtypeStruct((8, d), F32)],
        scratch_shapes=[pltpu.VMEM((rows, bn), F32), pltpu.VMEM((rows, bn), BF16), pltpu.VMEM((2, 2, bn, d), F32),
                        pltpu.SemaphoreType.DMA((2, 2)), pltpu.SemaphoreType.DMA((2, 2))],
        compiler_params=pltpu.CompilerParams(vmem_limit_bytes=VMEM_LIMIT),
        cost_estimate=pl.CostEstimate(flops=2 * rows * d * (k + d), bytes_accessed=rows * d * 20, transcendentals=0),
        name='back_c',
    )(x, featt, w2, n1, i1, g1, b1, dg2, db2, loss, p, q)


def solution(mesh):
    n = mesh.shape[AXIS]
    pair = [(i, i + 1 - 2 * (i % 2)) for i in range(n)]

    def swap(x):
        return lax.ppermute(x, AXIS, pair)

    def local_step(feat_a, feat_b, w_one, w_two, w_three, g_one, b_one, g_two, b_two, lam_off):
        width = w_two.shape[0]
        g1, b1, g2, b2 = (v.reshape(1, width) for v in (g_one, b_one, g_two, b_two))
        norm1, norm2, norm3, inv1, inv2, inv3, act1t, act2t, xt, emb, other = forward(
            feat_a, feat_b, w_one, w_two, w_three, g1, b1, g2, b2, n)
        loss, d_pre2, dg2, db2, dw3, dw2 = back_ab(
            lam_off.reshape(1, 1), emb, other, norm3, inv3, w_three, norm2, inv2, g2, b2, act2t, act1t)
        dw3, dw2, dw1, small = back_c(d_pre2, xt, w_two, norm1, inv1, g1, b1, dg2, db2, loss, dw3, dw2)
        dw1_other = swap(dw1)
        small = small + swap(small)
        dg1, db1, dg2, db2 = (small[i] for i in range(4))
        loss_val = jnp.sum(small[4, :loss.shape[1]]) * 0.5
        return (loss_val, dw1 + dw1_other, dw2, dw3, dg1, db1, dg2, db2)

    row_spec = P(AXIS, None)
    return jax.shard_map(local_step, mesh=mesh, in_specs=(row_spec, row_spec) + (P(),) * 8, out_specs=(P(),) * 8, check_vma=False)
```

```python
import functools

import jax
import jax.numpy as jnp
from jax import lax
from jax.experimental import pallas as pl
from jax.experimental.pallas import tpu as pltpu
from jax.sharding import PartitionSpec as P

NORM_EPS = 1e-5
AXIS = 'data'
MESH = pl.DeviceIdType.MESH
F32 = jnp.float32
BF16 = jnp.bfloat16
ONCE = pl.Buffered(1)
VMEM_LIMIT = 60 * 1024 * 1024
TILE = 256
CHUNK = 64


def fold(v):
    return jnp.sum(v.reshape(v.shape[0] // 8, 8, v.shape[1]), axis=0)


def dot(a, b, dims=((1,), (0,))):
    return lax.dot_general(a, b, (dims, ((), ())), preferred_element_type=F32)


def forward_kernel(nb, rows, fa_ref, fb_ref, w1_ref, w2_ref, w3_ref, g1_ref, b1_ref, g2_ref, b2_ref,
                   n1_hbm, n2_ref, n3_ref, i1_ref, i2_ref, i3_ref, t1_ref, t2_ref, xt_ref, emb_hbm, other_hbm,
                   xs, pre1, sums1, bufa, bufb, acc, norm_sem, copy_sem, feat_sem, send_sem, recv_sem, esend_sem, erecv_sem):
    j = pl.program_id(0)
    me = lax.axis_index(AXIS)
    core = lax.rem(me, 2)
    chip = me // 2
    x_pos, y_pos = lax.rem(chip, 2), chip // 2
    partner = me + 1 - 2 * core
    x_chip, y_chip = chip + 1 - 2 * x_pos, chip + 2 - 4 * y_pos
    piece = fa_ref.shape[0]
    bn = acc.shape[1]

    def remote(src, dst, send, recv, dev):
        return pltpu.make_async_remote_copy(src_ref=src, dst_ref=dst, send_sem=send, recv_sem=recv, device_id=(dev,), device_id_type=MESH)

    def part(dev):
        return xs.at[pl.ds(pl.multiple_of(dev * piece, piece), piece), :]

    def gather():
        barrier = pltpu.get_barrier_semaphore()
        for dev in (partner, 2 * x_chip, 2 * x_chip + 1, 2 * y_chip, 2 * y_chip + 1):
            pl.semaphore_signal(barrier, inc=1, device_id=(dev,), device_id_type=MESH)
        pl.semaphore_wait(barrier, 5)

        def sends(mine, mine_src, theirs_src):
            for view, src in ((mine, mine_src), (1 - mine, theirs_src)):
                remote(src, part(me), send_sem.at[1 + view], recv_sem.at[1 + mine], 2 * x_chip + view).start()
                remote(src, part(me), send_sem.at[3 + view], recv_sem.at[3 + mine], 2 * y_chip + view).start()
            remote(theirs_src, part(me), send_sem.at[0], recv_sem.at[0], partner).start()
            pltpu.make_async_copy(mine_src, part(me), feat_sem).start()

        pl.when(core == 0)(lambda: sends(0, fa_ref, fb_ref))
        pl.when(core == 1)(lambda: sends(1, fb_ref, fa_ref))
        remote(fa_ref, part(2 * x_chip), send_sem.at[1], recv_sem.at[1], me).wait_recv()
        relay_y = remote(part(2 * x_chip), part(2 * x_chip), send_sem.at[5], recv_sem.at[5], 2 * y_chip + core)
        relay_y.start()
        remote(fa_ref, part(2 * y_chip + 1), send_sem.at[4], recv_sem.at[4], me).wait_recv()
        relay_x = remote(part(2 * y_chip + 1), part(2 * y_chip + 1), send_sem.at[6], recv_sem.at[6], 2 * x_chip + core)
        relay_x.start()
        pltpu.make_async_copy(fa_ref, part(me), feat_sem).wait()
        remote(fa_ref, part(me), send_sem.at[0], recv_sem.at[0], me).wait()
        layer_one(me, partner)
        layer_one(2 * x_chip, 2 * y_chip + 1)
        remote(fa_ref, part(me), send_sem.at[1], recv_sem.at[2], me).wait()
        remote(fa_ref, part(me), send_sem.at[2], recv_sem.at[3], me).wait()
        layer_one(2 * x_chip + 1, 2 * y_chip)
        remote(fa_ref, part(me), send_sem.at[3], recv_sem.at[5], me).wait()
        remote(fa_ref, part(me), send_sem.at[4], recv_sem.at[6], me).wait()
        far = 2 * (3 - chip)
        layer_one(far, far + 1)
        relay_y.wait_send()
        relay_x.wait_send()

    def layer_one(dev_p, dev_q):
        def work(i, carry):
            here = pl.ds(pl.multiple_of(jnp.where(i == 0, dev_p, dev_q) * piece, piece), piece)
            feats = xs[here, :]
            for c in range(0, w1_ref.shape[1], bn):
                pre = dot(feats, w1_ref[:, c:c + bn])
                pre1[here, c:c + bn] = pre
                sums1[0:8, c:c + bn] += fold(pre)
                sums1[8:16, c:c + bn] += fold(pre * pre)
            return carry

        lax.fori_loop(0, 2, work, 0)

    def norm_copy(block):
        cols = pl.ds(pl.multiple_of(block * bn, bn), bn)
        return pltpu.make_async_copy(pre1.at[:, cols], n1_hbm.at[:, cols], norm_sem.at[block])

    def finish_one():
        mean = jnp.sum(sums1[0:8, :], axis=0, keepdims=True) / rows
        inv = lax.rsqrt(jnp.sum(sums1[8:16, :], axis=0, keepdims=True) / rows - mean * mean + NORM_EPS)
        sums1[0:1, :] = mean
        i1_ref[...] = inv

        def work(block, carry):
            cols = pl.ds(pl.multiple_of(block * bn, bn), bn)
            mean, inv, g, b = sums1[0:1, cols], i1_ref[:, cols], g1_ref[:, cols], b1_ref[:, cols]
            for r in range(0, rows, CHUNK):
                norm = (pre1[r:r + CHUNK, cols] - mean) * inv
                pre1[r:r + CHUNK, cols] = norm
                bufa[r:r + CHUNK, cols] = jnp.maximum(norm * g + b, 0.0).astype(BF16)
            return carry

        lax.fori_loop(0, nb, work, 0)
        for block in range(nb):
            norm_copy(block).start()

    def fin(layer):
        norm_ref, inv_ref = ((n2_ref, i2_ref), (n3_ref, i3_ref))[layer]
        buf = (bufb, bufa)[layer]
        base = pl.multiple_of(jnp.maximum(j - 1 - layer * nb, 0) * bn, bn)
        total = jnp.zeros((8, bn), F32)
        square = jnp.zeros((8, bn), F32)
        for r in range(0, rows, CHUNK):
            pre = acc[r:r + CHUNK, :]
            total += fold(pre)
            square += fold(pre * pre)
        mean = jnp.sum(total, axis=0, keepdims=True) / rows
        inv = lax.rsqrt(jnp.sum(square, axis=0, keepdims=True) / rows - mean * mean + NORM_EPS)
        inv_ref[...] = inv
        if layer == 0:
            g, b = g2_ref[...], b2_ref[...]
        for r in range(0, rows, CHUNK):
            norm = (acc[r:r + CHUNK, :] - mean) * inv
            norm_ref[r:r + CHUNK, :] = norm
            if layer == 0:
                norm = jnp.maximum(norm * g + b, 0.0)
            buf[r:r + CHUNK, pl.ds(base, bn)] = norm.astype(BF16)
        if layer == 0:
            for r in range(0, rows, TILE):
                t2_ref[:, r:r + TILE] = buf[r:r + TILE, pl.ds(base, bn)].T

    def mm(layer):
        x_ref, w_ref = ((bufa, w2_ref), (bufb, w3_ref))[layer]
        for r in range(0, rows, TILE):
            acc[r:r + TILE, :] = dot(x_ref[r:r + TILE, :], w_ref[...])

    def out_copy(block):
        cols = pl.ds(pl.multiple_of(block * bn, bn), bn)
        return pltpu.make_async_copy(bufa.at[:, cols], emb_hbm.at[:, cols], copy_sem.at[block])

    def emb_copy(block):
        cols = pl.ds(pl.multiple_of(block * bn, bn), bn)
        return remote(bufa.at[:, cols], other_hbm.at[:, cols], esend_sem.at[block], erecv_sem.at[block], partner)

    @pl.when(j == 0)
    def _():
        sums1[...] = jnp.zeros_like(sums1)
        gather()
        finish_one()

    for layer in range(2):
        @pl.when((j >= layer * nb) & (j < (layer + 1) * nb))
        def _(layer=layer):
            fin(layer)
            mm(layer)
            if layer == 0:
                base = pl.multiple_of(j * bn, bn)
                for r in range(0, rows, TILE):
                    t1_ref[:, r:r + TILE] = bufa[r:r + TILE, pl.ds(base, bn)].T

        @pl.when(j == (layer + 1) * nb)
        def _(layer=layer):
            fin(layer)

    @pl.when(j >= nb + 2)
    def _():
        block = j - 2 - nb
        out_copy(block).start()
        emb_copy(block).start()

    @pl.when(j == nb + 1)
    def _():
        for r in range(0, rows, TILE):
            xt_ref[:, r:r + TILE] = xs[r:r + TILE, :].T

    @pl.when(j == 2 * nb + 1)
    def _():
        for block in range(nb):
            norm_copy(block).wait()
            out_copy(block).wait()
            emb_copy(block).wait()


def forward(fa, fb, w1, w2, w3, g1, b1, g2, b2, n, bn=256):
    piece, k = fa.shape
    rows, d = piece * n, w2.shape[1]
    nb = d // bn

    def at(layer, delay):
        return lambda j: (0, jnp.clip(j - layer * nb - delay, 0, nb - 1))

    whole = pl.BlockSpec((piece, k), lambda j: (0, 0), pipeline_mode=ONCE)
    any_spec = pl.BlockSpec(memory_space=pl.ANY)
    col = [pl.BlockSpec((1, bn), at(layer, 1)) for layer in range(2)]
    norm = [pl.BlockSpec((rows, bn), at(layer, 1)) for layer in range(2)]
    vec = pl.BlockSpec((1, d), lambda j: (0, 0))
    big = jax.ShapeDtypeStruct((rows, d), BF16)
    return pl.pallas_call(
        functools.partial(forward_kernel, nb, rows),
        grid=(2 * nb + 2,),
        in_specs=[whole, whole, pl.BlockSpec((k, d), lambda j: (0, 0), pipeline_mode=ONCE), pl.BlockSpec((d, bn), at(0, 0)), pl.BlockSpec((d, bn), at(1, 0)),
                  vec, vec, col[0], col[0]],
        out_specs=[any_spec] + norm + [vec] + col + [pl.BlockSpec((bn, rows), lambda j, f=at(0, delay): f(j)[::-1]) for delay in range(2)]
        + [pl.BlockSpec((k, rows), lambda j: (0, 0), pipeline_mode=ONCE)] + [any_spec] * 2,
        out_shape=[jax.ShapeDtypeStruct((rows, d), F32)] * 3 + [jax.ShapeDtypeStruct((1, d), F32)] * 3
        + [jax.ShapeDtypeStruct((d, rows), BF16)] * 2 + [jax.ShapeDtypeStruct((k, rows), BF16)] + [big] * 2,
        scratch_shapes=[pltpu.VMEM((rows, k), BF16), pltpu.VMEM((rows, d), F32), pltpu.VMEM((16, d), F32), pltpu.VMEM((rows, d), BF16),
                        pltpu.VMEM((rows, d), BF16), pltpu.VMEM((rows, bn), F32), pltpu.SemaphoreType.DMA((nb,)),
                        pltpu.SemaphoreType.DMA((nb,)), pltpu.SemaphoreType.DMA, pltpu.SemaphoreType.DMA((7,)), pltpu.SemaphoreType.DMA((7,)),
                        pltpu.SemaphoreType.DMA((nb,)), pltpu.SemaphoreType.DMA((nb,))],
        compiler_params=pltpu.CompilerParams(collective_id=0, has_side_effects=True, vmem_limit_bytes=63 * 1024 * 1024),
        cost_estimate=pl.CostEstimate(flops=2 * rows * d * (k + 2 * d), bytes_accessed=rows * d * 20, transcendentals=0),
        name='forward',
    )(fa, fb, w1, w2, w3, g1, b1, g2, b2)


def finish_back(rows, acc, norm_ref, inv, g, b, put):
    bn = acc.shape[1]
    total = jnp.zeros((8, bn), F32)
    cross = jnp.zeros((8, bn), F32)
    for r in range(0, rows, CHUNK):
        part = acc[r:r + CHUNK, :]
        norm = norm_ref[r:r + CHUNK, :]
        if b is not None:
            part = jnp.where(norm * g + b > 0.0, part, 0.0)
            acc[r:r + CHUNK, :] = part
        total += fold(part)
        cross += fold(part * norm)
    total = jnp.sum(total, axis=0, keepdims=True)
    cross = jnp.sum(cross, axis=0, keepdims=True)
    scale = inv if g is None else inv * g
    shift, slope = scale * (total / rows), scale * (cross / rows)
    for r in range(0, rows, CHUNK):
        put(r, (acc[r:r + CHUNK, :] * scale - shift - norm_ref[r:r + CHUNK, :] * slope).astype(BF16))
    return total, cross


def back_ab_kernel(nb, rows, lam_ref, own_ref, other_hbm, n3_ref, i3_ref, w3_ref, n2_ref, i2_ref, g2_ref, b2_ref, t2_ref, t1_hbm,
                   loss_ref, dpre_ref, dg_ref, db_ref, dw3_hbm, dw2_hbm,
                   big, corr, grad, acc, dout, send3, recv3, send2, recv2, load_sem, ssem, rsem, osem, free3, free2):
    j = pl.program_id(0)
    me = lax.axis_index(AXIS)
    partner = me + 1 - 2 * lax.rem(me, 2)
    bn = acc.shape[1]
    d = big.shape[1]
    lam = lam_ref[0, 0]
    other_ref = big

    def pair(e):
        return ((send3, recv3, free3, nb), (send2, recv2, free2, nb + 1))[e]

    def swap_copy(e, b):
        send, recv, _, _ = pair(e)
        return pltpu.make_async_remote_copy(
            src_ref=send.at[lax.rem(b, 2)], dst_ref=recv.at[lax.rem(b, 3)], send_sem=ssem.at[e, lax.rem(b, 2)],
            recv_sem=rsem.at[e, lax.rem(b, 3)], device_id=(partner,), device_id_type=MESH)

    def sum_copy(e, b):
        span = pl.ds(pl.multiple_of(b * bn, bn), bn)
        dst = dw3_hbm.at[span, :] if e == 0 else dw2_hbm.at[:, span]
        return pltpu.make_async_copy(pair(e)[1].at[lax.rem(b, 3)], dst, osem.at[e, lax.rem(b, 3)])

    def exchange(e):
        send, recv, free, first = pair(e)

        @pl.when((j >= first + 3) & (j < first + 3 + nb))
        def _():
            b = j - first - 3
            sum_copy(e, b).wait()

            @pl.when(b < nb - 3)
            def _():
                pl.semaphore_signal(free, inc=1, device_id=(partner,), device_id_type=MESH)

        @pl.when((j >= first + 2) & (j < first + 2 + nb))
        def _():
            b = j - first - 2
            swap_copy(e, b).wait()
            mine, theirs = lax.rem(b, 2), lax.rem(b, 3)
            for r in range(0, send.shape[1], send.shape[1] // 32):
                part = pl.ds(r, send.shape[1] // 32)
                recv[theirs, part, :] = recv[theirs, part, :] + send[mine, part, :]
            sum_copy(e, b).start()

        @pl.when((j >= first + 1) & (j < first + 1 + nb))
        def _():
            b = j - first - 1

            @pl.when(b >= 3)
            def _():
                pl.semaphore_wait(free, 1)

            swap_copy(e, b).start()

    def fin_loss():
        base = pl.multiple_of(jnp.maximum(j - 1, 0) * bn, bn)

        def put(r, v):
            dout[r:r + CHUNK, pl.ds(base, bn)] = v

        finish_back(rows, acc, n3_ref, i3_ref[...], None, None, put)

    def mm_loss():
        own = own_ref[...]
        loss = jnp.zeros((8, bn), F32)
        for c in range(0, d, bn):
            part = dot(own, other_ref[:, c:c + bn], ((0,), (0,))) * (1.0 / rows)
            corr[:, c:c + bn] = part
            loss += fold(part * part)
            grad[:, c:c + bn] = ((2.0 * lam) * part).astype(BF16)
        here = pl.ds(pl.multiple_of(j * bn, bn), bn)
        part = corr[:, here]
        diag = lax.broadcasted_iota(jnp.int32, (bn, bn), 0) == lax.broadcasted_iota(jnp.int32, (bn, bn), 1)
        grad[:, here] = jnp.where(diag, -2.0 * (1.0 - part), (2.0 * lam) * part).astype(BF16)
        loss = lam * loss + fold(jnp.where(diag, (1.0 - part) * (1.0 - part) - lam * (part * part), 0.0))
        loss_ref[...] += jnp.sum(loss, axis=0, keepdims=True)
        for r in range(0, rows, TILE):
            acc[r:r + TILE, :] = dot(other_ref[r:r + TILE, :], grad[...], ((1,), (1,))) * (1.0 / rows)

    def fin_two():
        def put(r, v):
            dpre_ref[r:r + CHUNK, :] = v

        db_ref[...], dg_ref[...] = finish_back(rows, acc, n2_ref, i2_ref[...], g2_ref[...], b2_ref[...], put)

    def mm_two():
        for r in range(0, rows, TILE):
            acc[r:r + TILE, :] = dot(dout[r:r + TILE, :], w3_ref[...], ((1,), (1,)))
        act = t2_ref[...]
        slot = lax.rem(j - nb, 2)
        for c in range(0, d, 2 * bn):
            send3[slot, :, c:c + 2 * bn] = dot(act, dout[:, c:c + 2 * bn])

    def mm_dw2():
        slot = lax.rem(j - nb - 1, 2)
        for r in range(0, d, TILE):
            send2[slot, r:r + TILE, :] = dot(big[r:r + TILE, :], dpre_ref[...])

    @pl.when(j == 0)
    def _():
        load = pltpu.make_async_copy(other_hbm, big, load_sem)
        load.start()
        loss_ref[...] = jnp.zeros_like(loss_ref)
        barrier = pltpu.get_barrier_semaphore()
        pl.semaphore_signal(barrier, inc=1, device_id=(partner,), device_id_type=MESH)
        pl.semaphore_wait(barrier, 1)
        load.wait()

    @pl.when(j == nb)
    def _():
        pltpu.make_async_copy(t1_hbm, big, load_sem).start()

    exchange(0)
    exchange(1)

    @pl.when(j < nb)
    def _():
        fin_loss()
        mm_loss()

    @pl.when(j == nb)
    def _():
        fin_loss()

    @pl.when((j >= nb) & (j < 2 * nb))
    def _():
        fin_two()
        mm_two()

    @pl.when(j == 2 * nb)
    def _():
        fin_two()

    @pl.when(j == nb + 1)
    def _():
        pltpu.make_async_copy(t1_hbm, big, load_sem).wait()

    @pl.when((j > nb) & (j <= 2 * nb))
    def _():
        mm_dw2()


def back_ab(lam, own, other, n3, i3, w3, n2, i2, g2, b2, t2, t1, bn=256):
    rows, d = own.shape
    nb = d // bn

    def at(first):
        return lambda j: (0, jnp.clip(j - first, 0, nb - 1))

    def block(first):
        return pl.BlockSpec((rows, bn), at(first))

    def col(first):
        return pl.BlockSpec((1, bn), at(first))

    row = pl.BlockSpec((bn, d), lambda j: (jnp.clip(j - nb, 0, nb - 1), 0))
    vec = jax.ShapeDtypeStruct((1, d), F32)
    any_spec = pl.BlockSpec(memory_space=pl.ANY)
    return pl.pallas_call(
        functools.partial(back_ab_kernel, nb, rows),
        grid=(2 * nb + 4,),
        in_specs=[pl.BlockSpec(memory_space=pltpu.SMEM), block(0), any_spec,
                  block(1), col(1), row, block(nb + 1), col(nb + 1), col(nb + 1), col(nb + 1), row, any_spec],
        out_specs=[pl.BlockSpec((1, bn), lambda j: (0, 0)), block(nb + 1), col(nb + 1), col(nb + 1), any_spec, any_spec],
        out_shape=[jax.ShapeDtypeStruct((1, bn), F32), jax.ShapeDtypeStruct((rows, d), BF16), vec, vec]
        + [jax.ShapeDtypeStruct((d, d), F32)] * 2,
        scratch_shapes=[pltpu.VMEM((rows, d), BF16), pltpu.VMEM((bn, d), F32), pltpu.VMEM((bn, d), BF16), pltpu.VMEM((rows, bn), F32),
                        pltpu.VMEM((rows, d), BF16), pltpu.VMEM((2, bn, d), F32), pltpu.VMEM((3, bn, d), F32),
                        pltpu.VMEM((2, d, bn), F32), pltpu.VMEM((3, d, bn), F32), pltpu.SemaphoreType.DMA,
                        pltpu.SemaphoreType.DMA((2, 2)), pltpu.SemaphoreType.DMA((2, 3)), pltpu.SemaphoreType.DMA((2, 3)),
                        pltpu.SemaphoreType.REGULAR, pltpu.SemaphoreType.REGULAR],
        compiler_params=pltpu.CompilerParams(collective_id=1, has_side_effects=True, vmem_limit_bytes=63 * 1024 * 1024),
        cost_estimate=pl.CostEstimate(flops=10 * rows * d * d, bytes_accessed=rows * d * 24, transcendentals=0),
        name='back_ab',
    )(lam, own, other, n3, i3, w3, n2, i2, g2, b2, t2, t1)


def back_c_kernel(nb, rows, x_ref, featt, w2_ref, n1_ref, i1_ref, g1_ref, b1_ref, dg2_ref, db2_ref, loss_ref, p_ref, q_ref,
                  p_out, q_out, dw1_ref, small_ref, acc, dpre, ring, load_sem, store_sem):
    j = pl.program_id(0)
    bn = acc.shape[1]

    def moves(b):
        span = pl.ds(pl.multiple_of(b * bn, bn), bn)
        slot = lax.rem(b, 2)
        return [(pltpu.make_async_copy(src.at[span, :], ring.at[slot, i], load_sem.at[slot, i]),
                 pltpu.make_async_copy(ring.at[slot, i], dst.at[span, :], store_sem.at[slot, i]))
                for i, (src, dst) in enumerate(((p_ref, p_out), (q_ref, q_out)))]

    @pl.when(j >= 2)
    def _():
        for _, store in moves(j - 2):
            store.wait()

    @pl.when(j < nb)
    def _():
        for load, _ in moves(j):
            load.start()

    @pl.when((j >= 1) & (j <= nb))
    def _():
        for load, store in moves(j - 1):
            load.wait()
            store.start()

    def fin():
        def put(r, v):
            dpre[r:r + CHUNK, :] = v

        db, dg = finish_back(rows, acc, n1_ref, i1_ref[...], g1_ref[...], b1_ref[...], put)
        small_ref[0:1, :] = dg
        small_ref[1:2, :] = db
        small_ref[2:3, :] = dg2_ref[...]
        small_ref[3:4, :] = db2_ref[...]
        small_ref[4:5, :] = loss_ref[...]

    def mm():
        for r in range(0, rows, TILE):
            acc[r:r + TILE, :] = dot(x_ref[r:r + TILE, :], w2_ref[...], ((1,), (1,)))

    def dw():
        dw1_ref[...] = dot(featt[...], dpre[...])

    @pl.when(j < nb)
    def _():
        fin()
        mm()
        dw()

    @pl.when(j == nb)
    def _():
        fin()
        dw()


def back_c(x, featt, w2, n1, i1, g1, b1, dg2, db2, loss, p, q, bn=256):
    rows, d = x.shape
    k = featt.shape[0]
    nb = d // bn

    def at(first):
        return lambda j: (0, jnp.clip(j - first, 0, nb - 1))

    col = pl.BlockSpec((1, bn), at(1))
    row = pl.BlockSpec((bn, d), lambda j: (jnp.minimum(j, nb - 1), 0))
    any_spec = pl.BlockSpec(memory_space=pl.ANY)
    return pl.pallas_call(
        functools.partial(back_c_kernel, nb, rows),
        grid=(nb + 2,),
        in_specs=[pl.BlockSpec((rows, d), lambda j: (0, 0), pipeline_mode=ONCE), pl.BlockSpec((k, rows), lambda j: (0, 0), pipeline_mode=ONCE),
                  row, pl.BlockSpec((rows, bn), at(1)), col, col, col, col, col, pl.BlockSpec((1, bn), lambda j: (0, 0)), any_spec, any_spec],
        out_specs=[any_spec, any_spec, pl.BlockSpec((k, bn), at(1)), pl.BlockSpec((8, bn), at(1))],
        out_shape=[jax.ShapeDtypeStruct((d, d), F32)] * 2 + [jax.ShapeDtypeStruct((k, d), F32), jax.ShapeDtypeStruct((8, d), F32)],
        scratch_shapes=[pltpu.VMEM((rows, bn), F32), pltpu.VMEM((rows, bn), BF16), pltpu.VMEM((2, 2, bn, d), F32),
                        pltpu.SemaphoreType.DMA((2, 2)), pltpu.SemaphoreType.DMA((2, 2))],
        compiler_params=pltpu.CompilerParams(vmem_limit_bytes=VMEM_LIMIT),
        cost_estimate=pl.CostEstimate(flops=2 * rows * d * (k + d), bytes_accessed=rows * d * 20, transcendentals=0),
        name='back_c',
    )(x, featt, w2, n1, i1, g1, b1, dg2, db2, loss, p, q)


def solution(mesh):
    n = mesh.shape[AXIS]
    pair = [(i, i + 1 - 2 * (i % 2)) for i in range(n)]

    def swap(x):
        return lax.ppermute(x, AXIS, pair)

    def local_step(feat_a, feat_b, w_one, w_two, w_three, g_one, b_one, g_two, b_two, lam_off):
        width = w_two.shape[0]
        g1, b1, g2, b2 = (v.reshape(1, width) for v in (g_one, b_one, g_two, b_two))
        norm1, norm2, norm3, inv1, inv2, inv3, act1t, act2t, xt, emb, other = forward(
            feat_a, feat_b, w_one, w_two, w_three, g1, b1, g2, b2, n)
        loss, d_pre2, dg2, db2, dw3, dw2 = back_ab(
            lam_off.reshape(1, 1), emb, other, norm3, inv3, w_three, norm2, inv2, g2, b2, act2t, act1t)
        dw3, dw2, dw1, small = back_c(d_pre2, xt, w_two, norm1, inv1, g1, b1, dg2, db2, loss, dw3, dw2)
        dw1_other = swap(dw1)
        small = small + swap(small)
        dg1, db1, dg2, db2 = (small[i] for i in range(4))
        loss_val = jnp.sum(small[4, :loss.shape[1]]) * 0.5
        return (loss_val, dw1 + dw1_other, dw2, dw3, dg1, db1, dg2, db2)

    row_spec = P(AXIS, None)
    return jax.shard_map(local_step, mesh=mesh, in_specs=(row_spec, row_spec) + (P(),) * 8, out_specs=(P(),) * 8, check_vma=False)
```

```python
import functools

import jax
import jax.numpy as jnp
from jax import lax
from jax.experimental import pallas as pl
from jax.experimental.pallas import tpu as pltpu
from jax.sharding import PartitionSpec as P

NORM_EPS = 1e-5
AXIS = 'data'
MESH = pl.DeviceIdType.MESH
F32 = jnp.float32
BF16 = jnp.bfloat16
ONCE = pl.Buffered(1)
VMEM_LIMIT = 60 * 1024 * 1024
TILE = 256
CHUNK = 64


def fold(v):
    return jnp.sum(v.reshape(v.shape[0] // 8, 8, v.shape[1]), axis=0)


def dot(a, b, dims=((1,), (0,))):
    return lax.dot_general(a, b, (dims, ((), ())), preferred_element_type=F32)


def forward_kernel(nb, rows, fa_ref, fb_ref, w1_ref, w2_ref, w3_ref, g1_ref, b1_ref, g2_ref, b2_ref,
                   n1_hbm, n2_ref, n3_ref, i1_ref, i2_ref, i3_ref, t1_ref, t2_ref, xt_ref, emb_hbm, other_hbm,
                   xs, w1_buf, pre1, sums1, bufa, bufb, acc, w1_sem, norm_sem, copy_sem, feat_sem, send_sem, recv_sem, esend_sem, erecv_sem):
    j = pl.program_id(0)
    me = lax.axis_index(AXIS)
    core = lax.rem(me, 2)
    chip = me // 2
    x_pos, y_pos = lax.rem(chip, 2), chip // 2
    partner = me + 1 - 2 * core
    x_chip, y_chip = chip + 1 - 2 * x_pos, chip + 2 - 4 * y_pos
    piece = fa_ref.shape[0]
    bn = acc.shape[1]

    def remote(src, dst, send, recv, dev):
        return pltpu.make_async_remote_copy(src_ref=src, dst_ref=dst, send_sem=send, recv_sem=recv, device_id=(dev,), device_id_type=MESH)

    def part(dev):
        return xs.at[pl.ds(pl.multiple_of(dev * piece, piece), piece), :]

    def gather():
        pltpu.make_async_copy(w1_ref, w1_buf, w1_sem).start()
        barrier = pltpu.get_barrier_semaphore()
        for dev in (partner, 2 * x_chip, 2 * x_chip + 1, 2 * y_chip, 2 * y_chip + 1):
            pl.semaphore_signal(barrier, inc=1, device_id=(dev,), device_id_type=MESH)
        pl.semaphore_wait(barrier, 5)

        def sends(mine, mine_src, theirs_src):
            for view, src in ((mine, mine_src), (1 - mine, theirs_src)):
                remote(src, part(me), send_sem.at[1 + view], recv_sem.at[1 + mine], 2 * x_chip + view).start()
                remote(src, part(me), send_sem.at[3 + view], recv_sem.at[3 + mine], 2 * y_chip + view).start()
            remote(theirs_src, part(me), send_sem.at[0], recv_sem.at[0], partner).start()
            pltpu.make_async_copy(mine_src, part(me), feat_sem).start()

        pl.when(core == 0)(lambda: sends(0, fa_ref, fb_ref))
        pl.when(core == 1)(lambda: sends(1, fb_ref, fa_ref))
        remote(fa_ref, part(2 * x_chip), send_sem.at[1], recv_sem.at[1], me).wait_recv()
        relay_y = remote(part(2 * x_chip), part(2 * x_chip), send_sem.at[5], recv_sem.at[5], 2 * y_chip + core)
        relay_y.start()
        remote(fa_ref, part(2 * y_chip + 1), send_sem.at[4], recv_sem.at[4], me).wait_recv()
        relay_x = remote(part(2 * y_chip + 1), part(2 * y_chip + 1), send_sem.at[6], recv_sem.at[6], 2 * x_chip + core)
        relay_x.start()
        pltpu.make_async_copy(fa_ref, part(me), feat_sem).wait()
        remote(fa_ref, part(me), send_sem.at[0], recv_sem.at[0], me).wait()
        pltpu.make_async_copy(w1_ref, w1_buf, w1_sem).wait()
        layer_one(me, partner)
        layer_one(2 * x_chip, 2 * y_chip + 1)
        remote(fa_ref, part(me), send_sem.at[1], recv_sem.at[2], me).wait()
        remote(fa_ref, part(me), send_sem.at[2], recv_sem.at[3], me).wait()
        layer_one(2 * x_chip + 1, 2 * y_chip)
        remote(fa_ref, part(me), send_sem.at[3], recv_sem.at[5], me).wait()
        remote(fa_ref, part(me), send_sem.at[4], recv_sem.at[6], me).wait()
        far = 2 * (3 - chip)
        layer_one(far, far + 1)
        relay_y.wait_send()
        relay_x.wait_send()

    def layer_one(dev_p, dev_q):
        def work(i, carry):
            here = pl.ds(pl.multiple_of(jnp.where(i == 0, dev_p, dev_q) * piece, piece), piece)
            feats = xs[here, :]
            for c in range(0, w1_buf.shape[1], bn):
                pre = dot(feats, w1_buf[:, c:c + bn])
                pre1[here, c:c + bn] = pre
                sums1[0:8, c:c + bn] += fold(pre)
                sums1[8:16, c:c + bn] += fold(pre * pre)
            return carry

        lax.fori_loop(0, 2, work, 0)

    def norm_copy(block):
        cols = pl.ds(pl.multiple_of(block * bn, bn), bn)
        return pltpu.make_async_copy(pre1.at[:, cols], n1_hbm.at[:, cols], norm_sem.at[block])

    def finish_one():
        mean = jnp.sum(sums1[0:8, :], axis=0, keepdims=True) / rows
        inv = lax.rsqrt(jnp.sum(sums1[8:16, :], axis=0, keepdims=True) / rows - mean * mean + NORM_EPS)
        sums1[0:1, :] = mean
        i1_ref[...] = inv

        def work(block, carry):
            cols = pl.ds(pl.multiple_of(block * bn, bn), bn)
            mean, inv, g, b = sums1[0:1, cols], i1_ref[:, cols], g1_ref[:, cols], b1_ref[:, cols]
            for r in range(0, rows, CHUNK):
                norm = (pre1[r:r + CHUNK, cols] - mean) * inv
                pre1[r:r + CHUNK, cols] = norm
                bufa[r:r + CHUNK, cols] = jnp.maximum(norm * g + b, 0.0).astype(BF16)
            return carry

        lax.fori_loop(0, nb, work, 0)
        for block in range(nb):
            norm_copy(block).start()

    def fin(layer):
        norm_ref, inv_ref = ((n2_ref, i2_ref), (n3_ref, i3_ref))[layer]
        buf = (bufb, bufa)[layer]
        base = pl.multiple_of(jnp.maximum(j - 1 - layer * nb, 0) * bn, bn)
        total = jnp.zeros((8, bn), F32)
        square = jnp.zeros((8, bn), F32)
        for r in range(0, rows, CHUNK):
            pre = acc[r:r + CHUNK, :]
            total += fold(pre)
            square += fold(pre * pre)
        mean = jnp.sum(total, axis=0, keepdims=True) / rows
        inv = lax.rsqrt(jnp.sum(square, axis=0, keepdims=True) / rows - mean * mean + NORM_EPS)
        inv_ref[...] = inv
        if layer == 0:
            g, b = g2_ref[...], b2_ref[...]
        for r in range(0, rows, CHUNK):
            norm = (acc[r:r + CHUNK, :] - mean) * inv
            norm_ref[r:r + CHUNK, :] = norm
            if layer == 0:
                norm = jnp.maximum(norm * g + b, 0.0)
            buf[r:r + CHUNK, pl.ds(base, bn)] = norm.astype(BF16)
        if layer == 0:
            for r in range(0, rows, TILE):
                t2_ref[:, r:r + TILE] = buf[r:r + TILE, pl.ds(base, bn)].T

    def mm(layer):
        x_ref, w_ref = ((bufa, w2_ref), (bufb, w3_ref))[layer]
        for r in range(0, rows, TILE):
            acc[r:r + TILE, :] = dot(x_ref[r:r + TILE, :], w_ref[...])

    def out_copy(block):
        cols = pl.ds(pl.multiple_of(block * bn, bn), bn)
        return pltpu.make_async_copy(bufa.at[:, cols], emb_hbm.at[:, cols], copy_sem.at[block])

    def emb_copy(block):
        cols = pl.ds(pl.multiple_of(block * bn, bn), bn)
        return remote(bufa.at[:, cols], other_hbm.at[:, cols], esend_sem.at[block], erecv_sem.at[block], partner)

    @pl.when(j == 0)
    def _():
        sums1[...] = jnp.zeros_like(sums1)
        gather()
        finish_one()

    for layer in range(2):
        @pl.when((j >= layer * nb) & (j < (layer + 1) * nb))
        def _(layer=layer):
            fin(layer)
            mm(layer)
            if layer == 0:
                base = pl.multiple_of(j * bn, bn)
                for r in range(0, rows, TILE):
                    t1_ref[:, r:r + TILE] = bufa[r:r + TILE, pl.ds(base, bn)].T

        @pl.when(j == (layer + 1) * nb)
        def _(layer=layer):
            fin(layer)

    @pl.when(j >= nb + 2)
    def _():
        block = j - 2 - nb
        out_copy(block).start()
        emb_copy(block).start()

    @pl.when(j == nb + 1)
    def _():
        for r in range(0, rows, TILE):
            xt_ref[:, r:r + TILE] = xs[r:r + TILE, :].T

    @pl.when(j == 2 * nb + 1)
    def _():
        for block in range(nb):
            norm_copy(block).wait()
            out_copy(block).wait()
            emb_copy(block).wait()


def forward(fa, fb, w1, w2, w3, g1, b1, g2, b2, n, bn=256):
    piece, k = fa.shape
    rows, d = piece * n, w2.shape[1]
    nb = d // bn

    def at(layer, delay):
        return lambda j: (0, jnp.clip(j - layer * nb - delay, 0, nb - 1))

    whole = pl.BlockSpec((piece, k), lambda j: (0, 0), pipeline_mode=ONCE)
    any_spec = pl.BlockSpec(memory_space=pl.ANY)
    col = [pl.BlockSpec((1, bn), at(layer, 1)) for layer in range(2)]
    norm = [pl.BlockSpec((rows, bn), at(layer, 1)) for layer in range(2)]
    vec = pl.BlockSpec((1, d), lambda j: (0, 0))
    big = jax.ShapeDtypeStruct((rows, d), BF16)
    return pl.pallas_call(
        functools.partial(forward_kernel, nb, rows),
        grid=(2 * nb + 2,),
        in_specs=[whole, whole, any_spec, pl.BlockSpec((d, bn), at(0, 0)), pl.BlockSpec((d, bn), at(1, 0)),
                  vec, vec, col[0], col[0]],
        out_specs=[any_spec] + norm + [vec] + col + [pl.BlockSpec((bn, rows), lambda j, f=at(0, delay): f(j)[::-1]) for delay in range(2)]
        + [pl.BlockSpec((k, rows), lambda j: (0, 0), pipeline_mode=ONCE)] + [any_spec] * 2,
        out_shape=[jax.ShapeDtypeStruct((rows, d), F32)] * 3 + [jax.ShapeDtypeStruct((1, d), F32)] * 3
        + [jax.ShapeDtypeStruct((d, rows), BF16)] * 2 + [jax.ShapeDtypeStruct((k, rows), BF16)] + [big] * 2,
        scratch_shapes=[pltpu.VMEM((rows, k), BF16), pltpu.VMEM((k, d), BF16), pltpu.VMEM((rows, d), F32), pltpu.VMEM((16, d), F32),
                        pltpu.VMEM((rows, d), BF16), pltpu.VMEM((rows, d), BF16), pltpu.VMEM((rows, bn), F32), pltpu.SemaphoreType.DMA, pltpu.SemaphoreType.DMA((nb,)),
                        pltpu.SemaphoreType.DMA((nb,)), pltpu.SemaphoreType.DMA, pltpu.SemaphoreType.DMA((7,)), pltpu.SemaphoreType.DMA((7,)),
                        pltpu.SemaphoreType.DMA((nb,)), pltpu.SemaphoreType.DMA((nb,))],
        compiler_params=pltpu.CompilerParams(collective_id=0, has_side_effects=True, vmem_limit_bytes=63 * 1024 * 1024),
        cost_estimate=pl.CostEstimate(flops=2 * rows * d * (k + 2 * d), bytes_accessed=rows * d * 20, transcendentals=0),
        name='forward',
    )(fa, fb, w1, w2, w3, g1, b1, g2, b2)


def finish_back(rows, acc, norm_ref, inv, g, b, put):
    bn = acc.shape[1]
    total = jnp.zeros((8, bn), F32)
    cross = jnp.zeros((8, bn), F32)
    for r in range(0, rows, CHUNK):
        part = acc[r:r + CHUNK, :]
        norm = norm_ref[r:r + CHUNK, :]
        if b is not None:
            part = jnp.where(norm * g + b > 0.0, part, 0.0)
            acc[r:r + CHUNK, :] = part
        total += fold(part)
        cross += fold(part * norm)
    total = jnp.sum(total, axis=0, keepdims=True)
    cross = jnp.sum(cross, axis=0, keepdims=True)
    scale = inv if g is None else inv * g
    shift, slope = scale * (total / rows), scale * (cross / rows)
    for r in range(0, rows, CHUNK):
        put(r, (acc[r:r + CHUNK, :] * scale - shift - norm_ref[r:r + CHUNK, :] * slope).astype(BF16))
    return total, cross


def back_ab_kernel(nb, rows, lam_ref, own_ref, other_hbm, n3_ref, i3_ref, w3_ref, n2_ref, i2_ref, g2_ref, b2_ref, t2_ref, t1_hbm,
                   loss_ref, dpre_ref, dg_ref, db_ref, dw3_hbm, dw2_hbm,
                   big, corr, grad, acc, dout, send3, recv3, send2, recv2, load_sem, ssem, rsem, osem, free3, free2):
    j = pl.program_id(0)
    me = lax.axis_index(AXIS)
    partner = me + 1 - 2 * lax.rem(me, 2)
    bn = acc.shape[1]
    d = big.shape[1]
    lam = lam_ref[0, 0]
    other_ref = big

    def pair(e):
        return ((send3, recv3, free3, nb), (send2, recv2, free2, nb + 1))[e]

    def swap_copy(e, b, part=None):
        send, recv, _, _ = pair(e)
        src, dst = send.at[lax.rem(b, 2)], recv.at[lax.rem(b, 3)]
        if part is not None:
            src, dst = src.at[part, :], dst.at[part, :]
        return pltpu.make_async_remote_copy(
            src_ref=src, dst_ref=dst, send_sem=ssem.at[e, lax.rem(b, 2)],
            recv_sem=rsem.at[e, lax.rem(b, 3)], device_id=(partner,), device_id_type=MESH)

    def sum_copy(e, b):
        span = pl.ds(pl.multiple_of(b * bn, bn), bn)
        dst = dw3_hbm.at[span, :] if e == 0 else dw2_hbm.at[:, span]
        return pltpu.make_async_copy(pair(e)[1].at[lax.rem(b, 3)], dst, osem.at[e, lax.rem(b, 3)])

    def exchange(e):
        send, recv, free, first = pair(e)

        @pl.when((j >= first + 3) & (j < first + 3 + nb))
        def _():
            b = j - first - 3
            sum_copy(e, b).wait()

            @pl.when(b < nb - 3)
            def _():
                pl.semaphore_signal(free, inc=1, device_id=(partner,), device_id_type=MESH)

        @pl.when((j >= first + 2) & (j < first + 2 + nb))
        def _():
            b = j - first - 2
            swap_copy(e, b).wait()
            mine, theirs = lax.rem(b, 2), lax.rem(b, 3)
            for r in range(0, send.shape[1], send.shape[1] // 32):
                part = pl.ds(r, send.shape[1] // 32)
                recv[theirs, part, :] = recv[theirs, part, :] + send[mine, part, :]
            sum_copy(e, b).start()

    def ready(e, b):
        @pl.when(b >= 3)
        def _():
            pl.semaphore_wait(pair(e)[2], 1)

    def fin_loss():
        base = pl.multiple_of(jnp.maximum(j - 1, 0) * bn, bn)

        def put(r, v):
            dout[r:r + CHUNK, pl.ds(base, bn)] = v

        finish_back(rows, acc, n3_ref, i3_ref[...], None, None, put)

    def mm_loss():
        own = own_ref[...]
        loss = jnp.zeros((8, bn), F32)
        for c in range(0, d, bn):
            part = dot(own, other_ref[:, c:c + bn], ((0,), (0,))) * (1.0 / rows)
            corr[:, c:c + bn] = part
            loss += fold(part * part)
            grad[:, c:c + bn] = ((2.0 * lam) * part).astype(BF16)
        here = pl.ds(pl.multiple_of(j * bn, bn), bn)
        part = corr[:, here]
        diag = lax.broadcasted_iota(jnp.int32, (bn, bn), 0) == lax.broadcasted_iota(jnp.int32, (bn, bn), 1)
        grad[:, here] = jnp.where(diag, -2.0 * (1.0 - part), (2.0 * lam) * part).astype(BF16)
        loss = lam * loss + fold(jnp.where(diag, (1.0 - part) * (1.0 - part) - lam * (part * part), 0.0))
        loss_ref[...] += jnp.sum(loss, axis=0, keepdims=True)
        for r in range(0, rows, TILE):
            acc[r:r + TILE, :] = dot(other_ref[r:r + TILE, :], grad[...], ((1,), (1,))) * (1.0 / rows)

    def fin_two():
        def put(r, v):
            dpre_ref[r:r + CHUNK, :] = v

        db_ref[...], dg_ref[...] = finish_back(rows, acc, n2_ref, i2_ref[...], g2_ref[...], b2_ref[...], put)

    def mm_two():
        for r in range(0, rows, TILE):
            acc[r:r + TILE, :] = dot(dout[r:r + TILE, :], w3_ref[...], ((1,), (1,)))
        act = t2_ref[...]
        slot = lax.rem(j - nb, 2)
        for c in range(0, d, 2 * bn):
            send3[slot, :, c:c + 2 * bn] = dot(act, dout[:, c:c + 2 * bn])

    def mm_dw2(first, last):
        slot = lax.rem(j - nb - 1, 2)
        for r in range(first, last, TILE):
            send2[slot, r:r + TILE, :] = dot(big[r:r + TILE, :], dpre_ref[...])

    @pl.when(j == 0)
    def _():
        load = pltpu.make_async_copy(other_hbm, big, load_sem)
        load.start()
        loss_ref[...] = jnp.zeros_like(loss_ref)
        barrier = pltpu.get_barrier_semaphore()
        pl.semaphore_signal(barrier, inc=1, device_id=(partner,), device_id_type=MESH)
        pl.semaphore_wait(barrier, 1)
        load.wait()

    @pl.when(j == nb)
    def _():
        pltpu.make_async_copy(t1_hbm, big, load_sem).start()

    exchange(0)
    exchange(1)

    @pl.when(j < nb)
    def _():
        fin_loss()
        mm_loss()

    @pl.when(j == nb)
    def _():
        fin_loss()

    @pl.when((j >= nb) & (j < 2 * nb))
    def _():
        fin_two()
        mm_two()
        ready(0, j - nb)
        swap_copy(0, j - nb).start()

    @pl.when(j == 2 * nb)
    def _():
        fin_two()

    @pl.when(j == nb + 1)
    def _():
        pltpu.make_async_copy(t1_hbm, big, load_sem).wait()

    @pl.when((j > nb) & (j < 2 * nb))
    def _():
        mm_dw2(0, d)
        ready(1, j - nb - 1)
        swap_copy(1, j - nb - 1).start()

    @pl.when(j == 2 * nb)
    def _():
        ready(1, nb - 1)
        for r in range(0, d, d // 4):
            mm_dw2(r, r + d // 4)
            swap_copy(1, nb - 1, pl.ds(r, d // 4)).start()


def back_ab(lam, own, other, n3, i3, w3, n2, i2, g2, b2, t2, t1, bn=256):
    rows, d = own.shape
    nb = d // bn

    def at(first):
        return lambda j: (0, jnp.clip(j - first, 0, nb - 1))

    def block(first):
        return pl.BlockSpec((rows, bn), at(first))

    def col(first):
        return pl.BlockSpec((1, bn), at(first))

    row = pl.BlockSpec((bn, d), lambda j: (jnp.clip(j - nb, 0, nb - 1), 0))
    vec = jax.ShapeDtypeStruct((1, d), F32)
    any_spec = pl.BlockSpec(memory_space=pl.ANY)
    return pl.pallas_call(
        functools.partial(back_ab_kernel, nb, rows),
        grid=(2 * nb + 4,),
        in_specs=[pl.BlockSpec(memory_space=pltpu.SMEM), block(0), any_spec,
                  block(1), col(1), row, block(nb + 1), col(nb + 1), col(nb + 1), col(nb + 1), row, any_spec],
        out_specs=[pl.BlockSpec((1, bn), lambda j: (0, 0)), block(nb + 1), col(nb + 1), col(nb + 1), any_spec, any_spec],
        out_shape=[jax.ShapeDtypeStruct((1, bn), F32), jax.ShapeDtypeStruct((rows, d), BF16), vec, vec]
        + [jax.ShapeDtypeStruct((d, d), F32)] * 2,
        scratch_shapes=[pltpu.VMEM((rows, d), BF16), pltpu.VMEM((bn, d), F32), pltpu.VMEM((bn, d), BF16), pltpu.VMEM((rows, bn), F32),
                        pltpu.VMEM((rows, d), BF16), pltpu.VMEM((2, bn, d), F32), pltpu.VMEM((3, bn, d), F32),
                        pltpu.VMEM((2, d, bn), F32), pltpu.VMEM((3, d, bn), F32), pltpu.SemaphoreType.DMA,
                        pltpu.SemaphoreType.DMA((2, 2)), pltpu.SemaphoreType.DMA((2, 3)), pltpu.SemaphoreType.DMA((2, 3)),
                        pltpu.SemaphoreType.REGULAR, pltpu.SemaphoreType.REGULAR],
        compiler_params=pltpu.CompilerParams(collective_id=1, has_side_effects=True, vmem_limit_bytes=63 * 1024 * 1024),
        cost_estimate=pl.CostEstimate(flops=10 * rows * d * d, bytes_accessed=rows * d * 24, transcendentals=0),
        name='back_ab',
    )(lam, own, other, n3, i3, w3, n2, i2, g2, b2, t2, t1)


def back_c_kernel(nb, rows, x_ref, featt, w2_ref, n1_ref, i1_ref, g1_ref, b1_ref, dg2_ref, db2_ref, loss_ref, p_ref, q_ref,
                  p_out, q_out, dw1a_ref, dw1b_ref, acc, dpre, ring, load_sem, store_sem):
    j = pl.program_id(0)
    bn = acc.shape[1]

    def moves(b):
        span = pl.ds(pl.multiple_of(b * bn, bn), bn)
        slot = lax.rem(b, 2)
        return [(pltpu.make_async_copy(src.at[span, :], ring.at[slot, i], load_sem.at[slot, i]),
                 pltpu.make_async_copy(ring.at[slot, i], dst.at[span, :], store_sem.at[slot, i]))
                for i, (src, dst) in enumerate(((p_ref, p_out), (q_ref, q_out)))]

    @pl.when(j >= 2)
    def _():
        for _, store in moves(j - 2):
            store.wait()

    @pl.when(j < nb)
    def _():
        for load, _ in moves(j):
            load.start()

    @pl.when((j >= 1) & (j <= nb))
    def _():
        for load, store in moves(j - 1):
            load.wait()
            store.start()

    def fin():
        def put(r, v):
            dpre[r:r + CHUNK, :] = v

        db, dg = finish_back(rows, acc, n1_ref, i1_ref[...], g1_ref[...], b1_ref[...], put)
        half = dw1b_ref.shape[0]
        for i, row in enumerate((dg, db, dg2_ref[...], db2_ref[...], loss_ref[...])):
            dw1a_ref[half + i:half + i + 1, :] = row

    def mm():
        for r in range(0, rows, TILE):
            acc[r:r + TILE, :] = dot(x_ref[r:r + TILE, :], w2_ref[...], ((1,), (1,)))

    def dw():
        half = dw1b_ref.shape[0]
        dw1a_ref[:half, :] = dot(featt[:half, :], dpre[...])
        dw1b_ref[...] = dot(featt[half:, :], dpre[...])

    @pl.when(j < nb)
    def _():
        fin()
        mm()
        dw()

    @pl.when(j == nb)
    def _():
        fin()
        dw()


def back_c(x, featt, w2, n1, i1, g1, b1, dg2, db2, loss, p, q, bn=256):
    rows, d = x.shape
    k = featt.shape[0]
    nb = d // bn

    def at(first):
        return lambda j: (0, jnp.clip(j - first, 0, nb - 1))

    col = pl.BlockSpec((1, bn), at(1))
    row = pl.BlockSpec((bn, d), lambda j: (jnp.minimum(j, nb - 1), 0))
    any_spec = pl.BlockSpec(memory_space=pl.ANY)
    return pl.pallas_call(
        functools.partial(back_c_kernel, nb, rows),
        grid=(nb + 2,),
        in_specs=[pl.BlockSpec((rows, d), lambda j: (0, 0), pipeline_mode=ONCE), pl.BlockSpec((k, rows), lambda j: (0, 0), pipeline_mode=ONCE),
                  row, pl.BlockSpec((rows, bn), at(1)), col, col, col, col, col, pl.BlockSpec((1, bn), lambda j: (0, 0)), any_spec, any_spec],
        out_specs=[any_spec, any_spec, pl.BlockSpec((k // 2 + 8, bn), at(1)), pl.BlockSpec((k // 2, bn), at(1))],
        out_shape=[jax.ShapeDtypeStruct((d, d), F32)] * 2 + [jax.ShapeDtypeStruct((k // 2 + 8, d), F32), jax.ShapeDtypeStruct((k // 2, d), F32)],
        scratch_shapes=[pltpu.VMEM((rows, bn), F32), pltpu.VMEM((rows, bn), BF16), pltpu.VMEM((2, 2, bn, d), F32),
                        pltpu.SemaphoreType.DMA((2, 2)), pltpu.SemaphoreType.DMA((2, 2))],
        compiler_params=pltpu.CompilerParams(vmem_limit_bytes=VMEM_LIMIT),
        cost_estimate=pl.CostEstimate(flops=2 * rows * d * (k + d), bytes_accessed=rows * d * 20, transcendentals=0),
        name='back_c',
    )(x, featt, w2, n1, i1, g1, b1, dg2, db2, loss, p, q)


def add_first_kernel(p_ref, q_ref, out_ref, small_ref):
    half = out_ref.shape[0]
    out_ref[...] = p_ref[:half, :] + q_ref[:half, :]
    small_ref[...] = p_ref[half:, :] + q_ref[half:, :]


def add_second_kernel(p_ref, q_ref, _, out_ref):
    out_ref[...] = p_ref[...] + q_ref[...]


def add_half(p, q, half, whole=None):
    rows, d = p.shape
    blk = d // 2
    spec = pl.BlockSpec((rows, blk), lambda j: (0, j))
    first = whole is None
    out_specs = [pl.BlockSpec((half, blk), lambda j: (0 if first else 1, j))]
    out_shape = [jax.ShapeDtypeStruct((2 * half, d), F32)]
    if first:
        out_specs.append(pl.BlockSpec((rows - half, blk), lambda j: (0, j)))
        out_shape.append(jax.ShapeDtypeStruct((rows - half, d), F32))
    return pl.pallas_call(
        add_first_kernel if first else add_second_kernel,
        grid=(2,),
        in_specs=[spec, spec] + ([] if first else [pl.BlockSpec(memory_space=pl.ANY)]),
        out_specs=out_specs,
        out_shape=out_shape,
        input_output_aliases={} if first else {2: 0},
        compiler_params=pltpu.CompilerParams(vmem_limit_bytes=24 * 1024 * 1024),
        cost_estimate=pl.CostEstimate(flops=rows * d * 2000, bytes_accessed=rows * d * 12, transcendentals=0),
        name='add_half',
    )(*([p, q] if first else [p, q, whole]))


def solution(mesh):
    n = mesh.shape[AXIS]
    pair = [(i, i + 1 - 2 * (i % 2)) for i in range(n)]

    def swap(x):
        return lax.ppermute(x, AXIS, pair)

    def local_step(feat_a, feat_b, w_one, w_two, w_three, g_one, b_one, g_two, b_two, lam_off):
        width = w_two.shape[0]
        g1, b1, g2, b2 = (v.reshape(1, width) for v in (g_one, b_one, g_two, b_two))
        norm1, norm2, norm3, inv1, inv2, inv3, act1t, act2t, xt, emb, other = forward(
            feat_a, feat_b, w_one, w_two, w_three, g1, b1, g2, b2, n)
        loss, d_pre2, dg2, db2, dw3, dw2 = back_ab(
            lam_off.reshape(1, 1), emb, other, norm3, inv3, w_three, norm2, inv2, g2, b2, act2t, act1t)
        dw3, dw2, dw1a, dw1b = back_c(d_pre2, xt, w_two, norm1, inv1, g1, b1, dg2, db2, loss, dw3, dw2)
        half = dw1b.shape[0]
        dw1, small = add_half(dw1a, swap(dw1a), half)
        dw1, = add_half(dw1b, swap(dw1b), half, dw1)
        dg1, db1, dg2, db2 = (small[i] for i in range(4))
        loss_val = jnp.sum(small[4, :loss.shape[1]]) * 0.5
        return (loss_val, dw1, dw2, dw3, dg1, db1, dg2, db2)

    row_spec = P(AXIS, None)
    return jax.shard_map(local_step, mesh=mesh, in_specs=(row_spec, row_spec) + (P(),) * 8, out_specs=(P(),) * 8, check_vma=False)
```

```python
import functools

import jax
import jax.numpy as jnp
from jax import lax
from jax.experimental import pallas as pl
from jax.experimental.pallas import tpu as pltpu
from jax.sharding import PartitionSpec as P

NORM_EPS = 1e-5
AXIS = 'data'
MESH = pl.DeviceIdType.MESH
F32 = jnp.float32
BF16 = jnp.bfloat16
ONCE = pl.Buffered(1)
VMEM_LIMIT = 60 * 1024 * 1024
TILE = 256
CHUNK = 64


def fold(v):
    return jnp.sum(v.reshape(v.shape[0] // 8, 8, v.shape[1]), axis=0)


def dot(a, b, dims=((1,), (0,))):
    return lax.dot_general(a, b, (dims, ((), ())), preferred_element_type=F32)


def forward_kernel(nb, rows, fa_ref, fb_ref, w1_ref, w2_ref, w3_ref, g1_ref, b1_ref, g2_ref, b2_ref,
                   n1_hbm, n2_ref, n3_ref, i1_ref, i2_ref, i3_ref, t1_ref, t2_ref, xt_ref, emb_hbm, other_hbm,
                   xs, w1_buf, pre1, sums1, bufa, bufb, acc, w1_sem, norm_sem, copy_sem, feat_sem, send_sem, recv_sem, esend_sem, erecv_sem):
    j = pl.program_id(0)
    me = lax.axis_index(AXIS)
    core = lax.rem(me, 2)
    chip = me // 2
    x_pos, y_pos = lax.rem(chip, 2), chip // 2
    partner = me + 1 - 2 * core
    x_chip, y_chip = chip + 1 - 2 * x_pos, chip + 2 - 4 * y_pos
    piece = fa_ref.shape[0]
    bn = acc.shape[1]

    def remote(src, dst, send, recv, dev):
        return pltpu.make_async_remote_copy(src_ref=src, dst_ref=dst, send_sem=send, recv_sem=recv, device_id=(dev,), device_id_type=MESH)

    def part(dev):
        return xs.at[pl.ds(pl.multiple_of(dev * piece, piece), piece), :]

    def gather():
        pltpu.make_async_copy(w1_ref, w1_buf, w1_sem).start()
        barrier = pltpu.get_barrier_semaphore()
        for dev in (partner, 2 * x_chip, 2 * x_chip + 1, 2 * y_chip, 2 * y_chip + 1):
            pl.semaphore_signal(barrier, inc=1, device_id=(dev,), device_id_type=MESH)
        pl.semaphore_wait(barrier, 5)

        def sends(mine, mine_src, theirs_src):
            for view, src in ((mine, mine_src), (1 - mine, theirs_src)):
                remote(src, part(me), send_sem.at[1 + view], recv_sem.at[1 + mine], 2 * x_chip + view).start()
                remote(src, part(me), send_sem.at[3 + view], recv_sem.at[3 + mine], 2 * y_chip + view).start()
            remote(theirs_src, part(me), send_sem.at[0], recv_sem.at[0], partner).start()
            pltpu.make_async_copy(mine_src, part(me), feat_sem).start()

        pl.when(core == 0)(lambda: sends(0, fa_ref, fb_ref))
        pl.when(core == 1)(lambda: sends(1, fb_ref, fa_ref))
        remote(fa_ref, part(2 * x_chip), send_sem.at[1], recv_sem.at[1], me).wait_recv()
        relay_y = remote(part(2 * x_chip), part(2 * x_chip), send_sem.at[5], recv_sem.at[5], 2 * y_chip + core)
        relay_y.start()
        remote(fa_ref, part(2 * y_chip + 1), send_sem.at[4], recv_sem.at[4], me).wait_recv()
        relay_x = remote(part(2 * y_chip + 1), part(2 * y_chip + 1), send_sem.at[6], recv_sem.at[6], 2 * x_chip + core)
        relay_x.start()
        pltpu.make_async_copy(fa_ref, part(me), feat_sem).wait()
        remote(fa_ref, part(me), send_sem.at[0], recv_sem.at[0], me).wait()
        pltpu.make_async_copy(w1_ref, w1_buf, w1_sem).wait()
        layer_one(me, partner)
        layer_one(2 * x_chip, 2 * y_chip + 1)
        remote(fa_ref, part(me), send_sem.at[1], recv_sem.at[2], me).wait()
        remote(fa_ref, part(me), send_sem.at[2], recv_sem.at[3], me).wait()
        layer_one(2 * x_chip + 1, 2 * y_chip)
        remote(fa_ref, part(me), send_sem.at[3], recv_sem.at[5], me).wait()
        remote(fa_ref, part(me), send_sem.at[4], recv_sem.at[6], me).wait()
        far = 2 * (3 - chip)
        layer_one(far, far + 1)
        relay_y.wait_send()
        relay_x.wait_send()

    def layer_one(dev_p, dev_q):
        def work(i, carry):
            here = pl.ds(pl.multiple_of(jnp.where(i == 0, dev_p, dev_q) * piece, piece), piece)
            feats = xs[here, :]
            for c in range(0, w1_buf.shape[1], bn):
                pre = dot(feats, w1_buf[:, c:c + bn])
                pre1[here, c:c + bn] = pre
                sums1[0:8, c:c + bn] += fold(pre)
                sums1[8:16, c:c + bn] += fold(pre * pre)
            return carry

        lax.fori_loop(0, 2, work, 0)

    def norm_copy(block):
        cols = pl.ds(pl.multiple_of(block * bn, bn), bn)
        return pltpu.make_async_copy(pre1.at[:, cols], n1_hbm.at[:, cols], norm_sem.at[block])

    def finish_one():
        mean = jnp.sum(sums1[0:8, :], axis=0, keepdims=True) / rows
        inv = lax.rsqrt(jnp.sum(sums1[8:16, :], axis=0, keepdims=True) / rows - mean * mean + NORM_EPS)
        sums1[0:1, :] = mean
        i1_ref[...] = inv

        def work(block, carry):
            cols = pl.ds(pl.multiple_of(block * bn, bn), bn)
            mean, inv, g, b = sums1[0:1, cols], i1_ref[:, cols], g1_ref[:, cols], b1_ref[:, cols]
            for r in range(0, rows, CHUNK):
                norm = (pre1[r:r + CHUNK, cols] - mean) * inv
                pre1[r:r + CHUNK, cols] = norm
                bufa[r:r + CHUNK, cols] = jnp.maximum(norm * g + b, 0.0).astype(BF16)
            return carry

        lax.fori_loop(0, nb, work, 0)
        for block in range(nb):
            norm_copy(block).start()

    def fin(layer):
        norm_ref, inv_ref = ((n2_ref, i2_ref), (n3_ref, i3_ref))[layer]
        buf = (bufb, bufa)[layer]
        base = pl.multiple_of(jnp.maximum(j - 1 - layer * nb, 0) * bn, bn)
        total = jnp.zeros((8, bn), F32)
        square = jnp.zeros((8, bn), F32)
        for r in range(0, rows, CHUNK):
            pre = acc[r:r + CHUNK, :]
            total += fold(pre)
            square += fold(pre * pre)
        mean = jnp.sum(total, axis=0, keepdims=True) / rows
        inv = lax.rsqrt(jnp.sum(square, axis=0, keepdims=True) / rows - mean * mean + NORM_EPS)
        inv_ref[...] = inv
        if layer == 0:
            g, b = g2_ref[...], b2_ref[...]
        for r in range(0, rows, CHUNK):
            norm = (acc[r:r + CHUNK, :] - mean) * inv
            norm_ref[r:r + CHUNK, :] = norm
            if layer == 0:
                norm = jnp.maximum(norm * g + b, 0.0)
            buf[r:r + CHUNK, pl.ds(base, bn)] = norm.astype(BF16)
        if layer == 0:
            for r in range(0, rows, TILE):
                t2_ref[:, r:r + TILE] = buf[r:r + TILE, pl.ds(base, bn)].T

    def mm(layer):
        x_ref, w_ref = ((bufa, w2_ref), (bufb, w3_ref))[layer]
        for r in range(0, rows, TILE):
            acc[r:r + TILE, :] = dot(x_ref[r:r + TILE, :], w_ref[...])

    def out_copy(block):
        cols = pl.ds(pl.multiple_of(block * bn, bn), bn)
        return pltpu.make_async_copy(bufa.at[:, cols], emb_hbm.at[:, cols], copy_sem.at[block])

    def emb_copy(block):
        cols = pl.ds(pl.multiple_of(block * bn, bn), bn)
        return remote(bufa.at[:, cols], other_hbm.at[:, cols], esend_sem.at[block], erecv_sem.at[block], partner)

    @pl.when(j == 0)
    def _():
        sums1[...] = jnp.zeros_like(sums1)
        gather()
        finish_one()

    for layer in range(2):
        @pl.when((j >= layer * nb) & (j < (layer + 1) * nb))
        def _(layer=layer):
            fin(layer)
            mm(layer)
            if layer == 0:
                base = pl.multiple_of(j * bn, bn)
                for r in range(0, rows, TILE):
                    t1_ref[:, r:r + TILE] = bufa[r:r + TILE, pl.ds(base, bn)].T

        @pl.when(j == (layer + 1) * nb)
        def _(layer=layer):
            fin(layer)

    @pl.when(j >= nb + 2)
    def _():
        block = j - 2 - nb
        out_copy(block).start()
        emb_copy(block).start()

    @pl.when(j == nb + 1)
    def _():
        for r in range(0, rows, TILE):
            xt_ref[:, r:r + TILE] = xs[r:r + TILE, :].T

    @pl.when(j == 2 * nb + 1)
    def _():
        for block in range(nb):
            norm_copy(block).wait()
            out_copy(block).wait()
            emb_copy(block).wait()


def forward(fa, fb, w1, w2, w3, g1, b1, g2, b2, n, bn=256):
    piece, k = fa.shape
    rows, d = piece * n, w2.shape[1]
    nb = d // bn

    def at(layer, delay):
        return lambda j: (0, jnp.clip(j - layer * nb - delay, 0, nb - 1))

    whole = pl.BlockSpec((piece, k), lambda j: (0, 0), pipeline_mode=ONCE)
    any_spec = pl.BlockSpec(memory_space=pl.ANY)
    col = [pl.BlockSpec((1, bn), at(layer, 1)) for layer in range(2)]
    norm = [pl.BlockSpec((rows, bn), at(layer, 1)) for layer in range(2)]
    vec = pl.BlockSpec((1, d), lambda j: (0, 0))
    big = jax.ShapeDtypeStruct((rows, d), BF16)
    return pl.pallas_call(
        functools.partial(forward_kernel, nb, rows),
        grid=(2 * nb + 2,),
        in_specs=[whole, whole, any_spec, pl.BlockSpec((d, bn), at(0, 0)), pl.BlockSpec((d, bn), at(1, 0)),
                  vec, vec, col[0], col[0]],
        out_specs=[any_spec] + norm + [vec] + col + [pl.BlockSpec((bn, rows), lambda j, f=at(0, delay): f(j)[::-1]) for delay in range(2)]
        + [pl.BlockSpec((k, rows), lambda j: (0, 0), pipeline_mode=ONCE)] + [any_spec] * 2,
        out_shape=[jax.ShapeDtypeStruct((rows, d), F32)] * 3 + [jax.ShapeDtypeStruct((1, d), F32)] * 3
        + [jax.ShapeDtypeStruct((d, rows), BF16)] * 2 + [jax.ShapeDtypeStruct((k, rows), BF16)] + [big] * 2,
        scratch_shapes=[pltpu.VMEM((rows, k), BF16), pltpu.VMEM((k, d), BF16), pltpu.VMEM((rows, d), F32), pltpu.VMEM((16, d), F32),
                        pltpu.VMEM((rows, d), BF16), pltpu.VMEM((rows, d), BF16), pltpu.VMEM((rows, bn), F32), pltpu.SemaphoreType.DMA, pltpu.SemaphoreType.DMA((nb,)),
                        pltpu.SemaphoreType.DMA((nb,)), pltpu.SemaphoreType.DMA, pltpu.SemaphoreType.DMA((7,)), pltpu.SemaphoreType.DMA((7,)),
                        pltpu.SemaphoreType.DMA((nb,)), pltpu.SemaphoreType.DMA((nb,))],
        compiler_params=pltpu.CompilerParams(collective_id=0, has_side_effects=True, vmem_limit_bytes=63 * 1024 * 1024),
        cost_estimate=pl.CostEstimate(flops=2 * rows * d * (k + 2 * d), bytes_accessed=rows * d * 20, transcendentals=0),
        name='forward',
    )(fa, fb, w1, w2, w3, g1, b1, g2, b2)


def finish_back(rows, acc, norm_ref, inv, g, b, put):
    bn = acc.shape[1]
    total = jnp.zeros((8, bn), F32)
    cross = jnp.zeros((8, bn), F32)
    for r in range(0, rows, CHUNK):
        part = acc[r:r + CHUNK, :]
        norm = norm_ref[r:r + CHUNK, :]
        if b is not None:
            part = jnp.where(norm * g + b > 0.0, part, 0.0)
            acc[r:r + CHUNK, :] = part
        total += fold(part)
        cross += fold(part * norm)
    total = jnp.sum(total, axis=0, keepdims=True)
    cross = jnp.sum(cross, axis=0, keepdims=True)
    scale = inv if g is None else inv * g
    shift, slope = scale * (total / rows), scale * (cross / rows)
    for r in range(0, rows, CHUNK):
        put(r, (acc[r:r + CHUNK, :] * scale - shift - norm_ref[r:r + CHUNK, :] * slope).astype(BF16))
    return total, cross


def back_ab_kernel(nb, rows, lam_ref, own_ref, other_hbm, n3_ref, i3_ref, w3_ref, n2_ref, i2_ref, g2_ref, b2_ref, t2_ref, t1_hbm,
                   loss_ref, dpre_ref, dg_ref, db_ref, dw3_hbm, dw2_hbm,
                   big, corr, grad, acc, dout, send3, recv3, send2, recv2, load_sem, chunk_sem, ssem, rsem, osem, free3, free2):
    j = pl.program_id(0)
    me = lax.axis_index(AXIS)
    partner = me + 1 - 2 * lax.rem(me, 2)
    bn = acc.shape[1]
    d = big.shape[1]
    lam = lam_ref[0, 0]
    other_ref = big

    def pair(e):
        return ((send3, recv3, free3, nb), (send2, recv2, free2, nb + 1))[e]

    def swap_copy(e, b, part=None):
        send, recv, _, _ = pair(e)
        src, dst = send.at[lax.rem(b, 2)], recv.at[lax.rem(b, 3)]
        if part is not None:
            src, dst = src.at[part, :], dst.at[part, :]
        return pltpu.make_async_remote_copy(
            src_ref=src, dst_ref=dst, send_sem=ssem.at[e, lax.rem(b, 2)],
            recv_sem=rsem.at[e, lax.rem(b, 3)], device_id=(partner,), device_id_type=MESH)

    def sum_copy(e, b):
        span = pl.ds(pl.multiple_of(b * bn, bn), bn)
        dst = dw3_hbm.at[span, :] if e == 0 else dw2_hbm.at[:, span]
        return pltpu.make_async_copy(pair(e)[1].at[lax.rem(b, 3)], dst, osem.at[e, lax.rem(b, 3)])

    def exchange(e):
        send, recv, free, first = pair(e)

        @pl.when((j >= first + 3) & (j < first + 3 + nb))
        def _():
            b = j - first - 3
            sum_copy(e, b).wait()

            @pl.when(b < nb - 3)
            def _():
                pl.semaphore_signal(free, inc=1, device_id=(partner,), device_id_type=MESH)

        @pl.when((j >= first + 2) & (j < first + 2 + nb))
        def _():
            b = j - first - 2
            swap_copy(e, b).wait()
            mine, theirs = lax.rem(b, 2), lax.rem(b, 3)
            for r in range(0, send.shape[1], send.shape[1] // 32):
                part = pl.ds(r, send.shape[1] // 32)
                recv[theirs, part, :] = recv[theirs, part, :] + send[mine, part, :]
            sum_copy(e, b).start()

    def ready(e, b):
        @pl.when(b >= 3)
        def _():
            pl.semaphore_wait(pair(e)[2], 1)

    def fin_loss():
        base = pl.multiple_of(jnp.maximum(j - 1, 0) * bn, bn)

        def put(r, v):
            dout[r:r + CHUNK, pl.ds(base, bn)] = v

        finish_back(rows, acc, n3_ref, i3_ref[...], None, None, put)

    def load_other(c):
        cols = pl.ds(pl.multiple_of(c * bn, bn), bn)
        return pltpu.make_async_copy(other_hbm.at[:, cols], big.at[:, cols], chunk_sem.at[c])

    def mm_loss(arriving):
        own = own_ref[...]

        def correlate(c, loss):
            cols = pl.ds(pl.multiple_of(c * bn, bn), bn)
            if arriving:
                load_other(c).wait()
            part = dot(own, other_ref[:, cols], ((0,), (0,))) * (1.0 / rows)
            corr[:, cols] = part
            grad[:, cols] = ((2.0 * lam) * part).astype(BF16)
            return loss + fold(part * part)

        loss = jnp.zeros((8, bn), F32)
        if arriving:
            loss = lax.fori_loop(0, nb, correlate, loss)
        else:
            for c in range(nb):
                loss = correlate(c, loss)
        here = pl.ds(pl.multiple_of(j * bn, bn), bn)
        part = corr[:, here]
        diag = lax.broadcasted_iota(jnp.int32, (bn, bn), 0) == lax.broadcasted_iota(jnp.int32, (bn, bn), 1)
        grad[:, here] = jnp.where(diag, -2.0 * (1.0 - part), (2.0 * lam) * part).astype(BF16)
        loss = lam * loss + fold(jnp.where(diag, (1.0 - part) * (1.0 - part) - lam * (part * part), 0.0))
        loss_ref[...] += jnp.sum(loss, axis=0, keepdims=True)
        for r in range(0, rows, TILE):
            acc[r:r + TILE, :] = dot(other_ref[r:r + TILE, :], grad[...], ((1,), (1,))) * (1.0 / rows)

    def fin_two():
        def put(r, v):
            dpre_ref[r:r + CHUNK, :] = v

        db_ref[...], dg_ref[...] = finish_back(rows, acc, n2_ref, i2_ref[...], g2_ref[...], b2_ref[...], put)

    def mm_two():
        for r in range(0, rows, TILE):
            acc[r:r + TILE, :] = dot(dout[r:r + TILE, :], w3_ref[...], ((1,), (1,)))
        act = t2_ref[...]
        slot = lax.rem(j - nb, 2)
        for c in range(0, d, 2 * bn):
            send3[slot, :, c:c + 2 * bn] = dot(act, dout[:, c:c + 2 * bn])

    def mm_dw2(first, last):
        slot = lax.rem(j - nb - 1, 2)
        for r in range(first, last, TILE):
            send2[slot, r:r + TILE, :] = dot(big[r:r + TILE, :], dpre_ref[...])

    @pl.when(j == 0)
    def _():
        for c in range(nb):
            load_other(c).start()
        loss_ref[...] = jnp.zeros_like(loss_ref)
        barrier = pltpu.get_barrier_semaphore()
        pl.semaphore_signal(barrier, inc=1, device_id=(partner,), device_id_type=MESH)
        pl.semaphore_wait(barrier, 1)
        mm_loss(True)

    @pl.when(j == nb)
    def _():
        pltpu.make_async_copy(t1_hbm, big, load_sem).start()

    exchange(0)
    exchange(1)

    @pl.when((j > 0) & (j < nb))
    def _():
        fin_loss()
        mm_loss(False)

    @pl.when(j == nb)
    def _():
        fin_loss()

    @pl.when((j >= nb) & (j < 2 * nb))
    def _():
        fin_two()
        mm_two()
        ready(0, j - nb)
        swap_copy(0, j - nb).start()

    @pl.when(j == 2 * nb)
    def _():
        fin_two()

    @pl.when(j == nb + 1)
    def _():
        pltpu.make_async_copy(t1_hbm, big, load_sem).wait()

    @pl.when((j > nb) & (j < 2 * nb))
    def _():
        mm_dw2(0, d)
        ready(1, j - nb - 1)
        swap_copy(1, j - nb - 1).start()

    @pl.when(j == 2 * nb)
    def _():
        ready(1, nb - 1)
        for r in range(0, d, d // 4):
            mm_dw2(r, r + d // 4)
            swap_copy(1, nb - 1, pl.ds(r, d // 4)).start()


def back_ab(lam, own, other, n3, i3, w3, n2, i2, g2, b2, t2, t1, bn=256):
    rows, d = own.shape
    nb = d // bn

    def at(first):
        return lambda j: (0, jnp.clip(j - first, 0, nb - 1))

    def block(first):
        return pl.BlockSpec((rows, bn), at(first))

    def col(first):
        return pl.BlockSpec((1, bn), at(first))

    row = pl.BlockSpec((bn, d), lambda j: (jnp.clip(j - nb, 0, nb - 1), 0))
    vec = jax.ShapeDtypeStruct((1, d), F32)
    any_spec = pl.BlockSpec(memory_space=pl.ANY)
    return pl.pallas_call(
        functools.partial(back_ab_kernel, nb, rows),
        grid=(2 * nb + 4,),
        in_specs=[pl.BlockSpec(memory_space=pltpu.SMEM), block(0), any_spec,
                  block(1), col(1), row, block(nb + 1), col(nb + 1), col(nb + 1), col(nb + 1), row, any_spec],
        out_specs=[pl.BlockSpec((1, bn), lambda j: (0, 0)), block(nb + 1), col(nb + 1), col(nb + 1), any_spec, any_spec],
        out_shape=[jax.ShapeDtypeStruct((1, bn), F32), jax.ShapeDtypeStruct((rows, d), BF16), vec, vec]
        + [jax.ShapeDtypeStruct((d, d), F32)] * 2,
        scratch_shapes=[pltpu.VMEM((rows, d), BF16), pltpu.VMEM((bn, d), F32), pltpu.VMEM((bn, d), BF16), pltpu.VMEM((rows, bn), F32),
                        pltpu.VMEM((rows, d), BF16), pltpu.VMEM((2, bn, d), F32), pltpu.VMEM((3, bn, d), F32),
                        pltpu.VMEM((2, d, bn), F32), pltpu.VMEM((3, d, bn), F32), pltpu.SemaphoreType.DMA, pltpu.SemaphoreType.DMA((nb,)),
                        pltpu.SemaphoreType.DMA((2, 2)), pltpu.SemaphoreType.DMA((2, 3)), pltpu.SemaphoreType.DMA((2, 3)),
                        pltpu.SemaphoreType.REGULAR, pltpu.SemaphoreType.REGULAR],
        compiler_params=pltpu.CompilerParams(collective_id=1, has_side_effects=True, vmem_limit_bytes=63 * 1024 * 1024),
        cost_estimate=pl.CostEstimate(flops=10 * rows * d * d, bytes_accessed=rows * d * 24, transcendentals=0),
        name='back_ab',
    )(lam, own, other, n3, i3, w3, n2, i2, g2, b2, t2, t1)


def back_c_kernel(nb, rows, x_hbm, featt_hbm, w2_ref, n1_ref, i1_ref, g1_ref, b1_ref, dg2_ref, db2_ref, loss_ref, p_ref, q_ref,
                  p_out, q_out, dw1a_ref, dw1b_ref, acc, dpre, ring, x_ref, featt, load_sem, store_sem, x_sem, feat_sem):
    j = pl.program_id(0)
    bn = acc.shape[1]

    def load_x(r):
        here = pl.ds(pl.multiple_of(r * TILE, TILE), TILE)
        return pltpu.make_async_copy(x_hbm.at[here, :], x_ref.at[here, :], x_sem.at[r])

    @pl.when(j == 0)
    def _():
        for r in range(rows // TILE):
            load_x(r).start()
        pltpu.make_async_copy(featt_hbm, featt, feat_sem).start()

    @pl.when(j == 1)
    def _():
        pltpu.make_async_copy(featt_hbm, featt, feat_sem).wait()

    def moves(b):
        span = pl.ds(pl.multiple_of(b * bn, bn), bn)
        slot = lax.rem(b, 2)
        return [(pltpu.make_async_copy(src.at[span, :], ring.at[slot, i], load_sem.at[slot, i]),
                 pltpu.make_async_copy(ring.at[slot, i], dst.at[span, :], store_sem.at[slot, i]))
                for i, (src, dst) in enumerate(((p_ref, p_out), (q_ref, q_out)))]

    @pl.when(j >= 2)
    def _():
        for _, store in moves(j - 2):
            store.wait()

    @pl.when(j < nb)
    def _():
        for load, _ in moves(j):
            load.start()

    @pl.when((j >= 1) & (j <= nb))
    def _():
        for load, store in moves(j - 1):
            load.wait()
            store.start()

    def fin():
        def put(r, v):
            dpre[r:r + CHUNK, :] = v

        db, dg = finish_back(rows, acc, n1_ref, i1_ref[...], g1_ref[...], b1_ref[...], put)
        half = dw1b_ref.shape[0]
        for i, row in enumerate((dg, db, dg2_ref[...], db2_ref[...], loss_ref[...])):
            dw1a_ref[half + i:half + i + 1, :] = row

    def mm():
        for r in range(0, rows, TILE):
            acc[r:r + TILE, :] = dot(x_ref[r:r + TILE, :], w2_ref[...], ((1,), (1,)))

    def dw():
        half = dw1b_ref.shape[0]
        dw1a_ref[:half, :] = dot(featt[:half, :], dpre[...])
        dw1b_ref[...] = dot(featt[half:, :], dpre[...])

    @pl.when(j == 0)
    def _():
        def work(r, carry):
            load_x(r).wait()
            here = pl.ds(pl.multiple_of(r * TILE, TILE), TILE)
            acc[here, :] = dot(x_ref[here, :], w2_ref[...], ((1,), (1,)))
            return carry

        lax.fori_loop(0, rows // TILE, work, 0)

    @pl.when((j > 0) & (j < nb))
    def _():
        fin()
        mm()
        dw()

    @pl.when(j == nb)
    def _():
        fin()
        dw()


def back_c(x, featt, w2, n1, i1, g1, b1, dg2, db2, loss, p, q, bn=256):
    rows, d = x.shape
    k = featt.shape[0]
    nb = d // bn

    def at(first):
        return lambda j: (0, jnp.clip(j - first, 0, nb - 1))

    col = pl.BlockSpec((1, bn), at(1))
    row = pl.BlockSpec((bn, d), lambda j: (jnp.minimum(j, nb - 1), 0))
    any_spec = pl.BlockSpec(memory_space=pl.ANY)
    return pl.pallas_call(
        functools.partial(back_c_kernel, nb, rows),
        grid=(nb + 2,),
        in_specs=[any_spec, any_spec,
                  row, pl.BlockSpec((rows, bn), at(1)), col, col, col, col, col, pl.BlockSpec((1, bn), lambda j: (0, 0)), any_spec, any_spec],
        out_specs=[any_spec, any_spec, pl.BlockSpec((k // 2 + 8, bn), at(1)), pl.BlockSpec((k // 2, bn), at(1))],
        out_shape=[jax.ShapeDtypeStruct((d, d), F32)] * 2 + [jax.ShapeDtypeStruct((k // 2 + 8, d), F32), jax.ShapeDtypeStruct((k // 2, d), F32)],
        scratch_shapes=[pltpu.VMEM((rows, bn), F32), pltpu.VMEM((rows, bn), BF16), pltpu.VMEM((2, 2, bn, d), F32),
                        pltpu.VMEM((rows, d), BF16), pltpu.VMEM((k, rows), BF16), pltpu.SemaphoreType.DMA((2, 2)),
                        pltpu.SemaphoreType.DMA((2, 2)), pltpu.SemaphoreType.DMA((rows // TILE,)), pltpu.SemaphoreType.DMA],
        compiler_params=pltpu.CompilerParams(vmem_limit_bytes=VMEM_LIMIT),
        cost_estimate=pl.CostEstimate(flops=2 * rows * d * (k + d), bytes_accessed=rows * d * 20, transcendentals=0),
        name='back_c',
    )(x, featt, w2, n1, i1, g1, b1, dg2, db2, loss, p, q)


def add_first_kernel(p_ref, q_ref, out_ref, small_ref):
    half = out_ref.shape[0]
    out_ref[...] = p_ref[:half, :] + q_ref[:half, :]
    small_ref[...] = p_ref[half:, :] + q_ref[half:, :]


def add_second_kernel(p_ref, q_ref, _, out_ref):
    out_ref[...] = p_ref[...] + q_ref[...]


def add_half(p, q, half, whole=None):
    rows, d = p.shape
    blk = d // 2
    spec = pl.BlockSpec((rows, blk), lambda j: (0, j))
    first = whole is None
    out_specs = [pl.BlockSpec((half, blk), lambda j: (0 if first else 1, j))]
    out_shape = [jax.ShapeDtypeStruct((2 * half, d), F32)]
    if first:
        out_specs.append(pl.BlockSpec((rows - half, blk), lambda j: (0, j)))
        out_shape.append(jax.ShapeDtypeStruct((rows - half, d), F32))
    return pl.pallas_call(
        add_first_kernel if first else add_second_kernel,
        grid=(2,),
        in_specs=[spec, spec] + ([] if first else [pl.BlockSpec(memory_space=pl.ANY)]),
        out_specs=out_specs,
        out_shape=out_shape,
        input_output_aliases={} if first else {2: 0},
        compiler_params=pltpu.CompilerParams(vmem_limit_bytes=24 * 1024 * 1024),
        cost_estimate=pl.CostEstimate(flops=rows * d * 2000, bytes_accessed=rows * d * 12, transcendentals=0),
        name='add_half',
    )(*([p, q] if first else [p, q, whole]))


def solution(mesh):
    n = mesh.shape[AXIS]
    pair = [(i, i + 1 - 2 * (i % 2)) for i in range(n)]

    def swap(x):
        return lax.ppermute(x, AXIS, pair)

    def local_step(feat_a, feat_b, w_one, w_two, w_three, g_one, b_one, g_two, b_two, lam_off):
        width = w_two.shape[0]
        g1, b1, g2, b2 = (v.reshape(1, width) for v in (g_one, b_one, g_two, b_two))
        norm1, norm2, norm3, inv1, inv2, inv3, act1t, act2t, xt, emb, other = forward(
            feat_a, feat_b, w_one, w_two, w_three, g1, b1, g2, b2, n)
        loss, d_pre2, dg2, db2, dw3, dw2 = back_ab(
            lam_off.reshape(1, 1), emb, other, norm3, inv3, w_three, norm2, inv2, g2, b2, act2t, act1t)
        dw3, dw2, dw1a, dw1b = back_c(d_pre2, xt, w_two, norm1, inv1, g1, b1, dg2, db2, loss, dw3, dw2)
        half = dw1b.shape[0]
        dw1, small = add_half(dw1a, swap(dw1a), half)
        dw1, = add_half(dw1b, swap(dw1b), half, dw1)
        dg1, db1, dg2, db2 = (small[i] for i in range(4))
        loss_val = jnp.sum(small[4, :loss.shape[1]]) * 0.5
        return (loss_val, dw1, dw2, dw3, dg1, db1, dg2, db2)

    row_spec = P(AXIS, None)
    return jax.shard_map(local_step, mesh=mesh, in_specs=(row_spec, row_spec) + (P(),) * 8, out_specs=(P(),) * 8, check_vma=False)
```

```python
import functools

import jax
import jax.numpy as jnp
from jax import lax
from jax.experimental import pallas as pl
from jax.experimental.pallas import tpu as pltpu
from jax.sharding import PartitionSpec as P

NORM_EPS = 1e-5
AXIS = 'data'
MESH = pl.DeviceIdType.MESH
F32 = jnp.float32
BF16 = jnp.bfloat16
ONCE = pl.Buffered(1)
VMEM_LIMIT = 60 * 1024 * 1024
TILE = 256
SMALL = 128
CHUNK = 64


def fold(v):
    return jnp.sum(v.reshape(v.shape[0] // 8, 8, v.shape[1]), axis=0)


def dot(a, b, dims=((1,), (0,))):
    return lax.dot_general(a, b, (dims, ((), ())), preferred_element_type=F32)


def forward_kernel(nb, rows, fa_ref, fb_ref, w1_ref, w2_ref, w3_ref, g1_ref, b1_ref, g2_ref, b2_ref,
                   n1_hbm, n2_ref, n3_ref, i1_ref, i2_ref, i3_ref, t1_ref, t2_ref, xt_ref, emb_hbm, other_hbm,
                   xs, w1_buf, pre1, sums1, bufa, bufb, acc, sums, w1_sem, norm_sem, copy_sem, feat_sem, send_sem, recv_sem, esend_sem, erecv_sem):
    j = pl.program_id(0)
    me = lax.axis_index(AXIS)
    core = lax.rem(me, 2)
    chip = me // 2
    x_pos, y_pos = lax.rem(chip, 2), chip // 2
    partner = me + 1 - 2 * core
    x_chip, y_chip = chip + 1 - 2 * x_pos, chip + 2 - 4 * y_pos
    piece = fa_ref.shape[0]
    bn = acc.shape[1]

    def remote(src, dst, send, recv, dev):
        return pltpu.make_async_remote_copy(src_ref=src, dst_ref=dst, send_sem=send, recv_sem=recv, device_id=(dev,), device_id_type=MESH)

    def part(dev):
        return xs.at[pl.ds(pl.multiple_of(dev * piece, piece), piece), :]

    def gather():
        pltpu.make_async_copy(w1_ref, w1_buf, w1_sem).start()
        barrier = pltpu.get_barrier_semaphore()
        for dev in (partner, 2 * x_chip, 2 * x_chip + 1, 2 * y_chip, 2 * y_chip + 1):
            pl.semaphore_signal(barrier, inc=1, device_id=(dev,), device_id_type=MESH)
        pl.semaphore_wait(barrier, 5)

        def sends(mine, mine_src, theirs_src):
            for view, src in ((mine, mine_src), (1 - mine, theirs_src)):
                remote(src, part(me), send_sem.at[1 + view], recv_sem.at[1 + mine], 2 * x_chip + view).start()
                remote(src, part(me), send_sem.at[3 + view], recv_sem.at[3 + mine], 2 * y_chip + view).start()
            remote(theirs_src, part(me), send_sem.at[0], recv_sem.at[0], partner).start()
            pltpu.make_async_copy(mine_src, part(me), feat_sem).start()

        pl.when(core == 0)(lambda: sends(0, fa_ref, fb_ref))
        pl.when(core == 1)(lambda: sends(1, fb_ref, fa_ref))
        remote(fa_ref, part(2 * x_chip), send_sem.at[1], recv_sem.at[1], me).wait_recv()
        relay_y = remote(part(2 * x_chip), part(2 * x_chip), send_sem.at[5], recv_sem.at[5], 2 * y_chip + core)
        relay_y.start()
        remote(fa_ref, part(2 * y_chip + 1), send_sem.at[4], recv_sem.at[4], me).wait_recv()
        relay_x = remote(part(2 * y_chip + 1), part(2 * y_chip + 1), send_sem.at[6], recv_sem.at[6], 2 * x_chip + core)
        relay_x.start()
        pltpu.make_async_copy(fa_ref, part(me), feat_sem).wait()
        remote(fa_ref, part(me), send_sem.at[0], recv_sem.at[0], me).wait()
        pltpu.make_async_copy(w1_ref, w1_buf, w1_sem).wait()
        layer_one(me, partner)
        layer_one(2 * x_chip, 2 * y_chip + 1)
        remote(fa_ref, part(me), send_sem.at[1], recv_sem.at[2], me).wait()
        remote(fa_ref, part(me), send_sem.at[2], recv_sem.at[3], me).wait()
        layer_one(2 * x_chip + 1, 2 * y_chip)
        remote(fa_ref, part(me), send_sem.at[3], recv_sem.at[5], me).wait()
        remote(fa_ref, part(me), send_sem.at[4], recv_sem.at[6], me).wait()
        far = 2 * (3 - chip)
        layer_one(far, far + 1)
        relay_y.wait_send()
        relay_x.wait_send()

    def layer_one(dev_p, dev_q):
        def work(i, carry):
            here = pl.ds(pl.multiple_of(jnp.where(i == 0, dev_p, dev_q) * piece, piece), piece)
            feats = xs[here, :]
            for c in range(0, w1_buf.shape[1], bn):
                pre = dot(feats, w1_buf[:, c:c + bn])
                pre1[here, c:c + bn] = pre
                sums1[0:8, c:c + bn] += fold(pre)
                sums1[8:16, c:c + bn] += fold(pre * pre)
            return carry

        lax.fori_loop(0, 2, work, 0)

    def norm_copy(block):
        cols = pl.ds(pl.multiple_of(block * bn, bn), bn)
        return pltpu.make_async_copy(pre1.at[:, cols], n1_hbm.at[:, cols], norm_sem.at[block])

    def finish_one():
        mean = jnp.sum(sums1[0:8, :], axis=0, keepdims=True) / rows
        inv = lax.rsqrt(jnp.sum(sums1[8:16, :], axis=0, keepdims=True) / rows - mean * mean + NORM_EPS)
        sums1[0:1, :] = mean
        i1_ref[...] = inv

        def work(block, carry):
            cols = pl.ds(pl.multiple_of(block * bn, bn), bn)
            mean, inv, g, b = sums1[0:1, cols], i1_ref[:, cols], g1_ref[:, cols], b1_ref[:, cols]
            for r in range(0, rows, CHUNK):
                norm = (pre1[r:r + CHUNK, cols] - mean) * inv
                pre1[r:r + CHUNK, cols] = norm
                bufa[r:r + CHUNK, cols] = jnp.maximum(norm * g + b, 0.0).astype(BF16)
            return carry

        lax.fori_loop(0, nb, work, 0)
        for block in range(nb):
            norm_copy(block).start()

    def fin(layer):
        norm_ref, inv_ref = ((n2_ref, i2_ref), (n3_ref, i3_ref))[layer]
        buf = (bufb, bufa)[layer]
        base = pl.multiple_of(jnp.maximum(j - 1 - layer * nb, 0) * bn, bn)
        mean = jnp.sum(sums[0:8, :], axis=0, keepdims=True) / rows
        inv = lax.rsqrt(jnp.sum(sums[8:16, :], axis=0, keepdims=True) / rows - mean * mean + NORM_EPS)
        inv_ref[...] = inv
        if layer == 0:
            g, b = g2_ref[...], b2_ref[...]
        for r in range(0, rows, CHUNK):
            norm = (acc[r:r + CHUNK, :] - mean) * inv
            norm_ref[r:r + CHUNK, :] = norm
            if layer == 0:
                norm = jnp.maximum(norm * g + b, 0.0)
            buf[r:r + CHUNK, pl.ds(base, bn)] = norm.astype(BF16)
        if layer == 0:
            for r in range(0, rows, TILE):
                t2_ref[:, r:r + TILE] = buf[r:r + TILE, pl.ds(base, bn)].T

    def mm(layer):
        x_ref, w_ref = ((bufa, w2_ref), (bufb, w3_ref))[layer]
        total = jnp.zeros((8, bn), F32)
        square = jnp.zeros((8, bn), F32)
        for r in range(0, rows, SMALL):
            pre = dot(x_ref[r:r + SMALL, :], w_ref[...])
            acc[r:r + SMALL, :] = pre
            total += fold(pre)
            square += fold(pre * pre)
        sums[0:8, :] = total
        sums[8:16, :] = square

    def out_copy(block):
        cols = pl.ds(pl.multiple_of(block * bn, bn), bn)
        return pltpu.make_async_copy(bufa.at[:, cols], emb_hbm.at[:, cols], copy_sem.at[block])

    def emb_copy(block):
        cols = pl.ds(pl.multiple_of(block * bn, bn), bn)
        return remote(bufa.at[:, cols], other_hbm.at[:, cols], esend_sem.at[block], erecv_sem.at[block], partner)

    @pl.when(j == 0)
    def _():
        sums1[...] = jnp.zeros_like(sums1)
        gather()
        finish_one()

    for layer in range(2):
        @pl.when((j >= layer * nb) & (j < (layer + 1) * nb))
        def _(layer=layer):
            fin(layer)
            mm(layer)
            if layer == 0:
                base = pl.multiple_of(j * bn, bn)
                for r in range(0, rows, TILE):
                    t1_ref[:, r:r + TILE] = bufa[r:r + TILE, pl.ds(base, bn)].T

        @pl.when(j == (layer + 1) * nb)
        def _(layer=layer):
            fin(layer)

    @pl.when(j >= nb + 2)
    def _():
        block = j - 2 - nb
        out_copy(block).start()
        emb_copy(block).start()

    @pl.when(j == nb + 1)
    def _():
        for r in range(0, rows, TILE):
            xt_ref[:, r:r + TILE] = xs[r:r + TILE, :].T

    @pl.when(j == 2 * nb + 1)
    def _():
        for block in range(nb):
            norm_copy(block).wait()
            out_copy(block).wait()
            emb_copy(block).wait()


def forward(fa, fb, w1, w2, w3, g1, b1, g2, b2, n, bn=256):
    piece, k = fa.shape
    rows, d = piece * n, w2.shape[1]
    nb = d // bn

    def at(layer, delay):
        return lambda j: (0, jnp.clip(j - layer * nb - delay, 0, nb - 1))

    whole = pl.BlockSpec((piece, k), lambda j: (0, 0), pipeline_mode=ONCE)
    any_spec = pl.BlockSpec(memory_space=pl.ANY)
    col = [pl.BlockSpec((1, bn), at(layer, 1)) for layer in range(2)]
    norm = [pl.BlockSpec((rows, bn), at(layer, 1)) for layer in range(2)]
    vec = pl.BlockSpec((1, d), lambda j: (0, 0))
    big = jax.ShapeDtypeStruct((rows, d), BF16)
    return pl.pallas_call(
        functools.partial(forward_kernel, nb, rows),
        grid=(2 * nb + 2,),
        in_specs=[whole, whole, any_spec, pl.BlockSpec((d, bn), at(0, 0)), pl.BlockSpec((d, bn), at(1, 0)),
                  vec, vec, col[0], col[0]],
        out_specs=[any_spec] + norm + [vec] + col + [pl.BlockSpec((bn, rows), lambda j, f=at(0, delay): f(j)[::-1]) for delay in range(2)]
        + [pl.BlockSpec((k, rows), lambda j: (0, 0), pipeline_mode=ONCE)] + [any_spec] * 2,
        out_shape=[jax.ShapeDtypeStruct((rows, d), F32)] * 3 + [jax.ShapeDtypeStruct((1, d), F32)] * 3
        + [jax.ShapeDtypeStruct((d, rows), BF16)] * 2 + [jax.ShapeDtypeStruct((k, rows), BF16)] + [big] * 2,
        scratch_shapes=[pltpu.VMEM((rows, k), BF16), pltpu.VMEM((k, d), BF16), pltpu.VMEM((rows, d), F32), pltpu.VMEM((16, d), F32),
                        pltpu.VMEM((rows, d), BF16), pltpu.VMEM((rows, d), BF16), pltpu.VMEM((rows, bn), F32), pltpu.VMEM((16, bn), F32),
                        pltpu.SemaphoreType.DMA, pltpu.SemaphoreType.DMA((nb,)),
                        pltpu.SemaphoreType.DMA((nb,)), pltpu.SemaphoreType.DMA, pltpu.SemaphoreType.DMA((7,)), pltpu.SemaphoreType.DMA((7,)),
                        pltpu.SemaphoreType.DMA((nb,)), pltpu.SemaphoreType.DMA((nb,))],
        compiler_params=pltpu.CompilerParams(collective_id=0, has_side_effects=True, vmem_limit_bytes=63 * 1024 * 1024),
        cost_estimate=pl.CostEstimate(flops=2 * rows * d * (k + 2 * d), bytes_accessed=rows * d * 20, transcendentals=0),
        name='forward',
    )(fa, fb, w1, w2, w3, g1, b1, g2, b2)


def first_pass(products, acc, keep, sums, norm_ref, g, b):
    total = jnp.zeros((8, acc.shape[1]), F32)
    cross = jnp.zeros((8, acc.shape[1]), F32)
    for r, part in products:
        here = pl.ds(r, part.shape[0])
        norm = norm_ref[here, :]
        keep[here, :] = norm
        if b is not None:
            part = jnp.where(norm * g + b > 0.0, part, 0.0)
        acc[here, :] = part
        total += fold(part)
        cross += fold(part * norm)
    sums[0:8, :] = total
    sums[8:16, :] = cross


def second_pass(rows, acc, keep, sums, inv, g, put):
    total = jnp.sum(sums[0:8, :], axis=0, keepdims=True)
    cross = jnp.sum(sums[8:16, :], axis=0, keepdims=True)
    scale = inv if g is None else inv * g
    shift, slope = scale * (total / rows), scale * (cross / rows)
    for r in range(0, rows, CHUNK):
        put(r, (acc[r:r + CHUNK, :] * scale - shift - keep[r:r + CHUNK, :] * slope).astype(BF16))
    return total, cross


def back_ab_kernel(nb, rows, lam_ref, own_ref, other_hbm, n3_ref, i3_ref, w3_ref, n2_ref, i2_ref, g2d_ref, g2_ref, b2_ref, t2_ref, t1_hbm,
                   loss_ref, dpre_ref, dg_ref, db_ref, dw3_hbm, dw2_hbm,
                   big, corr, grad, acc, keep, sums, dout, send3, recv3, send2, recv2, load_sem, chunk_sem, ssem, rsem, osem, free3, free2):
    j = pl.program_id(0)
    me = lax.axis_index(AXIS)
    partner = me + 1 - 2 * lax.rem(me, 2)
    bn = acc.shape[1]
    d = big.shape[1]
    lam = lam_ref[0, 0]
    other_ref = big

    def pair(e):
        return ((send3, recv3, free3, nb), (send2, recv2, free2, nb + 1))[e]

    def swap_copy(e, b, part=None):
        send, recv, _, _ = pair(e)
        src, dst = send.at[lax.rem(b, 2)], recv.at[lax.rem(b, 3)]
        if part is not None:
            src, dst = src.at[part, :], dst.at[part, :]
        return pltpu.make_async_remote_copy(
            src_ref=src, dst_ref=dst, send_sem=ssem.at[e, lax.rem(b, 2)],
            recv_sem=rsem.at[e, lax.rem(b, 3)], device_id=(partner,), device_id_type=MESH)

    def sum_copy(e, b):
        span = pl.ds(pl.multiple_of(b * bn, bn), bn)
        dst = dw3_hbm.at[span, :] if e == 0 else dw2_hbm.at[:, span]
        return pltpu.make_async_copy(pair(e)[1].at[lax.rem(b, 3)], dst, osem.at[e, lax.rem(b, 3)])

    def exchange(e):
        send, recv, free, first = pair(e)

        @pl.when((j >= first + 3) & (j < first + 3 + nb))
        def _():
            b = j - first - 3
            sum_copy(e, b).wait()

            @pl.when(b < nb - 3)
            def _():
                pl.semaphore_signal(free, inc=1, device_id=(partner,), device_id_type=MESH)

        @pl.when((j >= first + 2) & (j < first + 2 + nb))
        def _():
            b = j - first - 2
            swap_copy(e, b).wait()
            mine, theirs = lax.rem(b, 2), lax.rem(b, 3)
            for r in range(0, send.shape[1], send.shape[1] // 32):
                part = pl.ds(r, send.shape[1] // 32)
                recv[theirs, part, :] = recv[theirs, part, :] + send[mine, part, :]
            sum_copy(e, b).start()

    def ready(e, b):
        @pl.when(b >= 3)
        def _():
            pl.semaphore_wait(pair(e)[2], 1)

    def fin_loss():
        base = pl.multiple_of(jnp.maximum(j - 1, 0) * bn, bn)

        def put(r, v):
            dout[r:r + CHUNK, pl.ds(base, bn)] = v

        second_pass(rows, acc, keep, sums, i3_ref[...], None, put)

    def load_other(c):
        cols = pl.ds(pl.multiple_of(c * bn, bn), bn)
        return pltpu.make_async_copy(other_hbm.at[:, cols], big.at[:, cols], chunk_sem.at[c])

    def mm_loss(arriving):
        own = own_ref[...]

        def correlate(c, loss):
            cols = pl.ds(pl.multiple_of(c * bn, bn), bn)
            if arriving:
                load_other(c).wait()
            part = dot(own, other_ref[:, cols], ((0,), (0,))) * (1.0 / rows)
            corr[:, cols] = part
            grad[:, cols] = ((2.0 * lam) * part).astype(BF16)
            return loss + fold(part * part)

        loss = jnp.zeros((8, bn), F32)
        if arriving:
            loss = lax.fori_loop(0, nb, correlate, loss)
        else:
            for c in range(nb):
                loss = correlate(c, loss)
        here = pl.ds(pl.multiple_of(j * bn, bn), bn)
        part = corr[:, here]
        diag = lax.broadcasted_iota(jnp.int32, (bn, bn), 0) == lax.broadcasted_iota(jnp.int32, (bn, bn), 1)
        grad[:, here] = jnp.where(diag, -2.0 * (1.0 - part), (2.0 * lam) * part).astype(BF16)
        loss = lam * loss + fold(jnp.where(diag, (1.0 - part) * (1.0 - part) - lam * (part * part), 0.0))
        loss_ref[...] += jnp.sum(loss, axis=0, keepdims=True)
        first_pass(((r, dot(other_ref[r:r + TILE, :], grad[...], ((1,), (1,))) * (1.0 / rows)) for r in range(0, rows, TILE)),
                   acc, keep, sums, n3_ref, None, None)

    def fin_two():
        def put(r, v):
            dpre_ref[r:r + CHUNK, :] = v

        db_ref[...], dg_ref[...] = second_pass(rows, acc, keep, sums, i2_ref[...], g2d_ref[...], put)

    def mm_two():
        first_pass(((r, dot(dout[r:r + TILE, :], w3_ref[...], ((1,), (1,)))) for r in range(0, rows, TILE)),
                   acc, keep, sums, n2_ref, g2_ref[...], b2_ref[...])
        act = t2_ref[...]
        slot = lax.rem(j - nb, 2)
        for c in range(0, d, 2 * bn):
            send3[slot, :, c:c + 2 * bn] = dot(act, dout[:, c:c + 2 * bn])

    def mm_dw2(first, last):
        slot = lax.rem(j - nb - 1, 2)
        for r in range(first, last, SMALL):
            send2[slot, r:r + SMALL, :] = dot(big[r:r + SMALL, :], dpre_ref[...])

    @pl.when(j == 0)
    def _():
        for c in range(nb):
            load_other(c).start()
        loss_ref[...] = jnp.zeros_like(loss_ref)
        barrier = pltpu.get_barrier_semaphore()
        pl.semaphore_signal(barrier, inc=1, device_id=(partner,), device_id_type=MESH)
        pl.semaphore_wait(barrier, 1)
        mm_loss(True)

    @pl.when(j == nb)
    def _():
        pltpu.make_async_copy(t1_hbm, big, load_sem).start()

    exchange(0)
    exchange(1)

    @pl.when((j > 0) & (j < nb))
    def _():
        fin_loss()
        mm_loss(False)

    @pl.when(j == nb)
    def _():
        fin_loss()

    @pl.when((j >= nb) & (j < 2 * nb))
    def _():
        fin_two()
        mm_two()
        ready(0, j - nb)
        swap_copy(0, j - nb).start()

    @pl.when(j == 2 * nb)
    def _():
        fin_two()

    @pl.when(j == nb + 1)
    def _():
        pltpu.make_async_copy(t1_hbm, big, load_sem).wait()

    @pl.when((j > nb) & (j < 2 * nb))
    def _():
        mm_dw2(0, d)
        ready(1, j - nb - 1)
        swap_copy(1, j - nb - 1).start()

    @pl.when(j == 2 * nb)
    def _():
        ready(1, nb - 1)
        for r in range(0, d, d // 4):
            mm_dw2(r, r + d // 4)
            swap_copy(1, nb - 1, pl.ds(r, d // 4)).start()


def back_ab(lam, own, other, n3, i3, w3, n2, i2, g2, b2, t2, t1, bn=256):
    rows, d = own.shape
    nb = d // bn

    def at(first):
        return lambda j: (0, jnp.clip(j - first, 0, nb - 1))

    def block(first):
        return pl.BlockSpec((rows, bn), at(first))

    def col(first):
        return pl.BlockSpec((1, bn), at(first))

    row = pl.BlockSpec((bn, d), lambda j: (jnp.clip(j - nb, 0, nb - 1), 0))
    vec = jax.ShapeDtypeStruct((1, d), F32)
    any_spec = pl.BlockSpec(memory_space=pl.ANY)
    return pl.pallas_call(
        functools.partial(back_ab_kernel, nb, rows),
        grid=(2 * nb + 4,),
        in_specs=[pl.BlockSpec(memory_space=pltpu.SMEM), block(0), any_spec,
                  block(0), col(1), row, block(nb), col(nb + 1), col(nb + 1), col(nb), col(nb), row, any_spec],
        out_specs=[pl.BlockSpec((1, bn), lambda j: (0, 0)), block(nb + 1), col(nb + 1), col(nb + 1), any_spec, any_spec],
        out_shape=[jax.ShapeDtypeStruct((1, bn), F32), jax.ShapeDtypeStruct((rows, d), BF16), vec, vec]
        + [jax.ShapeDtypeStruct((d, d), F32)] * 2,
        scratch_shapes=[pltpu.VMEM((rows, d), BF16), pltpu.VMEM((bn, d), F32), pltpu.VMEM((bn, d), BF16), pltpu.VMEM((rows, bn), F32),
                        pltpu.VMEM((rows, bn), F32), pltpu.VMEM((16, bn), F32),
                        pltpu.VMEM((rows, d), BF16), pltpu.VMEM((2, bn, d), F32), pltpu.VMEM((3, bn, d), F32),
                        pltpu.VMEM((2, d, bn), F32), pltpu.VMEM((3, d, bn), F32), pltpu.SemaphoreType.DMA, pltpu.SemaphoreType.DMA((nb,)),
                        pltpu.SemaphoreType.DMA((2, 2)), pltpu.SemaphoreType.DMA((2, 3)), pltpu.SemaphoreType.DMA((2, 3)),
                        pltpu.SemaphoreType.REGULAR, pltpu.SemaphoreType.REGULAR],
        compiler_params=pltpu.CompilerParams(collective_id=1, has_side_effects=True, vmem_limit_bytes=63 * 1024 * 1024),
        cost_estimate=pl.CostEstimate(flops=10 * rows * d * d, bytes_accessed=rows * d * 24, transcendentals=0),
        name='back_ab',
    )(lam, own, other, n3, i3, w3, n2, i2, g2, g2, b2, t2, t1)


def back_c_kernel(nb, rows, x_hbm, featt_hbm, w2_ref, n1_ref, i1_ref, g1d_ref, g1_ref, b1_ref, dg2_ref, db2_ref, loss_ref, p_ref, q_ref,
                  p_out, q_out, dw1a_ref, dw1b_ref, acc, keep, sums, dpre, ring, x_ref, featt, load_sem, store_sem, x_sem, feat_sem):
    j = pl.program_id(0)
    bn = acc.shape[1]

    def load_x(r):
        here = pl.ds(pl.multiple_of(r * TILE, TILE), TILE)
        return pltpu.make_async_copy(x_hbm.at[here, :], x_ref.at[here, :], x_sem.at[r])

    @pl.when(j == 0)
    def _():
        for r in range(rows // TILE):
            load_x(r).start()
        pltpu.make_async_copy(featt_hbm, featt, feat_sem).start()

    @pl.when(j == 1)
    def _():
        pltpu.make_async_copy(featt_hbm, featt, feat_sem).wait()

    def moves(b):
        span = pl.ds(pl.multiple_of(b * bn, bn), bn)
        slot = lax.rem(b, 2)
        return [(pltpu.make_async_copy(src.at[span, :], ring.at[slot, i], load_sem.at[slot, i]),
                 pltpu.make_async_copy(ring.at[slot, i], dst.at[span, :], store_sem.at[slot, i]))
                for i, (src, dst) in enumerate(((p_ref, p_out), (q_ref, q_out)))]

    @pl.when(j >= 2)
    def _():
        for _, store in moves(j - 2):
            store.wait()

    @pl.when(j < nb)
    def _():
        for load, _ in moves(j):
            load.start()

    @pl.when((j >= 1) & (j <= nb))
    def _():
        for load, store in moves(j - 1):
            load.wait()
            store.start()

    def fin():
        def put(r, v):
            dpre[r:r + CHUNK, :] = v

        db, dg = second_pass(rows, acc, keep, sums, i1_ref[...], g1d_ref[...], put)
        half = dw1b_ref.shape[0]
        for i, row in enumerate((dg, db, dg2_ref[...], db2_ref[...], loss_ref[...])):
            dw1a_ref[half + i:half + i + 1, :] = row

    def mm():
        first_pass(((r, dot(x_ref[r:r + TILE, :], w2_ref[...], ((1,), (1,)))) for r in range(0, rows, TILE)),
                   acc, keep, sums, n1_ref, g1_ref[...], b1_ref[...])

    def dw():
        half = dw1b_ref.shape[0]
        dw1a_ref[:half, :] = dot(featt[:half, :], dpre[...])
        dw1b_ref[...] = dot(featt[half:, :], dpre[...])

    @pl.when(j == 0)
    def _():
        def work(r, carry):
            load_x(r).wait()
            here = pl.ds(pl.multiple_of(r * TILE, TILE), TILE)
            norm = n1_ref[here, :]
            keep[here, :] = norm
            part = jnp.where(norm * g1_ref[...] + b1_ref[...] > 0.0, dot(x_ref[here, :], w2_ref[...], ((1,), (1,))), 0.0)
            acc[here, :] = part
            return carry[0] + fold(part), carry[1] + fold(part * norm)

        zero = jnp.zeros((8, bn), F32)
        sums[0:8, :], sums[8:16, :] = lax.fori_loop(0, rows // TILE, work, (zero, zero))

    @pl.when((j > 0) & (j < nb))
    def _():
        fin()
        mm()
        dw()

    @pl.when(j == nb)
    def _():
        fin()
        dw()


def back_c(x, featt, w2, n1, i1, g1, b1, dg2, db2, loss, p, q, bn=256):
    rows, d = x.shape
    k = featt.shape[0]
    nb = d // bn

    def at(first):
        return lambda j: (0, jnp.clip(j - first, 0, nb - 1))

    col, now = pl.BlockSpec((1, bn), at(1)), pl.BlockSpec((1, bn), at(0))
    row = pl.BlockSpec((bn, d), lambda j: (jnp.minimum(j, nb - 1), 0))
    any_spec = pl.BlockSpec(memory_space=pl.ANY)
    return pl.pallas_call(
        functools.partial(back_c_kernel, nb, rows),
        grid=(nb + 2,),
        in_specs=[any_spec, any_spec,
                  row, pl.BlockSpec((rows, bn), at(0)), col, col, now, now, col, col, pl.BlockSpec((1, bn), lambda j: (0, 0)), any_spec, any_spec],
        out_specs=[any_spec, any_spec, pl.BlockSpec((k // 2 + 8, bn), at(1)), pl.BlockSpec((k // 2, bn), at(1))],
        out_shape=[jax.ShapeDtypeStruct((d, d), F32)] * 2 + [jax.ShapeDtypeStruct((k // 2 + 8, d), F32), jax.ShapeDtypeStruct((k // 2, d), F32)],
        scratch_shapes=[pltpu.VMEM((rows, bn), F32), pltpu.VMEM((rows, bn), F32), pltpu.VMEM((16, bn), F32),
                        pltpu.VMEM((rows, bn), BF16), pltpu.VMEM((2, 2, bn, d), F32),
                        pltpu.VMEM((rows, d), BF16), pltpu.VMEM((k, rows), BF16), pltpu.SemaphoreType.DMA((2, 2)),
                        pltpu.SemaphoreType.DMA((2, 2)), pltpu.SemaphoreType.DMA((rows // TILE,)), pltpu.SemaphoreType.DMA],
        compiler_params=pltpu.CompilerParams(vmem_limit_bytes=VMEM_LIMIT),
        cost_estimate=pl.CostEstimate(flops=2 * rows * d * (k + d), bytes_accessed=rows * d * 20, transcendentals=0),
        name='back_c',
    )(x, featt, w2, n1, i1, g1, g1, b1, dg2, db2, loss, p, q)


def add_first_kernel(p_ref, q_ref, out_ref, small_ref):
    half = out_ref.shape[0]
    out_ref[...] = p_ref[:half, :] + q_ref[:half, :]
    small_ref[...] = p_ref[half:, :] + q_ref[half:, :]


def add_second_kernel(p_ref, q_ref, _, out_ref):
    out_ref[...] = p_ref[...] + q_ref[...]


def add_half(p, q, half, whole=None):
    rows, d = p.shape
    blk = d // 2
    spec = pl.BlockSpec((rows, blk), lambda j: (0, j))
    first = whole is None
    out_specs = [pl.BlockSpec((half, blk), lambda j: (0 if first else 1, j))]
    out_shape = [jax.ShapeDtypeStruct((2 * half, d), F32)]
    if first:
        out_specs.append(pl.BlockSpec((rows - half, blk), lambda j: (0, j)))
        out_shape.append(jax.ShapeDtypeStruct((rows - half, d), F32))
    return pl.pallas_call(
        add_first_kernel if first else add_second_kernel,
        grid=(2,),
        in_specs=[spec, spec] + ([] if first else [pl.BlockSpec(memory_space=pl.ANY)]),
        out_specs=out_specs,
        out_shape=out_shape,
        input_output_aliases={} if first else {2: 0},
        compiler_params=pltpu.CompilerParams(vmem_limit_bytes=24 * 1024 * 1024),
        cost_estimate=pl.CostEstimate(flops=rows * d * 2000, bytes_accessed=rows * d * 12, transcendentals=0),
        name='add_half',
    )(*([p, q] if first else [p, q, whole]))


def solution(mesh):
    n = mesh.shape[AXIS]
    pair = [(i, i + 1 - 2 * (i % 2)) for i in range(n)]

    def swap(x):
        return lax.ppermute(x, AXIS, pair)

    def local_step(feat_a, feat_b, w_one, w_two, w_three, g_one, b_one, g_two, b_two, lam_off):
        width = w_two.shape[0]
        g1, b1, g2, b2 = (v.reshape(1, width) for v in (g_one, b_one, g_two, b_two))
        norm1, norm2, norm3, inv1, inv2, inv3, act1t, act2t, xt, emb, other = forward(
            feat_a, feat_b, w_one, w_two, w_three, g1, b1, g2, b2, n)
        loss, d_pre2, dg2, db2, dw3, dw2 = back_ab(
            lam_off.reshape(1, 1), emb, other, norm3, inv3, w_three, norm2, inv2, g2, b2, act2t, act1t)
        dw3, dw2, dw1a, dw1b = back_c(d_pre2, xt, w_two, norm1, inv1, g1, b1, dg2, db2, loss, dw3, dw2)
        half = dw1b.shape[0]
        dw1, small = add_half(dw1a, swap(dw1a), half)
        dw1, = add_half(dw1b, swap(dw1b), half, dw1)
        dg1, db1, dg2, db2 = (small[i] for i in range(4))
        loss_val = jnp.sum(small[4, :loss.shape[1]]) * 0.5
        return (loss_val, dw1, dw2, dw3, dg1, db1, dg2, db2)

    row_spec = P(AXIS, None)
    return jax.shard_map(local_step, mesh=mesh, in_specs=(row_spec, row_spec) + (P(),) * 8, out_specs=(P(),) * 8, check_vma=False)
```

```python
import functools

import jax
import jax.numpy as jnp
from jax import lax
from jax.experimental import pallas as pl
from jax.experimental.pallas import tpu as pltpu
from jax.sharding import PartitionSpec as P

NORM_EPS = 1e-5
AXIS = 'data'
MESH = pl.DeviceIdType.MESH
F32 = jnp.float32
BF16 = jnp.bfloat16
ONCE = pl.Buffered(1)
VMEM_LIMIT = 60 * 1024 * 1024
TILE = 256
SMALL = 128
CHUNK = 64


def fold(v):
    return jnp.sum(v.reshape(v.shape[0] // 8, 8, v.shape[1]), axis=0)


def dot(a, b, dims=((1,), (0,))):
    return lax.dot_general(a, b, (dims, ((), ())), preferred_element_type=F32)


def forward_kernel(nb, rows, fa_ref, fb_ref, w1_ref, w2_ref, w3_ref, g1_ref, b1_ref, g2_ref, b2_ref,
                   n1_hbm, n2_ref, n3_ref, i1_ref, i2_ref, i3_ref, t1_ref, t2_ref, xt_ref, emb_hbm, other_hbm,
                   xs, w1_buf, pre1, sums1, bufa, bufb, acc, sums, w1_sem, norm_sem, copy_sem, feat_sem, send_sem, recv_sem, esend_sem, erecv_sem):
    j = pl.program_id(0)
    me = lax.axis_index(AXIS)
    core = lax.rem(me, 2)
    chip = me // 2
    x_pos, y_pos = lax.rem(chip, 2), chip // 2
    partner = me + 1 - 2 * core
    x_chip, y_chip = chip + 1 - 2 * x_pos, chip + 2 - 4 * y_pos
    piece = fa_ref.shape[0]
    bn = acc.shape[1]

    def remote(src, dst, send, recv, dev):
        return pltpu.make_async_remote_copy(src_ref=src, dst_ref=dst, send_sem=send, recv_sem=recv, device_id=(dev,), device_id_type=MESH)

    def part(dev):
        return xs.at[pl.ds(pl.multiple_of(dev * piece, piece), piece), :]

    def gather():
        pltpu.make_async_copy(w1_ref, w1_buf, w1_sem).start()
        barrier = pltpu.get_barrier_semaphore()
        for dev in (partner, 2 * x_chip, 2 * x_chip + 1, 2 * y_chip, 2 * y_chip + 1):
            pl.semaphore_signal(barrier, inc=1, device_id=(dev,), device_id_type=MESH)
        pl.semaphore_wait(barrier, 5)

        def sends(mine, mine_src, theirs_src):
            for view, src in ((mine, mine_src), (1 - mine, theirs_src)):
                remote(src, part(me), send_sem.at[1 + view], recv_sem.at[1 + mine], 2 * x_chip + view).start()
                remote(src, part(me), send_sem.at[3 + view], recv_sem.at[3 + mine], 2 * y_chip + view).start()
            remote(theirs_src, part(me), send_sem.at[0], recv_sem.at[0], partner).start()
            pltpu.make_async_copy(mine_src, part(me), feat_sem).start()

        pl.when(core == 0)(lambda: sends(0, fa_ref, fb_ref))
        pl.when(core == 1)(lambda: sends(1, fb_ref, fa_ref))
        remote(fa_ref, part(2 * x_chip), send_sem.at[1], recv_sem.at[1], me).wait_recv()
        relay_y = remote(part(2 * x_chip), part(2 * x_chip), send_sem.at[5], recv_sem.at[5], 2 * y_chip + core)
        relay_y.start()
        remote(fa_ref, part(2 * y_chip + 1), send_sem.at[4], recv_sem.at[4], me).wait_recv()
        relay_x = remote(part(2 * y_chip + 1), part(2 * y_chip + 1), send_sem.at[6], recv_sem.at[6], 2 * x_chip + core)
        relay_x.start()
        pltpu.make_async_copy(fa_ref, part(me), feat_sem).wait()
        remote(fa_ref, part(me), send_sem.at[0], recv_sem.at[0], me).wait()
        pltpu.make_async_copy(w1_ref, w1_buf, w1_sem).wait()
        layer_one(me, partner)
        layer_one(2 * x_chip, 2 * y_chip + 1)
        remote(fa_ref, part(me), send_sem.at[1], recv_sem.at[2], me).wait()
        remote(fa_ref, part(me), send_sem.at[2], recv_sem.at[3], me).wait()
        layer_one(2 * x_chip + 1, 2 * y_chip)
        remote(fa_ref, part(me), send_sem.at[3], recv_sem.at[5], me).wait()
        remote(fa_ref, part(me), send_sem.at[4], recv_sem.at[6], me).wait()
        far = 2 * (3 - chip)
        layer_one(far, far + 1)
        relay_y.wait_send()
        relay_x.wait_send()

    def layer_one(dev_p, dev_q):
        def work(i, carry):
            here = pl.ds(pl.multiple_of(jnp.where(i == 0, dev_p, dev_q) * piece, piece), piece)
            feats = xs[here, :]
            for c in range(0, w1_buf.shape[1], bn):
                pre = dot(feats, w1_buf[:, c:c + bn])
                pre1[here, c:c + bn] = pre
                sums1[0:8, c:c + bn] += fold(pre)
                sums1[8:16, c:c + bn] += fold(pre * pre)
            return carry

        lax.fori_loop(0, 2, work, 0)

    def norm_copy(block):
        cols = pl.ds(pl.multiple_of(block * bn, bn), bn)
        return pltpu.make_async_copy(pre1.at[:, cols], n1_hbm.at[:, cols], norm_sem.at[block])

    def finish_one():
        mean = jnp.sum(sums1[0:8, :], axis=0, keepdims=True) / rows
        inv = lax.rsqrt(jnp.sum(sums1[8:16, :], axis=0, keepdims=True) / rows - mean * mean + NORM_EPS)
        sums1[0:1, :] = mean
        i1_ref[...] = inv

        def work(block, carry):
            cols = pl.ds(pl.multiple_of(block * bn, bn), bn)
            mean, inv, g, b = sums1[0:1, cols], i1_ref[:, cols], g1_ref[:, cols], b1_ref[:, cols]
            for r in range(0, rows, CHUNK):
                norm = (pre1[r:r + CHUNK, cols] - mean) * inv
                pre1[r:r + CHUNK, cols] = norm
                bufa[r:r + CHUNK, cols] = jnp.maximum(norm * g + b, 0.0).astype(BF16)
            return carry

        lax.fori_loop(0, nb, work, 0)
        for block in range(nb):
            norm_copy(block).start()

    def fin(layer):
        norm_ref, inv_ref = ((n2_ref, i2_ref), (n3_ref, i3_ref))[layer]
        buf = (bufb, bufa)[layer]
        base = pl.multiple_of(jnp.maximum(j - 1 - layer * nb, 0) * bn, bn)
        mean = jnp.sum(sums[0:8, :], axis=0, keepdims=True) / rows
        inv = lax.rsqrt(jnp.sum(sums[8:16, :], axis=0, keepdims=True) / rows - mean * mean + NORM_EPS)
        inv_ref[...] = inv
        if layer == 0:
            g, b = g2_ref[...], b2_ref[...]
        for r in range(0, rows, CHUNK):
            norm = (acc[r:r + CHUNK, :] - mean) * inv
            norm_ref[r:r + CHUNK, :] = norm
            if layer == 0:
                norm = jnp.maximum(norm * g + b, 0.0)
            buf[r:r + CHUNK, pl.ds(base, bn)] = norm.astype(BF16)
        if layer == 0:
            for r in range(0, rows, TILE):
                t2_ref[:, r:r + TILE] = buf[r:r + TILE, pl.ds(base, bn)].T

    def mm(layer):
        x_ref, w_ref = ((bufa, w2_ref), (bufb, w3_ref))[layer]
        total = jnp.zeros((8, bn), F32)
        square = jnp.zeros((8, bn), F32)
        for r in range(0, rows, SMALL):
            pre = dot(x_ref[r:r + SMALL, :], w_ref[...])
            acc[r:r + SMALL, :] = pre
            total += fold(pre)
            square += fold(pre * pre)
        sums[0:8, :] = total
        sums[8:16, :] = square

    def out_copy(block):
        cols = pl.ds(pl.multiple_of(block * bn, bn), bn)
        return pltpu.make_async_copy(bufa.at[:, cols], emb_hbm.at[:, cols], copy_sem.at[block])

    def emb_copy(block):
        cols = pl.ds(pl.multiple_of(block * bn, bn), bn)
        return remote(bufa.at[:, cols], other_hbm.at[:, cols], esend_sem.at[block], erecv_sem.at[block], partner)

    @pl.when(j == 0)
    def _():
        sums1[...] = jnp.zeros_like(sums1)
        gather()
        finish_one()

    for layer in range(2):
        @pl.when((j >= layer * nb) & (j < (layer + 1) * nb))
        def _(layer=layer):
            fin(layer)
            mm(layer)
            if layer == 0:
                base = pl.multiple_of(j * bn, bn)
                for r in range(0, rows, TILE):
                    t1_ref[:, r:r + TILE] = bufa[r:r + TILE, pl.ds(base, bn)].T

        @pl.when(j == (layer + 1) * nb)
        def _(layer=layer):
            fin(layer)

    @pl.when(j >= nb + 2)
    def _():
        block = j - 2 - nb
        out_copy(block).start()
        emb_copy(block).start()

    @pl.when(j == nb + 1)
    def _():
        for r in range(0, rows, TILE):
            xt_ref[:, r:r + TILE] = xs[r:r + TILE, :].T

    @pl.when(j == 2 * nb + 1)
    def _():
        for block in range(nb):
            norm_copy(block).wait()
            out_copy(block).wait()
            emb_copy(block).wait()


def forward(fa, fb, w1, w2, w3, g1, b1, g2, b2, n, bn=256):
    piece, k = fa.shape
    rows, d = piece * n, w2.shape[1]
    nb = d // bn

    def at(layer, delay):
        return lambda j: (0, jnp.clip(j - layer * nb - delay, 0, nb - 1))

    whole = pl.BlockSpec((piece, k), lambda j: (0, 0), pipeline_mode=ONCE)
    any_spec = pl.BlockSpec(memory_space=pl.ANY)
    col = [pl.BlockSpec((1, bn), at(layer, 1)) for layer in range(2)]
    norm = [pl.BlockSpec((rows, bn), at(layer, 1)) for layer in range(2)]
    vec = pl.BlockSpec((1, d), lambda j: (0, 0))
    big = jax.ShapeDtypeStruct((rows, d), BF16)
    return pl.pallas_call(
        functools.partial(forward_kernel, nb, rows),
        grid=(2 * nb + 2,),
        in_specs=[whole, whole, any_spec, pl.BlockSpec((d, bn), at(0, 0)), pl.BlockSpec((d, bn), at(1, 0)),
                  vec, vec, col[0], col[0]],
        out_specs=[any_spec] + norm + [vec] + col + [pl.BlockSpec((bn, rows), lambda j, f=at(0, delay): f(j)[::-1]) for delay in range(2)]
        + [pl.BlockSpec((k, rows), lambda j: (0, 0), pipeline_mode=ONCE)] + [any_spec] * 2,
        out_shape=[jax.ShapeDtypeStruct((rows, d), F32)] * 3 + [jax.ShapeDtypeStruct((1, d), F32)] * 3
        + [jax.ShapeDtypeStruct((d, rows), BF16)] * 2 + [jax.ShapeDtypeStruct((k, rows), BF16)] + [big] * 2,
        scratch_shapes=[pltpu.VMEM((rows, k), BF16), pltpu.VMEM((k, d), BF16), pltpu.VMEM((rows, d), F32), pltpu.VMEM((16, d), F32),
                        pltpu.VMEM((rows, d), BF16), pltpu.VMEM((rows, d), BF16), pltpu.VMEM((rows, bn), F32), pltpu.VMEM((16, bn), F32),
                        pltpu.SemaphoreType.DMA, pltpu.SemaphoreType.DMA((nb,)),
                        pltpu.SemaphoreType.DMA((nb,)), pltpu.SemaphoreType.DMA, pltpu.SemaphoreType.DMA((7,)), pltpu.SemaphoreType.DMA((7,)),
                        pltpu.SemaphoreType.DMA((nb,)), pltpu.SemaphoreType.DMA((nb,))],
        compiler_params=pltpu.CompilerParams(collective_id=0, has_side_effects=True, vmem_limit_bytes=63 * 1024 * 1024),
        cost_estimate=pl.CostEstimate(flops=2 * rows * d * (k + 2 * d), bytes_accessed=rows * d * 20, transcendentals=0),
        name='forward',
    )(fa, fb, w1, w2, w3, g1, b1, g2, b2)


def finish_back(rows, acc, norm_ref, inv, g, b, put):
    bn = acc.shape[1]
    total = jnp.zeros((8, bn), F32)
    cross = jnp.zeros((8, bn), F32)
    for r in range(0, rows, CHUNK):
        part = acc[r:r + CHUNK, :]
        norm = norm_ref[r:r + CHUNK, :]
        if b is not None:
            part = jnp.where(norm * g + b > 0.0, part, 0.0)
            acc[r:r + CHUNK, :] = part
        total += fold(part)
        cross += fold(part * norm)
    total = jnp.sum(total, axis=0, keepdims=True)
    cross = jnp.sum(cross, axis=0, keepdims=True)
    scale = inv if g is None else inv * g
    shift, slope = scale * (total / rows), scale * (cross / rows)
    for r in range(0, rows, CHUNK):
        put(r, (acc[r:r + CHUNK, :] * scale - shift - norm_ref[r:r + CHUNK, :] * slope).astype(BF16))
    return total, cross


def back_ab_kernel(nb, rows, lam_ref, own_ref, other_hbm, n3_ref, i3_ref, w3_ref, n2_ref, i2_ref, g2_ref, b2_ref, t2_ref, t1_hbm,
                   loss_ref, dpre_ref, dg_ref, db_ref, dw3_hbm, dw2_hbm,
                   big, corr, grad, acc, dout, send3, recv3, send2, recv2, load_sem, chunk_sem, ssem, rsem, osem, free3, free2):
    j = pl.program_id(0)
    me = lax.axis_index(AXIS)
    partner = me + 1 - 2 * lax.rem(me, 2)
    bn = acc.shape[1]
    d = big.shape[1]
    lam = lam_ref[0, 0]
    other_ref = big

    def pair(e):
        return ((send3, recv3, free3, nb), (send2, recv2, free2, nb + 1))[e]

    def swap_copy(e, b, part=None):
        send, recv, _, _ = pair(e)
        src, dst = send.at[lax.rem(b, 2)], recv.at[lax.rem(b, 3)]
        if part is not None:
            src, dst = src.at[part, :], dst.at[part, :]
        return pltpu.make_async_remote_copy(
            src_ref=src, dst_ref=dst, send_sem=ssem.at[e, lax.rem(b, 2)],
            recv_sem=rsem.at[e, lax.rem(b, 3)], device_id=(partner,), device_id_type=MESH)

    def sum_copy(e, b):
        span = pl.ds(pl.multiple_of(b * bn, bn), bn)
        dst = dw3_hbm.at[span, :] if e == 0 else dw2_hbm.at[:, span]
        return pltpu.make_async_copy(pair(e)[1].at[lax.rem(b, 3)], dst, osem.at[e, lax.rem(b, 3)])

    def exchange(e):
        send, recv, free, first = pair(e)

        @pl.when((j >= first + 3) & (j < first + 3 + nb))
        def _():
            b = j - first - 3
            sum_copy(e, b).wait()

            @pl.when(b < nb - 3)
            def _():
                pl.semaphore_signal(free, inc=1, device_id=(partner,), device_id_type=MESH)

        @pl.when((j >= first + 2) & (j < first + 2 + nb))
        def _():
            b = j - first - 2
            swap_copy(e, b).wait()
            mine, theirs = lax.rem(b, 2), lax.rem(b, 3)
            for r in range(0, send.shape[1], send.shape[1] // 32):
                part = pl.ds(r, send.shape[1] // 32)
                recv[theirs, part, :] = recv[theirs, part, :] + send[mine, part, :]
            sum_copy(e, b).start()

    def ready(e, b):
        @pl.when(b >= 3)
        def _():
            pl.semaphore_wait(pair(e)[2], 1)

    def fin_loss():
        base = pl.multiple_of(jnp.maximum(j - 1, 0) * bn, bn)

        def put(r, v):
            dout[r:r + CHUNK, pl.ds(base, bn)] = v

        finish_back(rows, acc, n3_ref, i3_ref[...], None, None, put)

    def load_other(c):
        cols = pl.ds(pl.multiple_of(c * bn, bn), bn)
        return pltpu.make_async_copy(other_hbm.at[:, cols], big.at[:, cols], chunk_sem.at[c])

    def mm_loss(arriving):
        own = own_ref[...]

        def correlate(c, loss):
            cols = pl.ds(pl.multiple_of(c * bn, bn), bn)
            if arriving:
                load_other(c).wait()
            part = dot(own, other_ref[:, cols], ((0,), (0,))) * (1.0 / rows)
            corr[:, cols] = part
            grad[:, cols] = ((2.0 * lam) * part).astype(BF16)
            return loss + fold(part * part)

        loss = jnp.zeros((8, bn), F32)
        if arriving:
            loss = lax.fori_loop(0, nb, correlate, loss)
        else:
            for c in range(nb):
                loss = correlate(c, loss)
        here = pl.ds(pl.multiple_of(j * bn, bn), bn)
        part = corr[:, here]
        diag = lax.broadcasted_iota(jnp.int32, (bn, bn), 0) == lax.broadcasted_iota(jnp.int32, (bn, bn), 1)
        grad[:, here] = jnp.where(diag, -2.0 * (1.0 - part), (2.0 * lam) * part).astype(BF16)
        loss = lam * loss + fold(jnp.where(diag, (1.0 - part) * (1.0 - part) - lam * (part * part), 0.0))
        loss_ref[...] += jnp.sum(loss, axis=0, keepdims=True)
        for r in range(0, rows, TILE):
            acc[r:r + TILE, :] = dot(other_ref[r:r + TILE, :], grad[...], ((1,), (1,))) * (1.0 / rows)

    def fin_two():
        def put(r, v):
            dpre_ref[r:r + CHUNK, :] = v

        db_ref[...], dg_ref[...] = finish_back(rows, acc, n2_ref, i2_ref[...], g2_ref[...], b2_ref[...], put)

    def mm_two():
        for r in range(0, rows, TILE):
            acc[r:r + TILE, :] = dot(dout[r:r + TILE, :], w3_ref[...], ((1,), (1,)))
        act = t2_ref[...]
        slot = lax.rem(j - nb, 2)
        for c in range(0, d, 2 * bn):
            send3[slot, :, c:c + 2 * bn] = dot(act, dout[:, c:c + 2 * bn])

    def mm_dw2(first, last):
        slot = lax.rem(j - nb - 1, 2)
        for r in range(first, last, TILE):
            send2[slot, r:r + TILE, :] = dot(big[r:r + TILE, :], dpre_ref[...])

    @pl.when(j == 0)
    def _():
        for c in range(nb):
            load_other(c).start()
        loss_ref[...] = jnp.zeros_like(loss_ref)
        barrier = pltpu.get_barrier_semaphore()
        pl.semaphore_signal(barrier, inc=1, device_id=(partner,), device_id_type=MESH)
        pl.semaphore_wait(barrier, 1)
        mm_loss(True)

    @pl.when(j == nb)
    def _():
        pltpu.make_async_copy(t1_hbm, big, load_sem).start()

    exchange(0)
    exchange(1)

    @pl.when((j > 0) & (j < nb))
    def _():
        fin_loss()
        mm_loss(False)

    @pl.when(j == nb)
    def _():
        fin_loss()

    @pl.when((j >= nb) & (j < 2 * nb))
    def _():
        fin_two()
        mm_two()
        ready(0, j - nb)
        swap_copy(0, j - nb).start()

    @pl.when(j == 2 * nb)
    def _():
        fin_two()

    @pl.when(j == nb + 1)
    def _():
        pltpu.make_async_copy(t1_hbm, big, load_sem).wait()

    @pl.when((j > nb) & (j < 2 * nb))
    def _():
        mm_dw2(0, d)
        ready(1, j - nb - 1)
        swap_copy(1, j - nb - 1).start()

    @pl.when(j == 2 * nb)
    def _():
        ready(1, nb - 1)
        for r in range(0, d, d // 4):
            mm_dw2(r, r + d // 4)
            swap_copy(1, nb - 1, pl.ds(r, d // 4)).start()


def back_ab(lam, own, other, n3, i3, w3, n2, i2, g2, b2, t2, t1, bn=256):
    rows, d = own.shape
    nb = d // bn

    def at(first):
        return lambda j: (0, jnp.clip(j - first, 0, nb - 1))

    def block(first):
        return pl.BlockSpec((rows, bn), at(first))

    def col(first):
        return pl.BlockSpec((1, bn), at(first))

    row = pl.BlockSpec((bn, d), lambda j: (jnp.clip(j - nb, 0, nb - 1), 0))
    vec = jax.ShapeDtypeStruct((1, d), F32)
    any_spec = pl.BlockSpec(memory_space=pl.ANY)
    return pl.pallas_call(
        functools.partial(back_ab_kernel, nb, rows),
        grid=(2 * nb + 4,),
        in_specs=[pl.BlockSpec(memory_space=pltpu.SMEM), block(0), any_spec,
                  block(1), col(1), row, block(nb + 1), col(nb + 1), col(nb + 1), col(nb + 1), row, any_spec],
        out_specs=[pl.BlockSpec((1, bn), lambda j: (0, 0)), block(nb + 1), col(nb + 1), col(nb + 1), any_spec, any_spec],
        out_shape=[jax.ShapeDtypeStruct((1, bn), F32), jax.ShapeDtypeStruct((rows, d), BF16), vec, vec]
        + [jax.ShapeDtypeStruct((d, d), F32)] * 2,
        scratch_shapes=[pltpu.VMEM((rows, d), BF16), pltpu.VMEM((bn, d), F32), pltpu.VMEM((bn, d), BF16), pltpu.VMEM((rows, bn), F32),
                        pltpu.VMEM((rows, d), BF16), pltpu.VMEM((2, bn, d), F32), pltpu.VMEM((3, bn, d), F32),
                        pltpu.VMEM((2, d, bn), F32), pltpu.VMEM((3, d, bn), F32), pltpu.SemaphoreType.DMA, pltpu.SemaphoreType.DMA((nb,)),
                        pltpu.SemaphoreType.DMA((2, 2)), pltpu.SemaphoreType.DMA((2, 3)), pltpu.SemaphoreType.DMA((2, 3)),
                        pltpu.SemaphoreType.REGULAR, pltpu.SemaphoreType.REGULAR],
        compiler_params=pltpu.CompilerParams(collective_id=1, has_side_effects=True, vmem_limit_bytes=63 * 1024 * 1024),
        cost_estimate=pl.CostEstimate(flops=10 * rows * d * d, bytes_accessed=rows * d * 24, transcendentals=0),
        name='back_ab',
    )(lam, own, other, n3, i3, w3, n2, i2, g2, b2, t2, t1)


def back_c_kernel(nb, rows, x_hbm, featt_hbm, w2_ref, n1_ref, i1_ref, g1_ref, b1_ref, dg2_ref, db2_ref, loss_ref, p_ref, q_ref,
                  p_out, q_out, dw1a_ref, dw1b_ref, acc, dpre, ring, x_ref, featt, load_sem, store_sem, x_sem, feat_sem):
    j = pl.program_id(0)
    bn = acc.shape[1]

    def load_x(r):
        here = pl.ds(pl.multiple_of(r * TILE, TILE), TILE)
        return pltpu.make_async_copy(x_hbm.at[here, :], x_ref.at[here, :], x_sem.at[r])

    @pl.when(j == 0)
    def _():
        for r in range(rows // TILE):
            load_x(r).start()
        pltpu.make_async_copy(featt_hbm, featt, feat_sem).start()

    @pl.when(j == 1)
    def _():
        pltpu.make_async_copy(featt_hbm, featt, feat_sem).wait()

    def moves(b):
        span = pl.ds(pl.multiple_of(b * bn, bn), bn)
        slot = lax.rem(b, 2)
        return [(pltpu.make_async_copy(src.at[span, :], ring.at[slot, i], load_sem.at[slot, i]),
                 pltpu.make_async_copy(ring.at[slot, i], dst.at[span, :], store_sem.at[slot, i]))
                for i, (src, dst) in enumerate(((p_ref, p_out), (q_ref, q_out)))]

    @pl.when(j >= 2)
    def _():
        for _, store in moves(j - 2):
            store.wait()

    @pl.when(j < nb)
    def _():
        for load, _ in moves(j):
            load.start()

    @pl.when((j >= 1) & (j <= nb))
    def _():
        for load, store in moves(j - 1):
            load.wait()
            store.start()

    def fin():
        def put(r, v):
            dpre[r:r + CHUNK, :] = v

        db, dg = finish_back(rows, acc, n1_ref, i1_ref[...], g1_ref[...], b1_ref[...], put)
        half = dw1b_ref.shape[0]
        for i, row in enumerate((dg, db, dg2_ref[...], db2_ref[...], loss_ref[...])):
            dw1a_ref[half + i:half + i + 1, :] = row

    def mm():
        for r in range(0, rows, TILE):
            acc[r:r + TILE, :] = dot(x_ref[r:r + TILE, :], w2_ref[...], ((1,), (1,)))

    def dw():
        half = dw1b_ref.shape[0]
        dw1a_ref[:half, :] = dot(featt[:half, :], dpre[...])
        dw1b_ref[...] = dot(featt[half:, :], dpre[...])

    @pl.when(j == 0)
    def _():
        def work(r, carry):
            load_x(r).wait()
            here = pl.ds(pl.multiple_of(r * TILE, TILE), TILE)
            acc[here, :] = dot(x_ref[here, :], w2_ref[...], ((1,), (1,)))
            return carry

        lax.fori_loop(0, rows // TILE, work, 0)

    @pl.when((j > 0) & (j < nb))
    def _():
        fin()
        mm()
        dw()

    @pl.when(j == nb)
    def _():
        fin()
        dw()


def back_c(x, featt, w2, n1, i1, g1, b1, dg2, db2, loss, p, q, bn=256):
    rows, d = x.shape
    k = featt.shape[0]
    nb = d // bn

    def at(first):
        return lambda j: (0, jnp.clip(j - first, 0, nb - 1))

    col = pl.BlockSpec((1, bn), at(1))
    row = pl.BlockSpec((bn, d), lambda j: (jnp.minimum(j, nb - 1), 0))
    any_spec = pl.BlockSpec(memory_space=pl.ANY)
    return pl.pallas_call(
        functools.partial(back_c_kernel, nb, rows),
        grid=(nb + 2,),
        in_specs=[any_spec, any_spec,
                  row, pl.BlockSpec((rows, bn), at(1)), col, col, col, col, col, pl.BlockSpec((1, bn), lambda j: (0, 0)), any_spec, any_spec],
        out_specs=[any_spec, any_spec, pl.BlockSpec((k // 2 + 8, bn), at(1)), pl.BlockSpec((k // 2, bn), at(1))],
        out_shape=[jax.ShapeDtypeStruct((d, d), F32)] * 2 + [jax.ShapeDtypeStruct((k // 2 + 8, d), F32), jax.ShapeDtypeStruct((k // 2, d), F32)],
        scratch_shapes=[pltpu.VMEM((rows, bn), F32), pltpu.VMEM((rows, bn), BF16), pltpu.VMEM((2, 2, bn, d), F32),
                        pltpu.VMEM((rows, d), BF16), pltpu.VMEM((k, rows), BF16), pltpu.SemaphoreType.DMA((2, 2)),
                        pltpu.SemaphoreType.DMA((2, 2)), pltpu.SemaphoreType.DMA((rows // TILE,)), pltpu.SemaphoreType.DMA],
        compiler_params=pltpu.CompilerParams(vmem_limit_bytes=VMEM_LIMIT),
        cost_estimate=pl.CostEstimate(flops=2 * rows * d * (k + d), bytes_accessed=rows * d * 20, transcendentals=0),
        name='back_c',
    )(x, featt, w2, n1, i1, g1, b1, dg2, db2, loss, p, q)


def add_first_kernel(p_ref, q_ref, out_ref, small_ref):
    half = out_ref.shape[0]
    out_ref[...] = p_ref[:half, :] + q_ref[:half, :]
    small_ref[...] = p_ref[half:, :] + q_ref[half:, :]


def add_second_kernel(p_ref, q_ref, _, out_ref):
    out_ref[...] = p_ref[...] + q_ref[...]


def add_half(p, q, half, whole=None):
    rows, d = p.shape
    blk = d // 2
    spec = pl.BlockSpec((rows, blk), lambda j: (0, j))
    first = whole is None
    out_specs = [pl.BlockSpec((half, blk), lambda j: (0 if first else 1, j))]
    out_shape = [jax.ShapeDtypeStruct((2 * half, d), F32)]
    if first:
        out_specs.append(pl.BlockSpec((rows - half, blk), lambda j: (0, j)))
        out_shape.append(jax.ShapeDtypeStruct((rows - half, d), F32))
    return pl.pallas_call(
        add_first_kernel if first else add_second_kernel,
        grid=(2,),
        in_specs=[spec, spec] + ([] if first else [pl.BlockSpec(memory_space=pl.ANY)]),
        out_specs=out_specs,
        out_shape=out_shape,
        input_output_aliases={} if first else {2: 0},
        compiler_params=pltpu.CompilerParams(vmem_limit_bytes=24 * 1024 * 1024),
        cost_estimate=pl.CostEstimate(flops=rows * d * 2000, bytes_accessed=rows * d * 12, transcendentals=0),
        name='add_half',
    )(*([p, q] if first else [p, q, whole]))


def solution(mesh):
    n = mesh.shape[AXIS]
    pair = [(i, i + 1 - 2 * (i % 2)) for i in range(n)]

    def swap(x):
        return lax.ppermute(x, AXIS, pair)

    def local_step(feat_a, feat_b, w_one, w_two, w_three, g_one, b_one, g_two, b_two, lam_off):
        width = w_two.shape[0]
        g1, b1, g2, b2 = (v.reshape(1, width) for v in (g_one, b_one, g_two, b_two))
        norm1, norm2, norm3, inv1, inv2, inv3, act1t, act2t, xt, emb, other = forward(
            feat_a, feat_b, w_one, w_two, w_three, g1, b1, g2, b2, n)
        loss, d_pre2, dg2, db2, dw3, dw2 = back_ab(
            lam_off.reshape(1, 1), emb, other, norm3, inv3, w_three, norm2, inv2, g2, b2, act2t, act1t)
        dw3, dw2, dw1a, dw1b = back_c(d_pre2, xt, w_two, norm1, inv1, g1, b1, dg2, db2, loss, dw3, dw2)
        half = dw1b.shape[0]
        dw1, small = add_half(dw1a, swap(dw1a), half)
        dw1, = add_half(dw1b, swap(dw1b), half, dw1)
        dg1, db1, dg2, db2 = (small[i] for i in range(4))
        loss_val = jnp.sum(small[4, :loss.shape[1]]) * 0.5
        return (loss_val, dw1, dw2, dw3, dg1, db1, dg2, db2)

    row_spec = P(AXIS, None)
    return jax.shard_map(local_step, mesh=mesh, in_specs=(row_spec, row_spec) + (P(),) * 8, out_specs=(P(),) * 8, check_vma=False)
```

```python
import functools

import jax
import jax.numpy as jnp
from jax import lax
from jax.experimental import pallas as pl
from jax.experimental.pallas import tpu as pltpu
from jax.sharding import PartitionSpec as P

NORM_EPS = 1e-5
AXIS = 'data'
MESH = pl.DeviceIdType.MESH
F32 = jnp.float32
BF16 = jnp.bfloat16
ONCE = pl.Buffered(1)
VMEM_LIMIT = 60 * 1024 * 1024
TILE = 256
SMALL = 128
CHUNK = 64


def fold(v):
    return jnp.sum(v.reshape(v.shape[0] // 8, 8, v.shape[1]), axis=0)


def dot(a, b, dims=((1,), (0,))):
    return lax.dot_general(a, b, (dims, ((), ())), preferred_element_type=F32)


def forward_kernel(nb, rows, fa_ref, fb_ref, w1_ref, w2_ref, w3_ref, g1_ref, b1_ref, g2_ref, b2_ref,
                   n1_hbm, n2_ref, n3_ref, i1_ref, i2_ref, i3_ref, t1_ref, t2_ref, xt_ref, emb_hbm, other_hbm,
                   xs, w1_buf, pre1, sums1, bufa, bufb, acc, sums, w1_sem, norm_sem, copy_sem, feat_sem, send_sem, recv_sem, esend_sem, erecv_sem):
    j = pl.program_id(0)
    me = lax.axis_index(AXIS)
    core = lax.rem(me, 2)
    chip = me // 2
    x_pos, y_pos = lax.rem(chip, 2), chip // 2
    partner = me + 1 - 2 * core
    x_chip, y_chip = chip + 1 - 2 * x_pos, chip + 2 - 4 * y_pos
    piece = fa_ref.shape[0]
    bn = acc.shape[1]

    def remote(src, dst, send, recv, dev):
        return pltpu.make_async_remote_copy(src_ref=src, dst_ref=dst, send_sem=send, recv_sem=recv, device_id=(dev,), device_id_type=MESH)

    def part(dev):
        return xs.at[pl.ds(pl.multiple_of(dev * piece, piece), piece), :]

    def gather():
        pltpu.make_async_copy(w1_ref, w1_buf, w1_sem).start()
        barrier = pltpu.get_barrier_semaphore()
        for dev in (partner, 2 * x_chip, 2 * x_chip + 1, 2 * y_chip, 2 * y_chip + 1):
            pl.semaphore_signal(barrier, inc=1, device_id=(dev,), device_id_type=MESH)
        pl.semaphore_wait(barrier, 5)

        def sends(mine, mine_src, theirs_src):
            for view, src in ((mine, mine_src), (1 - mine, theirs_src)):
                remote(src, part(me), send_sem.at[1 + view], recv_sem.at[1 + mine], 2 * x_chip + view).start()
                remote(src, part(me), send_sem.at[3 + view], recv_sem.at[3 + mine], 2 * y_chip + view).start()
            remote(theirs_src, part(me), send_sem.at[0], recv_sem.at[0], partner).start()
            pltpu.make_async_copy(mine_src, part(me), feat_sem).start()

        pl.when(core == 0)(lambda: sends(0, fa_ref, fb_ref))
        pl.when(core == 1)(lambda: sends(1, fb_ref, fa_ref))
        remote(fa_ref, part(2 * x_chip), send_sem.at[1], recv_sem.at[1], me).wait_recv()
        relay_y = remote(part(2 * x_chip), part(2 * x_chip), send_sem.at[5], recv_sem.at[5], 2 * y_chip + core)
        relay_y.start()
        remote(fa_ref, part(2 * y_chip + 1), send_sem.at[4], recv_sem.at[4], me).wait_recv()
        relay_x = remote(part(2 * y_chip + 1), part(2 * y_chip + 1), send_sem.at[6], recv_sem.at[6], 2 * x_chip + core)
        relay_x.start()
        pltpu.make_async_copy(fa_ref, part(me), feat_sem).wait()
        remote(fa_ref, part(me), send_sem.at[0], recv_sem.at[0], me).wait()
        pltpu.make_async_copy(w1_ref, w1_buf, w1_sem).wait()
        layer_one(me, partner)
        layer_one(2 * x_chip, 2 * y_chip + 1)
        remote(fa_ref, part(me), send_sem.at[1], recv_sem.at[2], me).wait()
        remote(fa_ref, part(me), send_sem.at[2], recv_sem.at[3], me).wait()
        layer_one(2 * x_chip + 1, 2 * y_chip)
        remote(fa_ref, part(me), send_sem.at[3], recv_sem.at[5], me).wait()
        remote(fa_ref, part(me), send_sem.at[4], recv_sem.at[6], me).wait()
        far = 2 * (3 - chip)
        layer_one(far, far + 1)
        relay_y.wait_send()
        relay_x.wait_send()

    def layer_one(dev_p, dev_q):
        def work(i, carry):
            here = pl.ds(pl.multiple_of(jnp.where(i == 0, dev_p, dev_q) * piece, piece), piece)
            feats = xs[here, :]
            for c in range(0, w1_buf.shape[1], bn):
                pre = dot(feats, w1_buf[:, c:c + bn])
                pre1[here, c:c + bn] = pre
                sums1[0:8, c:c + bn] += fold(pre)
                sums1[8:16, c:c + bn] += fold(pre * pre)
            return carry

        lax.fori_loop(0, 2, work, 0)

    def norm_copy(block):
        cols = pl.ds(pl.multiple_of(block * bn, bn), bn)
        return pltpu.make_async_copy(pre1.at[:, cols], n1_hbm.at[:, cols], norm_sem.at[block])

    def finish_one():
        mean = jnp.sum(sums1[0:8, :], axis=0, keepdims=True) / rows
        inv = lax.rsqrt(jnp.sum(sums1[8:16, :], axis=0, keepdims=True) / rows - mean * mean + NORM_EPS)
        sums1[0:1, :] = mean
        i1_ref[...] = inv

        def work(block, carry):
            cols = pl.ds(pl.multiple_of(block * bn, bn), bn)
            mean, inv, g, b = sums1[0:1, cols], i1_ref[:, cols], g1_ref[:, cols], b1_ref[:, cols]
            for r in range(0, rows, CHUNK):
                norm = (pre1[r:r + CHUNK, cols] - mean) * inv
                pre1[r:r + CHUNK, cols] = norm
                bufa[r:r + CHUNK, cols] = jnp.maximum(norm * g + b, 0.0).astype(BF16)
            return carry

        lax.fori_loop(0, nb, work, 0)
        for block in range(nb):
            norm_copy(block).start()

    def fin(layer):
        norm_ref, inv_ref = ((n2_ref, i2_ref), (n3_ref, i3_ref))[layer]
        buf = (bufb, bufa)[layer]
        base = pl.multiple_of(jnp.maximum(j - 1 - layer * nb, 0) * bn, bn)
        mean = jnp.sum(sums[0:8, :], axis=0, keepdims=True) / rows
        inv = lax.rsqrt(jnp.sum(sums[8:16, :], axis=0, keepdims=True) / rows - mean * mean + NORM_EPS)
        inv_ref[...] = inv
        if layer == 0:
            g, b = g2_ref[...], b2_ref[...]
        for r in range(0, rows, CHUNK):
            norm = (acc[r:r + CHUNK, :] - mean) * inv
            norm_ref[r:r + CHUNK, :] = norm
            if layer == 0:
                norm = jnp.maximum(norm * g + b, 0.0)
            buf[r:r + CHUNK, pl.ds(base, bn)] = norm.astype(BF16)
        if layer == 0:
            for r in range(0, rows, TILE):
                t2_ref[:, r:r + TILE] = buf[r:r + TILE, pl.ds(base, bn)].T

    def mm(layer):
        x_ref, w_ref = ((bufa, w2_ref), (bufb, w3_ref))[layer]
        total = jnp.zeros((8, bn), F32)
        square = jnp.zeros((8, bn), F32)
        for r in range(0, rows, SMALL):
            pre = dot(x_ref[r:r + SMALL, :], w_ref[...])
            acc[r:r + SMALL, :] = pre
            total += fold(pre)
            square += fold(pre * pre)
        sums[0:8, :] = total
        sums[8:16, :] = square

    def out_copy(block):
        cols = pl.ds(pl.multiple_of(block * bn, bn), bn)
        return pltpu.make_async_copy(bufa.at[:, cols], emb_hbm.at[:, cols], copy_sem.at[block])

    def emb_copy(block):
        cols = pl.ds(pl.multiple_of(block * bn, bn), bn)
        return remote(bufa.at[:, cols], other_hbm.at[:, cols], esend_sem.at[block], erecv_sem.at[block], partner)

    @pl.when(j == 0)
    def _():
        sums1[...] = jnp.zeros_like(sums1)
        gather()
        finish_one()

    for layer in range(2):
        @pl.when((j >= layer * nb) & (j < (layer + 1) * nb))
        def _(layer=layer):
            fin(layer)
            mm(layer)
            if layer == 0:
                base = pl.multiple_of(j * bn, bn)
                for r in range(0, rows, TILE):
                    t1_ref[:, r:r + TILE] = bufa[r:r + TILE, pl.ds(base, bn)].T

        @pl.when(j == (layer + 1) * nb)
        def _(layer=layer):
            fin(layer)

    @pl.when(j >= nb + 2)
    def _():
        block = j - 2 - nb
        out_copy(block).start()
        emb_copy(block).start()

    @pl.when(j == nb + 1)
    def _():
        for r in range(0, rows, TILE):
            xt_ref[:, r:r + TILE] = xs[r:r + TILE, :].T

    @pl.when(j == 2 * nb + 1)
    def _():
        for block in range(nb):
            norm_copy(block).wait()
            out_copy(block).wait()
            emb_copy(block).wait()


def forward(fa, fb, w1, w2, w3, g1, b1, g2, b2, n, bn=256):
    piece, k = fa.shape
    rows, d = piece * n, w2.shape[1]
    nb = d // bn

    def at(layer, delay):
        return lambda j: (0, jnp.clip(j - layer * nb - delay, 0, nb - 1))

    whole = pl.BlockSpec((piece, k), lambda j: (0, 0), pipeline_mode=ONCE)
    any_spec = pl.BlockSpec(memory_space=pl.ANY)
    col = [pl.BlockSpec((1, bn), at(layer, 1)) for layer in range(2)]
    norm = [pl.BlockSpec((rows, bn), at(layer, 1)) for layer in range(2)]
    vec = pl.BlockSpec((1, d), lambda j: (0, 0))
    big = jax.ShapeDtypeStruct((rows, d), BF16)
    return pl.pallas_call(
        functools.partial(forward_kernel, nb, rows),
        grid=(2 * nb + 2,),
        in_specs=[whole, whole, any_spec, pl.BlockSpec((d, bn), at(0, 0)), pl.BlockSpec((d, bn), at(1, 0)),
                  vec, vec, col[0], col[0]],
        out_specs=[any_spec] + norm + [vec] + col + [pl.BlockSpec((bn, rows), lambda j, f=at(0, delay): f(j)[::-1]) for delay in range(2)]
        + [pl.BlockSpec((k, rows), lambda j: (0, 0), pipeline_mode=ONCE)] + [any_spec] * 2,
        out_shape=[jax.ShapeDtypeStruct((rows, d), F32)] * 3 + [jax.ShapeDtypeStruct((1, d), F32)] * 3
        + [jax.ShapeDtypeStruct((d, rows), BF16)] * 2 + [jax.ShapeDtypeStruct((k, rows), BF16)] + [big] * 2,
        scratch_shapes=[pltpu.VMEM((rows, k), BF16), pltpu.VMEM((k, d), BF16), pltpu.VMEM((rows, d), F32), pltpu.VMEM((16, d), F32),
                        pltpu.VMEM((rows, d), BF16), pltpu.VMEM((rows, d), BF16), pltpu.VMEM((rows, bn), F32), pltpu.VMEM((16, bn), F32),
                        pltpu.SemaphoreType.DMA, pltpu.SemaphoreType.DMA((nb,)),
                        pltpu.SemaphoreType.DMA((nb,)), pltpu.SemaphoreType.DMA, pltpu.SemaphoreType.DMA((7,)), pltpu.SemaphoreType.DMA((7,)),
                        pltpu.SemaphoreType.DMA((nb,)), pltpu.SemaphoreType.DMA((nb,))],
        compiler_params=pltpu.CompilerParams(collective_id=0, has_side_effects=True, vmem_limit_bytes=63 * 1024 * 1024),
        cost_estimate=pl.CostEstimate(flops=2 * rows * d * (k + 2 * d), bytes_accessed=rows * d * 20, transcendentals=0),
        name='forward',
    )(fa, fb, w1, w2, w3, g1, b1, g2, b2)


def finish_back(rows, acc, norm_ref, inv, g, b, put):
    bn = acc.shape[1]
    total = jnp.zeros((8, bn), F32)
    cross = jnp.zeros((8, bn), F32)
    for r in range(0, rows, CHUNK):
        part = acc[r:r + CHUNK, :]
        norm = norm_ref[r:r + CHUNK, :]
        if b is not None:
            part = jnp.where(norm * g + b > 0.0, part, 0.0)
            acc[r:r + CHUNK, :] = part
        total += fold(part)
        cross += fold(part * norm)
    total = jnp.sum(total, axis=0, keepdims=True)
    cross = jnp.sum(cross, axis=0, keepdims=True)
    scale = inv if g is None else inv * g
    shift, slope = scale * (total / rows), scale * (cross / rows)
    for r in range(0, rows, CHUNK):
        put(r, (acc[r:r + CHUNK, :] * scale - shift - norm_ref[r:r + CHUNK, :] * slope).astype(BF16))
    return total, cross


def back_ab_kernel(nb, rows, lam_ref, own_ref, other_hbm, n3_ref, i3_ref, w3_ref, n2_ref, i2_ref, g2_ref, b2_ref, t2_ref, t1_hbm,
                   loss_ref, dpre_ref, dg_ref, db_ref, dw3_hbm, dw2_hbm,
                   big, corr, grad, acc, dout, send3, recv3, send2, recv2, load_sem, chunk_sem, ssem, rsem, osem, free3, free2):
    j = pl.program_id(0)
    me = lax.axis_index(AXIS)
    partner = me + 1 - 2 * lax.rem(me, 2)
    bn = acc.shape[1]
    d = big.shape[1]
    lam = lam_ref[0, 0]
    other_ref = big

    def pair(e):
        return ((send3, recv3, free3, nb), (send2, recv2, free2, nb + 1))[e]

    def swap_copy(e, b, part=None):
        send, recv, _, _ = pair(e)
        src, dst = send.at[lax.rem(b, 2)], recv.at[lax.rem(b, 3)]
        if part is not None:
            src, dst = src.at[part, :], dst.at[part, :]
        return pltpu.make_async_remote_copy(
            src_ref=src, dst_ref=dst, send_sem=ssem.at[e, lax.rem(b, 2)],
            recv_sem=rsem.at[e, lax.rem(b, 3)], device_id=(partner,), device_id_type=MESH)

    def sum_copy(e, b):
        span = pl.ds(pl.multiple_of(b * bn, bn), bn)
        dst = dw3_hbm.at[span, :] if e == 0 else dw2_hbm.at[:, span]
        return pltpu.make_async_copy(pair(e)[1].at[lax.rem(b, 3)], dst, osem.at[e, lax.rem(b, 3)])

    def exchange(e):
        send, recv, free, first = pair(e)

        @pl.when((j >= first + 3) & (j < first + 3 + nb))
        def _():
            b = j - first - 3
            sum_copy(e, b).wait()

            @pl.when(b < nb - 3)
            def _():
                pl.semaphore_signal(free, inc=1, device_id=(partner,), device_id_type=MESH)

        @pl.when((j >= first + 2) & (j < first + 2 + nb))
        def _():
            b = j - first - 2
            swap_copy(e, b).wait()
            mine, theirs = lax.rem(b, 2), lax.rem(b, 3)
            for r in range(0, send.shape[1], send.shape[1] // 32):
                part = pl.ds(r, send.shape[1] // 32)
                recv[theirs, part, :] = recv[theirs, part, :] + send[mine, part, :]
            sum_copy(e, b).start()

    def ready(e, b):
        @pl.when(b >= 3)
        def _():
            pl.semaphore_wait(pair(e)[2], 1)

    def fin_loss():
        base = pl.multiple_of(jnp.maximum(j - 1, 0) * bn, bn)

        def put(r, v):
            dout[r:r + CHUNK, pl.ds(base, bn)] = v

        finish_back(rows, acc, n3_ref, i3_ref[...], None, None, put)

    def load_other(c):
        cols = pl.ds(pl.multiple_of(c * bn, bn), bn)
        return pltpu.make_async_copy(other_hbm.at[:, cols], big.at[:, cols], chunk_sem.at[c])

    def mm_loss(arriving):
        own = own_ref[...]

        def correlate(c, loss):
            cols = pl.ds(pl.multiple_of(c * bn, bn), bn)
            if arriving:
                load_other(c).wait()
            part = dot(own, other_ref[:, cols], ((0,), (0,))) * (1.0 / rows)
            corr[:, cols] = part
            grad[:, cols] = ((2.0 * lam) * part).astype(BF16)
            return loss + fold(part * part)

        loss = jnp.zeros((8, bn), F32)
        if arriving:
            loss = lax.fori_loop(0, nb, correlate, loss)
        else:
            for c in range(nb):
                loss = correlate(c, loss)
        here = pl.ds(pl.multiple_of(j * bn, bn), bn)
        part = corr[:, here]
        diag = lax.broadcasted_iota(jnp.int32, (bn, bn), 0) == lax.broadcasted_iota(jnp.int32, (bn, bn), 1)
        grad[:, here] = jnp.where(diag, -2.0 * (1.0 - part), (2.0 * lam) * part).astype(BF16)
        loss = lam * loss + fold(jnp.where(diag, (1.0 - part) * (1.0 - part) - lam * (part * part), 0.0))
        loss_ref[...] += jnp.sum(loss, axis=0, keepdims=True)
        for r in range(0, rows, TILE):
            acc[r:r + TILE, :] = dot(other_ref[r:r + TILE, :], grad[...], ((1,), (1,))) * (1.0 / rows)

    def fin_two():
        def put(r, v):
            dpre_ref[r:r + CHUNK, :] = v

        db_ref[...], dg_ref[...] = finish_back(rows, acc, n2_ref, i2_ref[...], g2_ref[...], b2_ref[...], put)

    def mm_two():
        for r in range(0, rows, TILE):
            acc[r:r + TILE, :] = dot(dout[r:r + TILE, :], w3_ref[...], ((1,), (1,)))
        act = t2_ref[...]
        slot = lax.rem(j - nb, 2)
        for c in range(0, d, 2 * bn):
            send3[slot, :, c:c + 2 * bn] = dot(act, dout[:, c:c + 2 * bn])

    def mm_dw2(first, last):
        slot = lax.rem(j - nb - 1, 2)
        for r in range(first, last, TILE):
            send2[slot, r:r + TILE, :] = dot(big[r:r + TILE, :], dpre_ref[...])

    @pl.when(j == 0)
    def _():
        for c in range(nb):
            load_other(c).start()
        loss_ref[...] = jnp.zeros_like(loss_ref)
        barrier = pltpu.get_barrier_semaphore()
        pl.semaphore_signal(barrier, inc=1, device_id=(partner,), device_id_type=MESH)
        pl.semaphore_wait(barrier, 1)
        mm_loss(True)

    @pl.when(j == nb)
    def _():
        pltpu.make_async_copy(t1_hbm, big, load_sem).start()

    exchange(0)
    exchange(1)

    @pl.when((j > 0) & (j < nb))
    def _():
        fin_loss()
        mm_loss(False)

    @pl.when(j == nb)
    def _():
        fin_loss()

    @pl.when((j >= nb) & (j < 2 * nb))
    def _():
        fin_two()
        mm_two()
        ready(0, j - nb)
        swap_copy(0, j - nb).start()

    @pl.when(j == 2 * nb)
    def _():
        fin_two()

    @pl.when(j == nb + 1)
    def _():
        pltpu.make_async_copy(t1_hbm, big, load_sem).wait()

    @pl.when((j > nb) & (j < 2 * nb))
    def _():
        mm_dw2(0, d)
        ready(1, j - nb - 1)
        swap_copy(1, j - nb - 1).start()

    @pl.when(j == 2 * nb)
    def _():
        ready(1, nb - 1)
        for r in range(0, d, d // 4):
            mm_dw2(r, r + d // 4)
            swap_copy(1, nb - 1, pl.ds(r, d // 4)).start()


def back_ab(lam, own, other, n3, i3, w3, n2, i2, g2, b2, t2, t1, bn=256):
    rows, d = own.shape
    nb = d // bn

    def at(first):
        return lambda j: (0, jnp.clip(j - first, 0, nb - 1))

    def block(first):
        return pl.BlockSpec((rows, bn), at(first))

    def col(first):
        return pl.BlockSpec((1, bn), at(first))

    row = pl.BlockSpec((bn, d), lambda j: (jnp.clip(j - nb, 0, nb - 1), 0))
    vec = jax.ShapeDtypeStruct((1, d), F32)
    any_spec = pl.BlockSpec(memory_space=pl.ANY)
    return pl.pallas_call(
        functools.partial(back_ab_kernel, nb, rows),
        grid=(2 * nb + 4,),
        in_specs=[pl.BlockSpec(memory_space=pltpu.SMEM), block(0), any_spec,
                  block(1), col(1), row, block(nb + 1), col(nb + 1), col(nb + 1), col(nb + 1), row, any_spec],
        out_specs=[pl.BlockSpec((1, bn), lambda j: (0, 0)), block(nb + 1), col(nb + 1), col(nb + 1), any_spec, any_spec],
        out_shape=[jax.ShapeDtypeStruct((1, bn), F32), jax.ShapeDtypeStruct((rows, d), BF16), vec, vec]
        + [jax.ShapeDtypeStruct((d, d), F32)] * 2,
        scratch_shapes=[pltpu.VMEM((rows, d), BF16), pltpu.VMEM((bn, d), F32), pltpu.VMEM((bn, d), BF16), pltpu.VMEM((rows, bn), F32),
                        pltpu.VMEM((rows, d), BF16), pltpu.VMEM((2, bn, d), F32), pltpu.VMEM((3, bn, d), F32),
                        pltpu.VMEM((2, d, bn), F32), pltpu.VMEM((3, d, bn), F32), pltpu.SemaphoreType.DMA, pltpu.SemaphoreType.DMA((nb,)),
                        pltpu.SemaphoreType.DMA((2, 2)), pltpu.SemaphoreType.DMA((2, 3)), pltpu.SemaphoreType.DMA((2, 3)),
                        pltpu.SemaphoreType.REGULAR, pltpu.SemaphoreType.REGULAR],
        compiler_params=pltpu.CompilerParams(collective_id=1, has_side_effects=True, vmem_limit_bytes=63 * 1024 * 1024),
        cost_estimate=pl.CostEstimate(flops=10 * rows * d * d, bytes_accessed=rows * d * 24, transcendentals=0),
        name='back_ab',
    )(lam, own, other, n3, i3, w3, n2, i2, g2, b2, t2, t1)


def back_c_kernel(nb, rows, x_hbm, featt_hbm, w2_ref, n1_ref, i1_ref, g1_ref, b1_ref, dg2_ref, db2_ref, loss_ref, p_ref, q_ref,
                  p_out, q_out, dw1a_ref, dw1b_ref, acc, dpre, ring, x_ref, featt, load_sem, store_sem, x_sem, feat_sem):
    j = pl.program_id(0)
    bn = acc.shape[1]

    def load_x(r):
        here = pl.ds(pl.multiple_of(r * TILE, TILE), TILE)
        return pltpu.make_async_copy(x_hbm.at[here, :], x_ref.at[here, :], x_sem.at[r])

    @pl.when(j == 0)
    def _():
        for r in range(rows // TILE):
            load_x(r).start()
        pltpu.make_async_copy(featt_hbm, featt, feat_sem).start()

    @pl.when(j == 1)
    def _():
        pltpu.make_async_copy(featt_hbm, featt, feat_sem).wait()

    def moves(b):
        span = pl.ds(pl.multiple_of(b * bn, bn), bn)
        slot = lax.rem(b, 2)
        return [(pltpu.make_async_copy(src.at[span, :], ring.at[slot, i], load_sem.at[slot, i]),
                 pltpu.make_async_copy(ring.at[slot, i], dst.at[span, :], store_sem.at[slot, i]))
                for i, (src, dst) in enumerate(((p_ref, p_out), (q_ref, q_out)))]

    @pl.when(j >= 2)
    def _():
        for _, store in moves(j - 2):
            store.wait()

    @pl.when(j < nb)
    def _():
        for load, _ in moves(j):
            load.start()

    @pl.when((j >= 1) & (j <= nb))
    def _():
        for load, store in moves(j - 1):
            load.wait()
            store.start()

    def fin():
        def put(r, v):
            dpre[r:r + CHUNK, :] = v

        db, dg = finish_back(rows, acc, n1_ref, i1_ref[...], g1_ref[...], b1_ref[...], put)
        half = dw1b_ref.shape[0]
        for i, row in enumerate((dg, db, dg2_ref[...], db2_ref[...], loss_ref[...])):
            dw1a_ref[half + i:half + i + 1, :] = row

    def mm():
        for r in range(0, rows, TILE):
            acc[r:r + TILE, :] = dot(x_ref[r:r + TILE, :], w2_ref[...], ((1,), (1,)))

    def dw():
        half = dw1b_ref.shape[0]
        dw1a_ref[:half, :] = dot(featt[:half, :], dpre[...])
        dw1b_ref[...] = dot(featt[half:, :], dpre[...])

    @pl.when(j == 0)
    def _():
        def work(r, carry):
            load_x(r).wait()
            here = pl.ds(pl.multiple_of(r * TILE, TILE), TILE)
            acc[here, :] = dot(x_ref[here, :], w2_ref[...], ((1,), (1,)))
            return carry

        lax.fori_loop(0, rows // TILE, work, 0)

    @pl.when((j > 0) & (j < nb))
    def _():
        fin()
        mm()
        dw()

    @pl.when(j == nb)
    def _():
        fin()
        dw()


def back_c(x, featt, w2, n1, i1, g1, b1, dg2, db2, loss, p, q, bn=256):
    rows, d = x.shape
    k = featt.shape[0]
    nb = d // bn

    def at(first):
        return lambda j: (0, jnp.clip(j - first, 0, nb - 1))

    col = pl.BlockSpec((1, bn), at(1))
    row = pl.BlockSpec((bn, d), lambda j: (jnp.minimum(j, nb - 1), 0))
    any_spec = pl.BlockSpec(memory_space=pl.ANY)
    return pl.pallas_call(
        functools.partial(back_c_kernel, nb, rows),
        grid=(nb + 2,),
        in_specs=[any_spec, any_spec,
                  row, pl.BlockSpec((rows, bn), at(1)), col, col, col, col, col, pl.BlockSpec((1, bn), lambda j: (0, 0)), any_spec, any_spec],
        out_specs=[any_spec, any_spec, pl.BlockSpec((k // 2 + 8, bn), at(1)), pl.BlockSpec((k // 2, bn), at(1))],
        out_shape=[jax.ShapeDtypeStruct((d, d), F32)] * 2 + [jax.ShapeDtypeStruct((k // 2 + 8, d), F32), jax.ShapeDtypeStruct((k // 2, d), F32)],
        scratch_shapes=[pltpu.VMEM((rows, bn), F32), pltpu.VMEM((rows, bn), BF16), pltpu.VMEM((2, 2, bn, d), F32),
                        pltpu.VMEM((rows, d), BF16), pltpu.VMEM((k, rows), BF16), pltpu.SemaphoreType.DMA((2, 2)),
                        pltpu.SemaphoreType.DMA((2, 2)), pltpu.SemaphoreType.DMA((rows // TILE,)), pltpu.SemaphoreType.DMA],
        compiler_params=pltpu.CompilerParams(vmem_limit_bytes=VMEM_LIMIT),
        cost_estimate=pl.CostEstimate(flops=2 * rows * d * (k + d), bytes_accessed=rows * d * 20, transcendentals=0),
        name='back_c',
    )(x, featt, w2, n1, i1, g1, b1, dg2, db2, loss, p, q)


def add_first_kernel(loss_width, p_ref, q_ref, out_ref, dg1_ref, db1_ref, dg2_ref, db2_ref, loss_ref):
    half = out_ref.shape[0]
    out_ref[...] = p_ref[:half, :] + q_ref[:half, :]
    small = p_ref[half:, :] + q_ref[half:, :]
    for i, ref in enumerate((dg1_ref, db1_ref, dg2_ref, db2_ref)):
        ref[...] = small[i:i + 1, :]

    @pl.when(pl.program_id(0) == 0)
    def _():
        loss_ref[0, 0] = jnp.sum(small[4:5, :loss_width]) * 0.5


def add_second_kernel(p_ref, q_ref, _, out_ref):
    out_ref[...] = p_ref[...] + q_ref[...]


def add_half(p, q, half, whole=None, loss_width=0):
    rows, d = p.shape
    blk = d // 2
    spec = pl.BlockSpec((rows, blk), lambda j: (0, j))
    first = whole is None
    out_specs = [pl.BlockSpec((half, blk), lambda j: (0 if first else 1, j))]
    out_shape = [jax.ShapeDtypeStruct((2 * half, d), F32)]
    if first:
        out_specs += [pl.BlockSpec((1, blk), lambda j: (0, j))] * 4 + [pl.BlockSpec(memory_space=pltpu.SMEM)]
        out_shape += [jax.ShapeDtypeStruct((1, d), F32)] * 4 + [jax.ShapeDtypeStruct((1, 1), F32)]
    return pl.pallas_call(
        functools.partial(add_first_kernel, loss_width) if first else add_second_kernel,
        grid=(2,),
        in_specs=[spec, spec] + ([] if first else [pl.BlockSpec(memory_space=pl.ANY)]),
        out_specs=out_specs,
        out_shape=out_shape,
        input_output_aliases={} if first else {2: 0},
        compiler_params=pltpu.CompilerParams(vmem_limit_bytes=24 * 1024 * 1024),
        cost_estimate=pl.CostEstimate(flops=rows * d * 2000, bytes_accessed=rows * d * 12, transcendentals=0),
        name='add_half',
    )(*([p, q] if first else [p, q, whole]))


def solution(mesh):
    n = mesh.shape[AXIS]
    pair = [(i, i + 1 - 2 * (i % 2)) for i in range(n)]

    def swap(x):
        return lax.ppermute(x, AXIS, pair)

    def local_step(feat_a, feat_b, w_one, w_two, w_three, g_one, b_one, g_two, b_two, lam_off):
        width = w_two.shape[0]
        g1, b1, g2, b2 = (v.reshape(1, width) for v in (g_one, b_one, g_two, b_two))
        norm1, norm2, norm3, inv1, inv2, inv3, act1t, act2t, xt, emb, other = forward(
            feat_a, feat_b, w_one, w_two, w_three, g1, b1, g2, b2, n)
        loss, d_pre2, dg2, db2, dw3, dw2 = back_ab(
            lam_off.reshape(1, 1), emb, other, norm3, inv3, w_three, norm2, inv2, g2, b2, act2t, act1t)
        dw3, dw2, dw1a, dw1b = back_c(d_pre2, xt, w_two, norm1, inv1, g1, b1, dg2, db2, loss, dw3, dw2)
        half = dw1b.shape[0]
        dw1, dg1, db1, dg2, db2, loss = add_half(dw1a, swap(dw1a), half, loss_width=loss.shape[1])
        dw1, = add_half(dw1b, swap(dw1b), half, dw1)
        dg1, db1, dg2, db2 = (v.reshape(width) for v in (dg1, db1, dg2, db2))
        loss_val = loss.reshape(())
        return (loss_val, dw1, dw2, dw3, dg1, db1, dg2, db2)

    row_spec = P(AXIS, None)
    return jax.shard_map(local_step, mesh=mesh, in_specs=(row_spec, row_spec) + (P(),) * 8, out_specs=(P(),) * 8, check_vma=False)
```
